256 devices in a mesh: tm: 16 (over z, core), space: 16 (over y, x).
Axes of the slice: x: 4, y: 4, z: 8, core: 2. Of those that a mesh axis runs over, the one named last changes fastest.
Arguments:
- residual: float32 [64, 32, 128, 128], P('tm', 'space'), may hold values from -6 to 6
- absorption: float32 [32, 128, 128], P('space'), may hold values from 0.05 to 1
- counts: int32 [64], replicated, may hold values from 1 to 6
Outputs:
- preconditioned: float32 [64, 32, 128, 128], P('tm', 'space')
The draws below stay inside these ranges and needn't reach their ends.
Inputs may be any that keep to these rules, and one draw needn't show every extreme that they name: counts[k] is the number of minimal-residual steps of frequency k.
All inputs are finite; a program needn't handle non-finite values.
Results may differ from the reference program's by a relative error of at most 0.00022.
Values sent between devices are 32-bit elements; how exact they have to be, the bound alone decides.
No kernel may reach another device: no remote copies, remote signals or barrier semaphores. Data moves between devices by JAX's collectives and lax.ppermute only.
A program may use at most 64 MiB of HBM per device.

```python
import math
from functools import partial
import jax
import jax.numpy as jnp
from jax import lax

L = 64
MAXIT = 6
NX = 128
NY = 128
NZ = 32


def plant(drawn, own_key, low, largest):
    spot = [jax.random.randint(jax.random.fold_in(own_key, axis), (), 0, length) for axis, length in enumerate(drawn.shape)]
    main_axis = drawn.shape.index(max(drawn.shape))
    beside = spot[:main_axis] + [(spot[main_axis] + 1) % drawn.shape[main_axis]] + spot[main_axis + 1:]
    return drawn.at[tuple(spot)].set(low).at[tuple(beside)].set(largest)


def block_levels(stream_key, shape, pieces, least, top_value):
    factor_of = 1.0
    for dim, blocks in pieces:
        draws = jax.random.uniform(jax.random.fold_in(jax.random.fold_in(stream_key, 6), dim), (blocks,), jnp.float32, least / len(pieces), top_value / len(pieces))
        factor_of = factor_of * jnp.repeat(jnp.exp(draws), shape[dim] // blocks).reshape((-1,) + (1,) * (len(shape) - 1 - dim))
    return factor_of


def gaussian(rng, dims, scale, most, split=(), kind=jnp.bfloat16):
    entries = scale * jax.random.normal(rng, dims, jnp.float32)
    if split:
        entries = entries * block_levels(rng, dims, split, -0.22, 0.18)
    return jnp.clip(entries, -most, most).astype(kind)


def setup_inputs(seed: int = 0) -> dict:
    key_of = jax.random.split(jax.random.key(seed), 4)
    residual = gaussian(key_of[0], (L, NZ, NX, NY), 1.0, 6.0, ((0, 16), (1, 16)), jnp.float32)
    absorption = jnp.clip(jnp.exp(math.log(1.0) - 2.9957323 * jax.random.uniform(key_of[1], (NZ, NX, NY), jnp.float32) ** block_levels(key_of[1], (NZ, NX, NY), ((0, 16),), -0.2, 0.2)), 0.05, 1.0)
    counts = plant(jax.random.randint(key_of[2], (L,), 1, MAXIT + 1), jax.random.fold_in(key_of[2], 1), 1, MAXIT).astype(jnp.int32)
    return {"residual": residual, "absorption": absorption, "counts": counts}


wrap_factor = 0.1
step_size = 1.0
norm_floor = 1e-6


def neighbours(field):
    padded = jnp.pad(field, 1)
    summed = padded[2:, 1:-1, 1:-1] + padded[:-2, 1:-1, 1:-1]
    summed = summed + padded[1:-1, 2:, 1:-1] + padded[1:-1, :-2, 1:-1]
    summed = summed + padded[1:-1, 1:-1, 2:] + padded[1:-1, 1:-1, :-2]
    return summed


def solve_frequency(packed, absorption):
    rhs_re, rhs_im, step_counts, frequency = packed
    angles = frequency.astype(rhs_re.dtype) * (2.0 * math.pi / L)
    decay_rate = wrap_factor ** (1.0 / L)
    shift_re = (1.0 - decay_rate * jnp.cos(angles)) / step_size
    shift_im = decay_rate * jnp.sin(angles) / step_size
    diag_re = shift_re + 6.0 + absorption
    magnitude = diag_re * diag_re + shift_im * shift_im
    inv_re = diag_re / magnitude
    inv_im = -shift_im / magnitude

    def iterate(iteration, carried):
        sol_re, sol_im, res_re, res_im = carried
        dir_re = inv_re * res_re - inv_im * res_im
        dir_im = inv_re * res_im + inv_im * res_re
        img_re = diag_re * dir_re - shift_im * dir_im - neighbours(dir_re)
        img_im = diag_re * dir_im + shift_im * dir_re - neighbours(dir_im)
        num_re = jnp.sum(img_re * res_re + img_im * res_im)
        num_im = jnp.sum(img_re * res_im - img_im * res_re)
        denominator = jnp.sum(img_re * img_re + img_im * img_im) + norm_floor
        coef_re = num_re / denominator
        coef_im = num_im / denominator
        sol_re = sol_re + coef_re * dir_re - coef_im * dir_im
        sol_im = sol_im + coef_re * dir_im + coef_im * dir_re
        res_re = res_re - (coef_re * img_re - coef_im * img_im)
        res_im = res_im - (coef_re * img_im + coef_im * img_re)
        return sol_re, sol_im, res_re, res_im

    blank = jnp.zeros_like(rhs_re)
    finished = lax.fori_loop(0, step_counts, iterate, (blank, blank, rhs_re, rhs_im))
    return finished[0], finished[1]


def reference(residual, absorption, counts):
    decay_rate = wrap_factor ** (1.0 / L)
    stamps = jnp.arange(L).astype(residual.dtype)
    scaling = jnp.power(decay_rate, stamps)
    spectrum = jnp.fft.fft(residual * scaling[:, None, None, None], axis=0)
    spec_re = spectrum.real
    spec_im = spectrum.imag
    frequencies = jnp.arange(L, dtype=jnp.int32)
    sol_re, sol_im = lax.map(partial(solve_frequency, absorption=absorption), (spec_re, spec_im, counts, frequencies))
    back = jnp.fft.ifft(sol_re + 1j * sol_im, axis=0).real
    unscale = jnp.power(decay_rate, -stamps)
    return (back * unscale[:, None, None, None]).astype(jnp.float32)
```

```python
import math

import jax
import jax.numpy as jnp
import numpy as np
from jax import lax
from jax.experimental import pallas as pl
from jax.experimental.pallas import tpu as pltpu
from jax.sharding import Mesh
from jax.sharding import PartitionSpec as P

L = 64
STEPS = 6
NZ = 32
PAIRS = L // 2
TM = ("z", "core")
SPACE = ("y", "x")
SLOTS = ("core", "y", "x")

wrap_factor = 0.1
step_size = 1.0
norm_floor = 1e-06
highest = lax.Precision.HIGHEST
decay = wrap_factor ** (1.0 / L)

gram_rounding = 2.5e-7
error_allowed = 5e-4


def with_halo(cells, sides, width):
    for axis, dim in sides:
        count = lax.axis_size(axis)
        ends = count - 1
        head = lax.slice_in_dim(cells, 0, width, axis=dim)
        tail = lax.slice_in_dim(cells, cells.shape[dim] - width, cells.shape[dim], axis=dim)
        cells = jnp.concatenate(
            [
                lax.ppermute(tail, axis, [(i, (i + 1) % count) for i in range(ends)]),
                cells,
                lax.ppermute(head, axis, [((i + 1) % count, i) for i in range(ends)]),
            ],
            axis=dim,
        )
    return cells


def copy_for_each(shard, axis):
    copies = jnp.broadcast_to(shard, (lax.axis_size(axis), *shard.shape))
    return lax.all_to_all(copies, axis, split_axis=0, concat_axis=0, tiled=True)


def taken_together(shard, axis):
    return copy_for_each(shard, axis).sum(axis=0)


def packed_total(arrays, axis):
    vector, at, finished = (jnp.concatenate([a.reshape(-1) for a in arrays]), 0, [])
    so_far = taken_together(vector, axis)
    for a in arrays:
        finished.append(so_far[at : at + a.size].reshape(a.shape))
        at += a.size
    return tuple(finished)


def shifts(frequency):
    angles = frequency.astype(jnp.float32) * (2.0 * math.pi / L)
    decay_rate = wrap_factor ** (1.0 / L)
    shift_re = (1.0 - decay_rate * jnp.cos(angles)) / step_size
    shift_im = decay_rate * jnp.sin(angles) / step_size
    return (shift_re, shift_im)


def near_sum(padded):
    interior = padded[..., 1:-1, :, :]
    widths = [(0, 0)] * (interior.ndim - 2) + [(1, 1), (1, 1)]
    padded_xy = jnp.pad(interior, widths)
    summed = padded[..., 2:, :, :] + padded[..., :-2, :, :]
    summed = summed + padded_xy[..., 2:, 1:-1] + padded_xy[..., :-2, 1:-1]
    summed = summed + padded_xy[..., 1:-1, 2:] + padded_xy[..., 1:-1, :-2]
    return summed


def advance(carried, dir_re, dir_im, img_re, img_im, coef_re, coef_im):
    sol_re, sol_im, res_re, res_im = carried
    sol_re = sol_re + coef_re * dir_re - coef_im * dir_im
    sol_im = sol_im + coef_re * dir_im + coef_im * dir_re
    res_re = res_re - (coef_re * img_re - coef_im * img_im)
    res_im = res_im - (coef_re * img_im + coef_im * img_re)
    return (sol_re, sol_im, res_re, res_im)


def solve_together(spectrum, absorption, frequencies, step_counts, longest):
    shift_re, shift_im = shifts(frequencies)
    shift_re = shift_re[:, None, None, None]
    shift_im = shift_im[:, None, None, None]
    diag_re = shift_re + 6.0 + absorption[None]
    magnitude = diag_re * diag_re + shift_im * shift_im
    inv_re = diag_re / magnitude
    inv_im = -shift_im / magnitude

    def iterate(iteration, carried):
        res_re, res_im = (carried[2], carried[3])
        dir_re = inv_re * res_re - inv_im * res_im
        dir_im = inv_re * res_im + inv_im * res_re
        padded = with_halo(jnp.stack([dir_re, dir_im], axis=1), ((SPACE, 2),), 1)
        nearby = near_sum(padded)
        img_re = diag_re * dir_re - shift_im * dir_im - nearby[:, 0]
        img_im = diag_re * dir_im + shift_im * dir_re - nearby[:, 1]
        totals = packed_total(
            (
                jnp.sum(img_re * res_re + img_im * res_im, axis=(1, 2, 3)),
                jnp.sum(img_re * res_im - img_im * res_re, axis=(1, 2, 3)),
                jnp.sum(img_re * img_re + img_im * img_im, axis=(1, 2, 3)),
            ),
            SPACE,
        )
        active = iteration < step_counts
        denominator = totals[2] + norm_floor
        coef_re = jnp.where(active, totals[0] / denominator, 0.0)[:, None, None, None]
        coef_im = jnp.where(active, totals[1] / denominator, 0.0)[:, None, None, None]
        return advance(carried, dir_re, dir_im, img_re, img_im, coef_re, coef_im)

    blank = jnp.zeros_like(spectrum[:, 0])
    finished = lax.fori_loop(0, longest, iterate, (blank, blank, spectrum[:, 0], spectrum[:, 1]))
    return jnp.stack([finished[0], finished[1]], axis=1)


def slot_order():
    return jnp.arange(L, dtype=jnp.int32)


def phase_table(left, right):
    return (left[:, None] * right[None, :] % L).astype(jnp.float32) * (2.0 * math.pi / L)


def stepwise(residual, absorption, counts):
    per_device = residual.shape[0]
    decay_rate = wrap_factor ** (1.0 / L)
    first_step = lax.axis_index(TM) * per_device
    times_here = first_step + jnp.arange(per_device, dtype=jnp.int32)
    scaled = residual * jnp.power(decay_rate, times_here.astype(jnp.float32))[:, None, None, None]
    slot_freqs = slot_order()
    own_freqs = lax.dynamic_slice_in_dim(slot_freqs, first_step, per_device)
    own_counts = counts[own_freqs]
    longest = jnp.max(counts)
    all_times = jnp.arange(L, dtype=jnp.int32)
    series = lax.all_to_all(scaled, TM, split_axis=2, concat_axis=0, tiled=True)
    phases = phase_table(slot_freqs, all_times)
    real_part = jnp.einsum("sn,nzxy->szxy", jnp.cos(phases), series, precision=highest)
    imag_part = -jnp.einsum("sn,nzxy->szxy", jnp.sin(phases), series, precision=highest)
    spectrum = lax.all_to_all(
        jnp.stack([real_part, imag_part], axis=1), TM, split_axis=0, concat_axis=3, tiled=True
    )
    solved = solve_together(spectrum, absorption, own_freqs, own_counts, longest)
    gathered = lax.all_to_all(solved, TM, split_axis=3, concat_axis=0, tiled=True)
    phases = phase_table(all_times, slot_freqs)
    values = jnp.einsum("ns,szxy->nzxy", jnp.cos(phases), gathered[:, 0], precision=highest)
    values = values - jnp.einsum(
        "ns,szxy->nzxy", jnp.sin(phases), gathered[:, 1], precision=highest
    )
    weight = jnp.power(decay_rate, -all_times.astype(jnp.float32)) / L
    values = values * weight[:, None, None, None]
    return lax.all_to_all(values, TM, split_axis=0, concat_axis=2, tiled=True)


def real_transform(x):
    n = len(x)
    if n == 2:
        return [(x[0] + x[1], None), (x[0] - x[1], None)]
    even, odd = real_transform(x[0::2]), real_transform(x[1::2])
    out = [None] * (n // 2 + 1)
    out[0] = (even[0][0] + odd[0][0], None)
    out[n // 2] = (even[0][0] - odd[0][0], None)
    out[n // 4] = (even[n // 4][0], -odd[n // 4][0])
    for k in range(1, n // 4):
        cos, sin = math.cos(2 * math.pi * k / n), math.sin(2 * math.pi * k / n)
        (er, ei), (cr, ci) = even[k], odd[k]
        tr, ti = cos * cr + sin * ci, cos * ci - sin * cr
        out[k] = (er + tr, ei + ti)
        out[n // 2 - k] = (er - tr, ti - ei)
    return out


def real_inverse(spectrum):
    n = 2 * (len(spectrum) - 1)
    first, last = spectrum[0][0], spectrum[n // 2][0]
    if n == 2:
        return [first + last, first - last]
    even, odd = [None] * (n // 4 + 1), [None] * (n // 4 + 1)
    even[0], odd[0] = (first + last, None), (first - last, None)
    mid_re, mid_im = spectrum[n // 4]
    even[n // 4], odd[n // 4] = (mid_re + mid_re, None), (-(mid_im + mid_im), None)
    for k in range(1, n // 4):
        cos, sin = math.cos(2 * math.pi * k / n), math.sin(2 * math.pi * k / n)
        (ar, ai), (br, bi) = spectrum[k], spectrum[n // 2 - k]
        even[k] = (ar + br, ai - bi)
        tr, ti = ar - br, ai + bi
        odd[k] = (cos * tr - sin * ti, cos * ti + sin * tr)
    halves = real_inverse(even), real_inverse(odd)
    return [halves[i % 2][i // 2] for i in range(n)]


def forward_kernel(x_ref, out_ref):
    for zz in range(2):
        spectrum = real_transform([x_ref[n, zz] * decay**n for n in range(L)])
        out_ref[0, 0, zz] = spectrum[0][0]
        out_ref[0, 1, zz] = spectrum[PAIRS][0]
        for k in range(1, PAIRS):
            out_ref[k, 0, zz] = spectrum[k][0]
            out_ref[k, 1, zz] = spectrum[k][1]


def inverse_kernel(s_ref, out_ref):
    for zz in range(2):
        ends = [s_ref[0, part, zz] for part in range(2)]
        spectrum = [(ends[0] + ends[0], None)]
        spectrum += [(s_ref[k, 0, zz], s_ref[k, 1, zz]) for k in range(1, PAIRS)]
        spectrum += [(ends[1] + ends[1], None)]
        values = real_inverse(spectrum)
        for n in range(L):
            out_ref[n, zz] = values[n] * (decay ** (-n) / (2 * L))


same = [(i, j) for i in range(STEPS + 1) for j in range(i, STEPS + 1)]
cross = [(i, j) for i in range(STEPS + 1) for j in range(i + 1, STEPS + 1)]
entry = {(kind, i, j): None for kind, ij in (("re", same), ("im", same), ("x", cross)) for i, j in ij}
for at, name in enumerate(entry):
    entry[name] = at


def tree_sum(terms):
    while len(terms) > 1:
        terms = [sum(terms[i : i + 2][1:], terms[i]) for i in range(0, len(terms), 2)]
    return terms[0]


def basis_kernel(at_ref, shift_ref, own_ref, left_ref, right_ref, abs_ref, v_ref, inv_ref, gram_ref, u, edge, edge_inv, last, sums):
    slot, z = at_ref[0], at_ref[1]
    shift_a, shift_b, shift_im = (shift_ref[slot, i] for i in range(3))
    lanes = lax.broadcasted_iota(jnp.int32, (8, 128), 1)
    first_lane, last_lane = lanes == 0, lanes == 127
    blank = jnp.zeros((8, 128), jnp.float32)

    for part in range(2):
        for row in range(0, 48, 8):
            u[part, 0, pl.ds(row, 8), :] = blank
            u[part, NZ + 1, pl.ds(row, 8), :] = blank

    def prepare(sp, _):
        for part in range(2):
            for zz in range(2):
                u[part, 2 * sp + zz + 1, pl.ds(0, 8), :] = blank
                u[part, 2 * sp + zz + 1, pl.ds(40, 8), :] = blank
        for tile in range(4):
            inside = True
            if tile == 0:
                inside = z > 0
            if tile == 3:
                inside = z < lax.axis_size("z") - 1
            for zz in range(2):
                base = abs_ref[tile // 2, sp, zz, tile % 2]
                da, db = (shift_a + 6.0) + base, (shift_b + 6.0) + base
                ra, rb = 1.0 / (da * da + shift_im * shift_im), 1.0 / (db * db + shift_im * shift_im)
                found = (da * ra, db * rb, -shift_im * ra)
                for i in range(3):
                    if tile in (1, 2):
                        inv_ref[i, tile - 1, sp, zz] = found[i]
                    else:
                        edge_inv[i, tile // 3, sp, zz] = jnp.where(inside, found[i], 0.0)
        return 0

    lax.fori_loop(0, NZ // 2, prepare, 0)

    for j in range(STEPS):
        def scaled(sp, _, j=j):
            for tile in range(4):
                for zz in range(2):
                    if tile in (1, 2):
                        a, b, c = (inv_ref[i, tile - 1, sp, zz] for i in range(3))
                        re, im = ((own_ref[tile - 1, sp, part, zz] if j == 0 else v_ref[j - 1, part, tile - 1, sp, zz]) for part in range(2))
                    else:
                        a, b, c = (edge_inv[i, tile // 3, sp, zz] for i in range(3))
                        side = (left_ref, None, None, right_ref)[tile]
                        re, im = ((side[sp, part, zz] if j == 0 else edge[part, tile // 3, sp, zz]) for part in range(2))
                    u[0, 2 * sp + zz + 1, pl.ds(8 + 8 * tile, 8), :] = a * re - c * im
                    u[1, 2 * sp + zz + 1, pl.ds(8 + 8 * tile, 8), :] = b * im + c * re
            return 0

        lax.fori_loop(0, NZ // 2, scaled, 0)

        def spread(sp, _, j=j):
            for tile in range(4) if j < STEPS - 1 else (1, 2):
                for zz in range(2):
                    for part in range(2):
                        layer, row = 2 * sp + zz + 1, 8 + 8 * tile
                        here = u[part, layer, pl.ds(row, 8), :]
                        total = u[part, layer - 1, pl.ds(row, 8), :] + u[part, layer + 1, pl.ds(row, 8), :]
                        total = total + (u[part, layer, pl.ds(row - 1, 8), :] + u[part, layer, pl.ds(row + 1, 8), :])
                        total = total + (
                            jnp.where(first_lane, 0.0, pltpu.roll(here, 1, 1))
                            + jnp.where(last_lane, 0.0, pltpu.roll(here, 127, 1))
                        )
                        if tile in (1, 2):
                            if j < STEPS - 1:
                                v_ref[j, part, tile - 1, sp, zz] = total
                            else:
                                last[part, tile - 1, sp, zz] = total
                        else:
                            edge[part, tile // 3, sp, zz] = total
            return 0

        lax.fori_loop(0, NZ // 2, spread, 0)

    def vector(j, part, side, sp, zz):
        if j == 0:
            return own_ref[side, sp, part, zz]
        if j == STEPS:
            return last[part, side, sp, zz]
        return v_ref[j - 1, part, side, sp, zz]

    for i in range(STEPS + 1):
        names = [name for name in entry if name[1] == i]

        def inner(sp, totals, names=names, i=i):
            places = [(side, zz) for side in range(2) for zz in range(2)]
            left = [[vector(i, part, side, sp, zz) for part in range(2)] for side, zz in places]
            out = []
            for j in range(i, STEPS + 1):
                right = left if j == i else [[vector(j, part, side, sp, zz) for part in range(2)] for side, zz in places]
                pairs = list(zip(left, right))
                out.append(("re", i, j, tree_sum([a[0] * b[0] for a, b in pairs])))
                out.append(("im", i, j, tree_sum([a[1] * b[1] for a, b in pairs])))
                if j > i:
                    out.append(("x", i, j, tree_sum([a[0] * b[1] - a[1] * b[0] for a, b in pairs])))
            found = {o[:3]: o[3] for o in out}
            return tuple(t + found[name] for t, name in zip(totals, names))

        def outer(group, totals, names=names, inner=inner):
            part_totals = tuple(blank for _ in names)
            part_totals = lax.fori_loop(group * 4, group * 4 + 4, inner, part_totals)
            return tuple(a + b for a, b in zip(totals, part_totals))

        totals = lax.fori_loop(0, 4, outer, tuple(blank for _ in names))
        for name, total in zip(names, totals):
            sums[entry[name]] = total
    for spare in range(len(entry), sums.shape[0]):
        sums[spare] = blank

    rows = jnp.sum(sums[...], axis=1)
    column = jnp.sum(rows, axis=1, keepdims=True)
    where = lax.broadcasted_iota(jnp.int32, rows.shape, 0) == lax.broadcasted_iota(jnp.int32, rows.shape, 1)
    packed = jnp.sum(jnp.where(where, column, 0.0), axis=0, keepdims=True)
    gram_ref[...] = jnp.broadcast_to(packed[None], gram_ref.shape)


def multiplied(a, b):
    return (a[0] * b[0] - a[1] * b[1], a[0] * b[1] + a[1] * b[0])


def combine_kernel(at_ref, count_ref, part_ref, own_ref, v_ref, inv_ref, out_ref):
    slot = at_ref[0]
    ends = slot == 0
    low = lax.broadcasted_iota(jnp.int32, (8, 128), 1) < 64
    row = tree_sum([part_ref[i] for i in range(part_ref.shape[0])])

    def spread(name):
        return jnp.broadcast_to(row[:, entry[name] : entry[name] + 1], (8, 128))

    gram = {}
    for i, j in same:
        re, im = spread(("re", i, j)), spread(("im", i, j))
        real = jnp.where(ends, jnp.where(low, re, im), re + im)
        imag = jnp.where(ends, 0.0, spread(("x", i, j))) if j > i else jnp.zeros_like(real)
        gram[i, j] = (real, imag)

    count_a = count_ref[slot]
    count_b = count_ref[jnp.where(ends, PAIRS, L - slot)]
    one, none = jnp.ones((8, 128), jnp.float32), jnp.zeros((8, 128), jnp.float32)
    poly, answer = [(one, none)], [(none, none) for _ in range(STEPS)]
    bound, doubt, scale = gram_rounding * gram[0, 0][0], none, None
    for m in range(STEPS):
        in_a, in_b = (jnp.where(m < count, one, none) for count in (count_a, count_b))
        weight = jnp.where(ends, jnp.where(low, in_a, in_b), in_a + in_b)
        g00, g01, g11 = gram[0, 0][0], gram[0, 1], gram[1, 1][0]
        denominator = (g00 - 2.0 * g01[0] + g11) + norm_floor
        inverse = 1.0 / denominator
        coef = ((g00 - g01[0]) * inverse, g01[1] * inverse)
        size = jnp.abs(coef[0]) + jnp.abs(coef[1])
        length = jnp.sqrt(jnp.maximum(g00, 0.0))
        if m == 0:
            scale = size * length
        step_doubt = bound * (2.0 + 4.0 * size) * jnp.abs(inverse) * length
        doubt = doubt + jnp.where(weight > 0.0, step_doubt, none)
        for j, p in enumerate(poly):
            term = multiplied(coef, p)
            answer[j] = (answer[j][0] + weight * term[0], answer[j][1] + weight * term[1])
        if m == STEPS - 1:
            break
        rest = (1.0 - coef[0], -coef[1])
        padded = [None] + poly + [None]
        following = []
        for j in range(len(poly) + 1):
            kept = multiplied(rest, poly[j]) if j < len(poly) else (none, none)
            moved = multiplied(coef, poly[j - 1]) if j > 0 else (none, none)
            following.append((kept[0] + moved[0], kept[1] + moved[1]))
        poly = following
        rr = rest[0] * rest[0] + rest[1] * rest[1]
        cc = coef[0] * coef[0] + coef[1] * coef[1]
        rc = multiplied((rest[0], -rest[1]), coef)
        cr = (rc[0], -rc[1])
        size_rest = jnp.abs(rest[0]) + jnp.abs(rest[1])
        bound = bound * (size + size_rest) * (size + size_rest)

        def at(i, j):
            return gram[i, j] if i <= j else (gram[j, i][0], -gram[j, i][1])

        shrunk = {}
        top = STEPS - m
        for i in range(top):
            for j in range(i, top):
                a, b, d = at(i, j), at(i, j + 1), at(i + 1, j + 1)
                if i == j:
                    ab = multiplied(rc, b)
                    shrunk[i, j] = (rr * a[0] + 2.0 * ab[0] + cc * d[0], none)
                else:
                    ab, ac = multiplied(rc, b), multiplied(cr, at(i + 1, j))
                    shrunk[i, j] = tuple(rr * a[x] + (ab[x] + ac[x]) + cc * d[x] for x in range(2))
        gram = shrunk

    trusted = doubt <= error_allowed * scale
    weights = []
    for re, im in answer:
        re = jnp.where(trusted, re, jnp.nan)
        weights.append(
            (
                jnp.broadcast_to(re[:, 0:1], (8, 128)),
                jnp.broadcast_to(re[:, 127:128], (8, 128)),
                jnp.broadcast_to(im[:, 0:1], (8, 128)),
            )
        )

    def finish(sp, _):
        for side in range(2):
            for zz in range(2):
                res, ims = [], []
                for j, (wa, wb, wi) in enumerate(weights):
                    re, im = ((own_ref[side, sp, part, zz] if j == 0 else v_ref[j - 1, part, side, sp, zz]) for part in range(2))
                    res.append(wa * re - wi * im)
                    ims.append(wb * im + wi * re)
                re, im = tree_sum(res), tree_sum(ims)
                a, b, c = (inv_ref[i, side, sp, zz] for i in range(3))
                out_ref[side, sp, 0, zz] = a * re - c * im
                out_ref[side, sp, 1, zz] = b * im + c * re
        return 0

    lax.fori_loop(0, NZ // 2, finish, 0)


def slot_shifts():
    table = np.zeros((PAIRS, 4), np.float32)
    for slot in range(PAIRS):
        angle = 2 * math.pi * slot / L
        table[slot, :2] = (1 - decay * math.cos(angle)) / step_size
        table[slot, 2] = decay * math.sin(angle) / step_size
    table[0, 1] = (1 + decay) / step_size
    return table


def exchanged(blocks, axes):
    return lax.all_to_all(blocks, axes, split_axis=0, concat_axis=0, tiled=True)


def f32(*shape):
    return jax.ShapeDtypeStruct(shape, jnp.float32)


VMEM = pl.BlockSpec(memory_space=pltpu.VMEM)
SMEM = pl.BlockSpec(memory_space=pltpu.SMEM)


def together(residual, absorption, counts):
    z = lax.axis_index("z")
    at = jnp.stack([lax.axis_index(SLOTS), z]).astype(jnp.int32)
    chips = lax.axis_size("z")

    tall = jnp.pad(absorption, ((0, 0), (8, 8), (0, 0)))
    first = 16 * z + 16 * lax.axis_index("core")
    near = lax.dynamic_slice_in_dim(tall, first, 16, axis=1).reshape(2, 2, 8, 128)
    near = exchanged(jnp.broadcast_to(near, (32, 2, 2, 8, 128)), SLOTS).reshape(2, 16, 2, 2, 8, 128)

    bands = residual.reshape(4, 2, 16, 8, 128).transpose(2, 0, 1, 3, 4)
    series = exchanged(bands, TM).reshape(L, 2, 8, 128)
    spectrum = pl.pallas_call(
        forward_kernel, out_shape=f32(PAIRS, 2, 2, 8, 128), in_specs=[VMEM], out_specs=VMEM, name="forward"
    )(series)
    own = exchanged(spectrum, SLOTS).reshape(2, 16, 2, 2, 8, 128)
    left = lax.ppermute(own[1], "z", [(i, i + 1) for i in range(chips - 1)])
    right = lax.ppermute(own[0], "z", [(i + 1, i) for i in range(chips - 1)])
    basis, inverses, partial = pl.pallas_call(
        basis_kernel,
        out_shape=(f32(STEPS - 1, 2, 2, 16, 2, 8, 128), f32(3, 2, 16, 2, 8, 128), f32(8, 8, 128)),
        in_specs=[SMEM, SMEM, VMEM, VMEM, VMEM, VMEM],
        out_specs=(VMEM, VMEM, VMEM),
        scratch_shapes=[
            pltpu.VMEM((2, NZ + 2, 48, 128), jnp.float32),
            pltpu.VMEM((2, 2, 16, 2, 8, 128), jnp.float32),
            pltpu.VMEM((3, 2, 16, 2, 8, 128), jnp.float32),
            pltpu.VMEM((2, 2, 16, 2, 8, 128), jnp.float32),
            pltpu.VMEM((80, 8, 128), jnp.float32),
        ],
        name="basis",
    )(at, jnp.asarray(slot_shifts()), own, left, right, near)
    partials = exchanged(partial, "z")
    solved = pl.pallas_call(
        combine_kernel,
        out_shape=f32(2, 16, 2, 2, 8, 128),
        in_specs=[SMEM, SMEM, VMEM, VMEM, VMEM, VMEM],
        out_specs=VMEM,
        name="combine",
    )(at, counts, partials, own, basis, inverses)
    gathered = exchanged(solved.reshape(32, 2, 2, 8, 128), SLOTS)
    values = pl.pallas_call(
        inverse_kernel, out_shape=f32(L, 2, 8, 128), in_specs=[VMEM], out_specs=VMEM, name="inverse"
    )(gathered)
    return exchanged(values.reshape(16, 4, 2, 8, 128), TM)


def body(residual, absorption, counts):
    bands = together(residual, absorption, counts)
    failed = jnp.isnan(bands[0, 0, 0, 0, 0])
    return lax.cond(
        failed,
        lambda r, a, c, b: stepwise(r, a, c),
        lambda r, a, c, b: b.transpose(1, 2, 0, 3, 4).reshape(r.shape),
        residual, absorption, counts, bands,
    )


def solution(mesh):
    chips, cores = mesh.shape["tm"] // 2, 2
    devices = mesh.devices.reshape(chips, cores, 4, 4)
    inner = Mesh(devices, ("z", "core", "y", "x"))
    in_specs = (P(TM, SPACE, None, None), P(SPACE, None, None), P())
    out_specs = P(TM, SPACE, None, None)
    return jax.shard_map(body, mesh=inner, in_specs=in_specs, out_specs=out_specs, check_vma=False)
```

```python
import math

import jax
import jax.numpy as jnp
import numpy as np
from jax import lax
from jax.experimental import pallas as pl
from jax.experimental.pallas import tpu as pltpu
from jax.sharding import Mesh
from jax.sharding import PartitionSpec as P

L = 64
STEPS = 6
NZ = 32
PAIRS = L // 2
TM = ("z", "core")
SPACE = ("y", "x")
SLOTS = ("core", "y", "x")

wrap_factor = 0.1
step_size = 1.0
norm_floor = 1e-06
highest = lax.Precision.HIGHEST
decay = wrap_factor ** (1.0 / L)

gram_rounding = 2.5e-7
error_allowed = 5e-4


def with_halo(cells, sides, width):
    for axis, dim in sides:
        count = lax.axis_size(axis)
        ends = count - 1
        head = lax.slice_in_dim(cells, 0, width, axis=dim)
        tail = lax.slice_in_dim(cells, cells.shape[dim] - width, cells.shape[dim], axis=dim)
        cells = jnp.concatenate(
            [
                lax.ppermute(tail, axis, [(i, (i + 1) % count) for i in range(ends)]),
                cells,
                lax.ppermute(head, axis, [((i + 1) % count, i) for i in range(ends)]),
            ],
            axis=dim,
        )
    return cells


def copy_for_each(shard, axis):
    copies = jnp.broadcast_to(shard, (lax.axis_size(axis), *shard.shape))
    return lax.all_to_all(copies, axis, split_axis=0, concat_axis=0, tiled=True)


def taken_together(shard, axis):
    return copy_for_each(shard, axis).sum(axis=0)


def packed_total(arrays, axis):
    vector, at, finished = (jnp.concatenate([a.reshape(-1) for a in arrays]), 0, [])
    so_far = taken_together(vector, axis)
    for a in arrays:
        finished.append(so_far[at : at + a.size].reshape(a.shape))
        at += a.size
    return tuple(finished)


def shifts(frequency):
    angles = frequency.astype(jnp.float32) * (2.0 * math.pi / L)
    decay_rate = wrap_factor ** (1.0 / L)
    shift_re = (1.0 - decay_rate * jnp.cos(angles)) / step_size
    shift_im = decay_rate * jnp.sin(angles) / step_size
    return (shift_re, shift_im)


def near_sum(padded):
    interior = padded[..., 1:-1, :, :]
    widths = [(0, 0)] * (interior.ndim - 2) + [(1, 1), (1, 1)]
    padded_xy = jnp.pad(interior, widths)
    summed = padded[..., 2:, :, :] + padded[..., :-2, :, :]
    summed = summed + padded_xy[..., 2:, 1:-1] + padded_xy[..., :-2, 1:-1]
    summed = summed + padded_xy[..., 1:-1, 2:] + padded_xy[..., 1:-1, :-2]
    return summed


def advance(carried, dir_re, dir_im, img_re, img_im, coef_re, coef_im):
    sol_re, sol_im, res_re, res_im = carried
    sol_re = sol_re + coef_re * dir_re - coef_im * dir_im
    sol_im = sol_im + coef_re * dir_im + coef_im * dir_re
    res_re = res_re - (coef_re * img_re - coef_im * img_im)
    res_im = res_im - (coef_re * img_im + coef_im * img_re)
    return (sol_re, sol_im, res_re, res_im)


def solve_together(spectrum, absorption, frequencies, step_counts, longest):
    shift_re, shift_im = shifts(frequencies)
    shift_re = shift_re[:, None, None, None]
    shift_im = shift_im[:, None, None, None]
    diag_re = shift_re + 6.0 + absorption[None]
    magnitude = diag_re * diag_re + shift_im * shift_im
    inv_re = diag_re / magnitude
    inv_im = -shift_im / magnitude

    def iterate(iteration, carried):
        res_re, res_im = (carried[2], carried[3])
        dir_re = inv_re * res_re - inv_im * res_im
        dir_im = inv_re * res_im + inv_im * res_re
        padded = with_halo(jnp.stack([dir_re, dir_im], axis=1), ((SPACE, 2),), 1)
        nearby = near_sum(padded)
        img_re = diag_re * dir_re - shift_im * dir_im - nearby[:, 0]
        img_im = diag_re * dir_im + shift_im * dir_re - nearby[:, 1]
        totals = packed_total(
            (
                jnp.sum(img_re * res_re + img_im * res_im, axis=(1, 2, 3)),
                jnp.sum(img_re * res_im - img_im * res_re, axis=(1, 2, 3)),
                jnp.sum(img_re * img_re + img_im * img_im, axis=(1, 2, 3)),
            ),
            SPACE,
        )
        active = iteration < step_counts
        denominator = totals[2] + norm_floor
        coef_re = jnp.where(active, totals[0] / denominator, 0.0)[:, None, None, None]
        coef_im = jnp.where(active, totals[1] / denominator, 0.0)[:, None, None, None]
        return advance(carried, dir_re, dir_im, img_re, img_im, coef_re, coef_im)

    blank = jnp.zeros_like(spectrum[:, 0])
    finished = lax.fori_loop(0, longest, iterate, (blank, blank, spectrum[:, 0], spectrum[:, 1]))
    return jnp.stack([finished[0], finished[1]], axis=1)


def slot_order():
    return jnp.arange(L, dtype=jnp.int32)


def phase_table(left, right):
    return (left[:, None] * right[None, :] % L).astype(jnp.float32) * (2.0 * math.pi / L)


def stepwise(residual, absorption, counts):
    per_device = residual.shape[0]
    decay_rate = wrap_factor ** (1.0 / L)
    first_step = lax.axis_index(TM) * per_device
    times_here = first_step + jnp.arange(per_device, dtype=jnp.int32)
    scaled = residual * jnp.power(decay_rate, times_here.astype(jnp.float32))[:, None, None, None]
    slot_freqs = slot_order()
    own_freqs = lax.dynamic_slice_in_dim(slot_freqs, first_step, per_device)
    own_counts = counts[own_freqs]
    longest = jnp.max(counts)
    all_times = jnp.arange(L, dtype=jnp.int32)
    series = lax.all_to_all(scaled, TM, split_axis=2, concat_axis=0, tiled=True)
    phases = phase_table(slot_freqs, all_times)
    real_part = jnp.einsum("sn,nzxy->szxy", jnp.cos(phases), series, precision=highest)
    imag_part = -jnp.einsum("sn,nzxy->szxy", jnp.sin(phases), series, precision=highest)
    spectrum = lax.all_to_all(
        jnp.stack([real_part, imag_part], axis=1), TM, split_axis=0, concat_axis=3, tiled=True
    )
    solved = solve_together(spectrum, absorption, own_freqs, own_counts, longest)
    gathered = lax.all_to_all(solved, TM, split_axis=3, concat_axis=0, tiled=True)
    phases = phase_table(all_times, slot_freqs)
    values = jnp.einsum("ns,szxy->nzxy", jnp.cos(phases), gathered[:, 0], precision=highest)
    values = values - jnp.einsum(
        "ns,szxy->nzxy", jnp.sin(phases), gathered[:, 1], precision=highest
    )
    weight = jnp.power(decay_rate, -all_times.astype(jnp.float32)) / L
    values = values * weight[:, None, None, None]
    return lax.all_to_all(values, TM, split_axis=0, concat_axis=2, tiled=True)


def real_transform(x):
    n = len(x)
    if n == 2:
        return [(x[0] + x[1], None), (x[0] - x[1], None)]
    even, odd = real_transform(x[0::2]), real_transform(x[1::2])
    out = [None] * (n // 2 + 1)
    out[0] = (even[0][0] + odd[0][0], None)
    out[n // 2] = (even[0][0] - odd[0][0], None)
    out[n // 4] = (even[n // 4][0], -odd[n // 4][0])
    for k in range(1, n // 4):
        cos, sin = math.cos(2 * math.pi * k / n), math.sin(2 * math.pi * k / n)
        (er, ei), (cr, ci) = even[k], odd[k]
        tr, ti = cos * cr + sin * ci, cos * ci - sin * cr
        out[k] = (er + tr, ei + ti)
        out[n // 2 - k] = (er - tr, ti - ei)
    return out


def real_inverse(spectrum):
    n = 2 * (len(spectrum) - 1)
    first, last = spectrum[0][0], spectrum[n // 2][0]
    if n == 2:
        return [first + last, first - last]
    even, odd = [None] * (n // 4 + 1), [None] * (n // 4 + 1)
    even[0], odd[0] = (first + last, None), (first - last, None)
    mid_re, mid_im = spectrum[n // 4]
    even[n // 4], odd[n // 4] = (mid_re + mid_re, None), (-(mid_im + mid_im), None)
    for k in range(1, n // 4):
        cos, sin = math.cos(2 * math.pi * k / n), math.sin(2 * math.pi * k / n)
        (ar, ai), (br, bi) = spectrum[k], spectrum[n // 2 - k]
        even[k] = (ar + br, ai - bi)
        tr, ti = ar - br, ai + bi
        odd[k] = (cos * tr - sin * ti, cos * ti + sin * tr)
    halves = real_inverse(even), real_inverse(odd)
    return [halves[i % 2][i // 2] for i in range(n)]


def forward_kernel(x_ref, after_ref, out_ref):
    del after_ref
    for zz in range(2):
        spectrum = real_transform([x_ref[n, zz] * decay**n for n in range(L)])
        out_ref[0, 0, zz] = spectrum[0][0]
        out_ref[0, 1, zz] = spectrum[PAIRS][0]
        for k in range(1, PAIRS):
            out_ref[k, 0, zz] = spectrum[k][0]
            out_ref[k, 1, zz] = spectrum[k][1]


def inverse_kernel(s_ref, out_ref, failed_ref):
    failed = jnp.zeros((8, 128), jnp.float32)
    for zz in range(2):
        ends = [s_ref[0, part, zz] for part in range(2)]
        spectrum = [(ends[0] + ends[0], None)]
        spectrum += [(s_ref[k, 0, zz], s_ref[k, 1, zz]) for k in range(1, PAIRS)]
        spectrum += [(ends[1] + ends[1], None)]
        values = real_inverse(spectrum)
        for n in range(L):
            out_ref[n, zz] = values[n] * (decay ** (-n) / (2 * L))
        failed = jnp.where(values[0] != values[0], 1.0, failed)
    failed_ref[0] = jnp.where(jnp.max(failed) > 0.0, 1, 0)


same = [(i, j) for i in range(STEPS + 1) for j in range(i, STEPS + 1)]
cross = [(i, j) for i in range(STEPS + 1) for j in range(i + 1, STEPS + 1)]
entry = {(kind, i, j): None for kind, ij in (("re", same), ("im", same), ("x", cross)) for i, j in ij}
for at, name in enumerate(entry):
    entry[name] = at


def tree_sum(terms):
    while len(terms) > 1:
        terms = [sum(terms[i : i + 2][1:], terms[i]) for i in range(0, len(terms), 2)]
    return terms[0]


def basis_kernel(shift_ref, own_ref, left_ref, right_ref, abs_ref, v_ref, inv_ref, gram_ref, u, edge, edge_inv, last, sums):
    slot, z = lax.axis_index(SLOTS), lax.axis_index("z")
    shift_a, shift_b, shift_im = (shift_ref[slot, i] for i in range(3))
    lanes = lax.broadcasted_iota(jnp.int32, (8, 128), 1)
    first_lane, last_lane = lanes == 0, lanes == 127
    blank = jnp.zeros((8, 128), jnp.float32)

    for part in range(2):
        for row in range(0, 48, 8):
            u[part, 0, pl.ds(row, 8), :] = blank
            u[part, NZ + 1, pl.ds(row, 8), :] = blank

    def prepare(sp, _):
        for part in range(2):
            for zz in range(2):
                u[part, 2 * sp + zz + 1, pl.ds(0, 8), :] = blank
                u[part, 2 * sp + zz + 1, pl.ds(40, 8), :] = blank
        for tile in range(4):
            inside = True
            if tile == 0:
                inside = z > 0
            if tile == 3:
                inside = z < lax.axis_size("z") - 1
            for zz in range(2):
                base = abs_ref[tile // 2, sp, zz, tile % 2]
                da, db = (shift_a + 6.0) + base, (shift_b + 6.0) + base
                ra, rb = 1.0 / (da * da + shift_im * shift_im), 1.0 / (db * db + shift_im * shift_im)
                found = (da * ra, db * rb, -shift_im * ra)
                for i in range(3):
                    if tile in (1, 2):
                        inv_ref[i, tile - 1, sp, zz] = found[i]
                    else:
                        edge_inv[i, tile // 3, sp, zz] = jnp.where(inside, found[i], 0.0)
        return 0

    lax.fori_loop(0, NZ // 2, prepare, 0, unroll=4)

    for j in range(STEPS):
        def scaled(sp, _, j=j):
            for tile in range(4):
                for zz in range(2):
                    if tile in (1, 2):
                        a, b, c = (inv_ref[i, tile - 1, sp, zz] for i in range(3))
                        re, im = ((own_ref[tile - 1, sp, part, zz] if j == 0 else v_ref[j - 1, part, tile - 1, sp, zz]) for part in range(2))
                    else:
                        a, b, c = (edge_inv[i, tile // 3, sp, zz] for i in range(3))
                        side = (left_ref, None, None, right_ref)[tile]
                        re, im = ((side[sp, part, zz] if j == 0 else edge[part, tile // 3, sp, zz]) for part in range(2))
                    u[0, 2 * sp + zz + 1, pl.ds(8 + 8 * tile, 8), :] = a * re - c * im
                    u[1, 2 * sp + zz + 1, pl.ds(8 + 8 * tile, 8), :] = b * im + c * re
            return 0

        lax.fori_loop(0, NZ // 2, scaled, 0, unroll=4)

        def spread(sp, _, j=j):
            for tile in range(4) if j < STEPS - 1 else (1, 2):
                for zz in range(2):
                    for part in range(2):
                        layer, row = 2 * sp + zz + 1, 8 + 8 * tile
                        here = u[part, layer, pl.ds(row, 8), :]
                        total = u[part, layer - 1, pl.ds(row, 8), :] + u[part, layer + 1, pl.ds(row, 8), :]
                        total = total + (u[part, layer, pl.ds(row - 1, 8), :] + u[part, layer, pl.ds(row + 1, 8), :])
                        total = total + (
                            jnp.where(first_lane, 0.0, pltpu.roll(here, 1, 1))
                            + jnp.where(last_lane, 0.0, pltpu.roll(here, 127, 1))
                        )
                        if tile in (1, 2):
                            if j < STEPS - 1:
                                v_ref[j, part, tile - 1, sp, zz] = total
                            else:
                                last[part, tile - 1, sp, zz] = total
                        else:
                            edge[part, tile // 3, sp, zz] = total
            return 0

        lax.fori_loop(0, NZ // 2, spread, 0, unroll=8)

    def vector(j, part, side, sp, zz):
        if j == 0:
            return own_ref[side, sp, part, zz]
        if j == STEPS:
            return last[part, side, sp, zz]
        return v_ref[j - 1, part, side, sp, zz]

    for i in range(STEPS + 1):
        names = [name for name in entry if name[1] == i]

        def inner(sp, totals, names=names, i=i):
            places = [(side, zz) for side in range(2) for zz in range(2)]
            left = [[vector(i, part, side, sp, zz) for part in range(2)] for side, zz in places]
            out = []
            for j in range(i, STEPS + 1):
                right = left if j == i else [[vector(j, part, side, sp, zz) for part in range(2)] for side, zz in places]
                pairs = list(zip(left, right))
                out.append(("re", i, j, tree_sum([a[0] * b[0] for a, b in pairs])))
                out.append(("im", i, j, tree_sum([a[1] * b[1] for a, b in pairs])))
                if j > i:
                    out.append(("x", i, j, tree_sum([a[0] * b[1] - a[1] * b[0] for a, b in pairs])))
            found = {o[:3]: o[3] for o in out}
            return tuple(t + found[name] for t, name in zip(totals, names))

        def outer(group, totals, names=names, inner=inner):
            part_totals = tuple(blank for _ in names)
            part_totals = lax.fori_loop(group * 4, group * 4 + 4, inner, part_totals)
            return tuple(a + b for a, b in zip(totals, part_totals))

        totals = lax.fori_loop(0, 4, outer, tuple(blank for _ in names))
        for name, total in zip(names, totals):
            sums[entry[name]] = total
    for spare in range(len(entry), sums.shape[0]):
        sums[spare] = blank

    rows = jnp.sum(sums[...], axis=1)
    column = jnp.sum(rows, axis=1, keepdims=True)
    where = lax.broadcasted_iota(jnp.int32, rows.shape, 0) == lax.broadcasted_iota(jnp.int32, rows.shape, 1)
    packed = jnp.sum(jnp.where(where, column, 0.0), axis=0, keepdims=True)
    gram_ref[...] = jnp.broadcast_to(packed[None], gram_ref.shape)


def multiplied(a, b):
    return (a[0] * b[0] - a[1] * b[1], a[0] * b[1] + a[1] * b[0])


def combine_kernel(count_ref, part_ref, own_ref, v_ref, inv_ref, out_ref):
    slot = lax.axis_index(SLOTS)
    ends = slot == 0
    low = lax.broadcasted_iota(jnp.int32, (8, 128), 1) < 64
    row = tree_sum([part_ref[i] for i in range(part_ref.shape[0])])

    def spread(name):
        return jnp.broadcast_to(row[:, entry[name] : entry[name] + 1], (8, 128))

    gram = {}
    for i, j in same:
        re, im = spread(("re", i, j)), spread(("im", i, j))
        real = jnp.where(ends, jnp.where(low, re, im), re + im)
        imag = jnp.where(ends, 0.0, spread(("x", i, j))) if j > i else jnp.zeros_like(real)
        gram[i, j] = (real, imag)

    count_a = count_ref[slot]
    count_b = count_ref[jnp.where(ends, PAIRS, L - slot)]
    one, none = jnp.ones((8, 128), jnp.float32), jnp.zeros((8, 128), jnp.float32)
    poly, answer = [(one, none)], [(none, none) for _ in range(STEPS)]
    bound, doubt, scale = gram_rounding * gram[0, 0][0], none, None
    for m in range(STEPS):
        in_a, in_b = (jnp.where(m < count, one, none) for count in (count_a, count_b))
        weight = jnp.where(ends, jnp.where(low, in_a, in_b), in_a + in_b)
        g00, g01, g11 = gram[0, 0][0], gram[0, 1], gram[1, 1][0]
        denominator = (g00 - 2.0 * g01[0] + g11) + norm_floor
        inverse = 1.0 / denominator
        coef = ((g00 - g01[0]) * inverse, g01[1] * inverse)
        size = jnp.abs(coef[0]) + jnp.abs(coef[1])
        length = jnp.sqrt(jnp.maximum(g00, 0.0))
        if m == 0:
            scale = size * length
        step_doubt = bound * (2.0 + 4.0 * size) * jnp.abs(inverse) * length
        doubt = doubt + jnp.where(weight > 0.0, step_doubt, none)
        for j, p in enumerate(poly):
            term = multiplied(coef, p)
            answer[j] = (answer[j][0] + weight * term[0], answer[j][1] + weight * term[1])
        if m == STEPS - 1:
            break
        rest = (1.0 - coef[0], -coef[1])
        padded = [None] + poly + [None]
        following = []
        for j in range(len(poly) + 1):
            kept = multiplied(rest, poly[j]) if j < len(poly) else (none, none)
            moved = multiplied(coef, poly[j - 1]) if j > 0 else (none, none)
            following.append((kept[0] + moved[0], kept[1] + moved[1]))
        poly = following
        rr = rest[0] * rest[0] + rest[1] * rest[1]
        cc = coef[0] * coef[0] + coef[1] * coef[1]
        rc = multiplied((rest[0], -rest[1]), coef)
        cr = (rc[0], -rc[1])
        size_rest = jnp.abs(rest[0]) + jnp.abs(rest[1])
        bound = bound * (size + size_rest) * (size + size_rest)

        def at(i, j):
            return gram[i, j] if i <= j else (gram[j, i][0], -gram[j, i][1])

        shrunk = {}
        top = STEPS - m
        for i in range(top):
            for j in range(i, top):
                a, b, d = at(i, j), at(i, j + 1), at(i + 1, j + 1)
                if i == j:
                    ab = multiplied(rc, b)
                    shrunk[i, j] = (rr * a[0] + 2.0 * ab[0] + cc * d[0], none)
                else:
                    ab, ac = multiplied(rc, b), multiplied(cr, at(i + 1, j))
                    shrunk[i, j] = tuple(rr * a[x] + (ab[x] + ac[x]) + cc * d[x] for x in range(2))
        gram = shrunk

    trusted = doubt <= error_allowed * scale
    weights = []
    for re, im in answer:
        re = jnp.where(trusted, re, jnp.nan)
        weights.append(
            (
                jnp.broadcast_to(re[:, 0:1], (8, 128)),
                jnp.broadcast_to(re[:, 127:128], (8, 128)),
                jnp.broadcast_to(im[:, 0:1], (8, 128)),
            )
        )

    def finish(sp, _):
        for side in range(2):
            for zz in range(2):
                res, ims = [], []
                for j, (wa, wb, wi) in enumerate(weights):
                    re, im = ((own_ref[side, sp, part, zz] if j == 0 else v_ref[j - 1, part, side, sp, zz]) for part in range(2))
                    res.append(wa * re - wi * im)
                    ims.append(wb * im + wi * re)
                re, im = tree_sum(res), tree_sum(ims)
                a, b, c = (inv_ref[i, side, sp, zz] for i in range(3))
                out_ref[side, sp, 0, zz] = a * re - c * im
                out_ref[side, sp, 1, zz] = b * im + c * re
        return 0

    lax.fori_loop(0, NZ // 2, finish, 0, unroll=2)


def slot_shifts():
    table = np.zeros((PAIRS, 4), np.float32)
    for slot in range(PAIRS):
        angle = 2 * math.pi * slot / L
        table[slot, :2] = (1 - decay * math.cos(angle)) / step_size
        table[slot, 2] = decay * math.sin(angle) / step_size
    table[0, 1] = (1 + decay) / step_size
    return table


def exchanged(blocks, axes):
    return lax.all_to_all(blocks, axes, split_axis=0, concat_axis=0, tiled=True)


VMEM = pl.BlockSpec(memory_space=pltpu.VMEM)
SMEM = pl.BlockSpec(memory_space=pltpu.SMEM)


def f32(*shape):
    return pltpu.VMEM(shape, jnp.float32)


def held(x):
    return pltpu.with_memory_space_constraint(x, pltpu.MemorySpace.VMEM)


def room(mebibytes):
    return pltpu.CompilerParams(vmem_limit_bytes=mebibytes * 2**20)


def together(residual, absorption, counts):
    z, chips = lax.axis_index("z"), lax.axis_size("z")

    tall = jnp.pad(absorption, ((0, 0), (8, 8), (0, 0)))
    first = 16 * z + 16 * lax.axis_index("core")
    near = lax.dynamic_slice_in_dim(tall, first, 16, axis=1).reshape(2, 2, 8, 128)
    near = exchanged(jnp.broadcast_to(near, (32, 2, 2, 8, 128)), SLOTS)

    bands = residual.reshape(4, 2, 16, 8, 128).transpose(2, 0, 1, 3, 4)
    series = exchanged(bands, TM).reshape(L, 2, 8, 128)
    spectrum = pl.pallas_call(
        forward_kernel,
        out_shape=f32(PAIRS, 2, 2, 8, 128),
        in_specs=[VMEM, VMEM],
        out_specs=VMEM,
        compiler_params=room(4),
        name="forward",
    )(held(series), held(near))
    own = exchanged(spectrum, SLOTS).reshape(2, 16, 2, 2, 8, 128)
    left = lax.ppermute(own[1], "z", [(i, i + 1) for i in range(chips - 1)])
    right = lax.ppermute(own[0], "z", [(i + 1, i) for i in range(chips - 1)])
    basis, inverses, partial = pl.pallas_call(
        basis_kernel,
        out_shape=(f32(STEPS - 1, 2, 2, 16, 2, 8, 128), f32(3, 2, 16, 2, 8, 128), f32(8, 8, 128)),
        in_specs=[SMEM, VMEM, VMEM, VMEM, VMEM],
        out_specs=(VMEM, VMEM, VMEM),
        scratch_shapes=[
            pltpu.VMEM((2, NZ + 2, 48, 128), jnp.float32),
            pltpu.VMEM((2, 2, 16, 2, 8, 128), jnp.float32),
            pltpu.VMEM((3, 2, 16, 2, 8, 128), jnp.float32),
            pltpu.VMEM((2, 2, 16, 2, 8, 128), jnp.float32),
            pltpu.VMEM((80, 8, 128), jnp.float32),
        ],
        compiler_params=room(10),
        name="basis",
    )(jnp.asarray(slot_shifts()), held(own), held(left), held(right), held(near.reshape(2, 16, 2, 2, 8, 128)))
    partials = exchanged(partial, "z")
    solved = pl.pallas_call(
        combine_kernel,
        out_shape=f32(2, 16, 2, 2, 8, 128),
        in_specs=[SMEM, VMEM, VMEM, VMEM, VMEM],
        out_specs=VMEM,
        compiler_params=room(6),
        name="combine",
    )(counts, held(partials), held(own), held(basis), held(inverses))
    gathered = exchanged(solved.reshape(32, 2, 2, 8, 128), SLOTS)
    values, failed = pl.pallas_call(
        inverse_kernel,
        out_shape=(f32(L, 2, 8, 128), jax.ShapeDtypeStruct((1,), jnp.int32)),
        in_specs=[VMEM],
        out_specs=(VMEM, SMEM),
        compiler_params=room(4),
        name="inverse",
    )(held(gathered))
    return exchanged(values.reshape(16, 4, 2, 8, 128), TM), failed


def body(residual, absorption, counts):
    bands, failed = together(residual, absorption, counts)
    return lax.cond(
        failed[0] > 0,
        lambda r, a, c, b: stepwise(r, a, c),
        lambda r, a, c, b: b.transpose(1, 2, 0, 3, 4).reshape(r.shape),
        residual, absorption, counts, bands,
    )


def solution(mesh):
    chips, cores = mesh.shape["tm"] // 2, 2
    devices = mesh.devices.reshape(chips, cores, 4, 4)
    inner = Mesh(devices, ("z", "core", "y", "x"))
    in_specs = (P(TM, SPACE, None, None), P(SPACE, None, None), P())
    out_specs = P(TM, SPACE, None, None)
    return jax.shard_map(body, mesh=inner, in_specs=in_specs, out_specs=out_specs, check_vma=False)
```

```python
import math

import jax
import jax.numpy as jnp
import numpy as np
from jax import lax
from jax.experimental import pallas as pl
from jax.experimental.pallas import tpu as pltpu
from jax.sharding import Mesh
from jax.sharding import PartitionSpec as P

L = 64
STEPS = 6
HALO = 6
NX = 128
NZ = 32
PAIRS = L // 2
TM = ("z", "core")
SPACE = ("y", "x")
SLOTS = ("core", "y", "x")

wrap_factor = 0.1
step_size = 1.0
norm_floor = 1e-06
highest = lax.Precision.HIGHEST
decay = wrap_factor ** (1.0 / L)

gram_rounding = 2.5e-7
error_allowed = 5e-4


def with_halo(cells, sides, width):
    for axis, dim in sides:
        count = lax.axis_size(axis)
        ends = count - 1
        head = lax.slice_in_dim(cells, 0, width, axis=dim)
        tail = lax.slice_in_dim(cells, cells.shape[dim] - width, cells.shape[dim], axis=dim)
        cells = jnp.concatenate(
            [
                lax.ppermute(tail, axis, [(i, (i + 1) % count) for i in range(ends)]),
                cells,
                lax.ppermute(head, axis, [((i + 1) % count, i) for i in range(ends)]),
            ],
            axis=dim,
        )
    return cells


def copy_for_each(shard, axis):
    copies = jnp.broadcast_to(shard, (lax.axis_size(axis), *shard.shape))
    return lax.all_to_all(copies, axis, split_axis=0, concat_axis=0, tiled=True)


def taken_together(shard, axis):
    return copy_for_each(shard, axis).sum(axis=0)


def packed_total(arrays, axis):
    vector, at, finished = (jnp.concatenate([a.reshape(-1) for a in arrays]), 0, [])
    so_far = taken_together(vector, axis)
    for a in arrays:
        finished.append(so_far[at : at + a.size].reshape(a.shape))
        at += a.size
    return tuple(finished)


def shifts(frequency):
    angles = frequency.astype(jnp.float32) * (2.0 * math.pi / L)
    decay_rate = wrap_factor ** (1.0 / L)
    shift_re = (1.0 - decay_rate * jnp.cos(angles)) / step_size
    shift_im = decay_rate * jnp.sin(angles) / step_size
    return (shift_re, shift_im)


def near_sum(padded):
    interior = padded[..., 1:-1, :, :]
    widths = [(0, 0)] * (interior.ndim - 2) + [(1, 1), (1, 1)]
    padded_xy = jnp.pad(interior, widths)
    summed = padded[..., 2:, :, :] + padded[..., :-2, :, :]
    summed = summed + padded_xy[..., 2:, 1:-1] + padded_xy[..., :-2, 1:-1]
    summed = summed + padded_xy[..., 1:-1, 2:] + padded_xy[..., 1:-1, :-2]
    return summed


def advance(carried, dir_re, dir_im, img_re, img_im, coef_re, coef_im):
    sol_re, sol_im, res_re, res_im = carried
    sol_re = sol_re + coef_re * dir_re - coef_im * dir_im
    sol_im = sol_im + coef_re * dir_im + coef_im * dir_re
    res_re = res_re - (coef_re * img_re - coef_im * img_im)
    res_im = res_im - (coef_re * img_im + coef_im * img_re)
    return (sol_re, sol_im, res_re, res_im)


def solve_together(spectrum, absorption, frequencies, step_counts, longest):
    shift_re, shift_im = shifts(frequencies)
    shift_re = shift_re[:, None, None, None]
    shift_im = shift_im[:, None, None, None]
    diag_re = shift_re + 6.0 + absorption[None]
    magnitude = diag_re * diag_re + shift_im * shift_im
    inv_re = diag_re / magnitude
    inv_im = -shift_im / magnitude

    def iterate(iteration, carried):
        res_re, res_im = (carried[2], carried[3])
        dir_re = inv_re * res_re - inv_im * res_im
        dir_im = inv_re * res_im + inv_im * res_re
        padded = with_halo(jnp.stack([dir_re, dir_im], axis=1), ((SPACE, 2),), 1)
        nearby = near_sum(padded)
        img_re = diag_re * dir_re - shift_im * dir_im - nearby[:, 0]
        img_im = diag_re * dir_im + shift_im * dir_re - nearby[:, 1]
        totals = packed_total(
            (
                jnp.sum(img_re * res_re + img_im * res_im, axis=(1, 2, 3)),
                jnp.sum(img_re * res_im - img_im * res_re, axis=(1, 2, 3)),
                jnp.sum(img_re * img_re + img_im * img_im, axis=(1, 2, 3)),
            ),
            SPACE,
        )
        active = iteration < step_counts
        denominator = totals[2] + norm_floor
        coef_re = jnp.where(active, totals[0] / denominator, 0.0)[:, None, None, None]
        coef_im = jnp.where(active, totals[1] / denominator, 0.0)[:, None, None, None]
        return advance(carried, dir_re, dir_im, img_re, img_im, coef_re, coef_im)

    blank = jnp.zeros_like(spectrum[:, 0])
    finished = lax.fori_loop(0, longest, iterate, (blank, blank, spectrum[:, 0], spectrum[:, 1]))
    return jnp.stack([finished[0], finished[1]], axis=1)


def slot_order():
    return jnp.arange(L, dtype=jnp.int32)


def phase_table(left, right):
    return (left[:, None] * right[None, :] % L).astype(jnp.float32) * (2.0 * math.pi / L)


def stepwise(residual, absorption, counts):
    per_device = residual.shape[0]
    decay_rate = wrap_factor ** (1.0 / L)
    first_step = lax.axis_index(TM) * per_device
    times_here = first_step + jnp.arange(per_device, dtype=jnp.int32)
    scaled = residual * jnp.power(decay_rate, times_here.astype(jnp.float32))[:, None, None, None]
    slot_freqs = slot_order()
    own_freqs = lax.dynamic_slice_in_dim(slot_freqs, first_step, per_device)
    own_counts = counts[own_freqs]
    longest = jnp.max(counts)
    all_times = jnp.arange(L, dtype=jnp.int32)
    series = lax.all_to_all(scaled, TM, split_axis=2, concat_axis=0, tiled=True)
    phases = phase_table(slot_freqs, all_times)
    real_part = jnp.einsum("sn,nzxy->szxy", jnp.cos(phases), series, precision=highest)
    imag_part = -jnp.einsum("sn,nzxy->szxy", jnp.sin(phases), series, precision=highest)
    spectrum = lax.all_to_all(
        jnp.stack([real_part, imag_part], axis=1), TM, split_axis=0, concat_axis=3, tiled=True
    )
    solved = solve_together(spectrum, absorption, own_freqs, own_counts, longest)
    gathered = lax.all_to_all(solved, TM, split_axis=3, concat_axis=0, tiled=True)
    phases = phase_table(all_times, slot_freqs)
    values = jnp.einsum("ns,szxy->nzxy", jnp.cos(phases), gathered[:, 0], precision=highest)
    values = values - jnp.einsum(
        "ns,szxy->nzxy", jnp.sin(phases), gathered[:, 1], precision=highest
    )
    weight = jnp.power(decay_rate, -all_times.astype(jnp.float32)) / L
    values = values * weight[:, None, None, None]
    return lax.all_to_all(values, TM, split_axis=0, concat_axis=2, tiled=True)


def real_transform(x):
    n = len(x)
    if n == 2:
        return [(x[0] + x[1], None), (x[0] - x[1], None)]
    even, odd = real_transform(x[0::2]), real_transform(x[1::2])
    out = [None] * (n // 2 + 1)
    out[0] = (even[0][0] + odd[0][0], None)
    out[n // 2] = (even[0][0] - odd[0][0], None)
    out[n // 4] = (even[n // 4][0], -odd[n // 4][0])
    for k in range(1, n // 4):
        cos, sin = math.cos(2 * math.pi * k / n), math.sin(2 * math.pi * k / n)
        (er, ei), (cr, ci) = even[k], odd[k]
        tr, ti = cos * cr + sin * ci, cos * ci - sin * cr
        out[k] = (er + tr, ei + ti)
        out[n // 2 - k] = (er - tr, ti - ei)
    return out


def real_inverse(spectrum):
    n = 2 * (len(spectrum) - 1)
    first, last = spectrum[0][0], spectrum[n // 2][0]
    if n == 2:
        return [first + last, first - last]
    even, odd = [None] * (n // 4 + 1), [None] * (n // 4 + 1)
    even[0], odd[0] = (first + last, None), (first - last, None)
    mid_re, mid_im = spectrum[n // 4]
    even[n // 4], odd[n // 4] = (mid_re + mid_re, None), (-(mid_im + mid_im), None)
    for k in range(1, n // 4):
        cos, sin = math.cos(2 * math.pi * k / n), math.sin(2 * math.pi * k / n)
        (ar, ai), (br, bi) = spectrum[k], spectrum[n // 2 - k]
        even[k] = (ar + br, ai - bi)
        tr, ti = ar - br, ai + bi
        odd[k] = (cos * tr - sin * ti, cos * ti + sin * tr)
    halves = real_inverse(even), real_inverse(odd)
    return [halves[i % 2][i // 2] for i in range(n)]


def band_edges():
    return 16 * lax.axis_index("z") + 16 * lax.axis_index("core") - 8


def forward_kernel(x_ref, abs_ref, out_ref):
    for core in range(2):
        row = pl.multiple_of(jnp.clip(band_edges() + 8 * core, 0, NX - 8), 8)
        for zz in range(2):
            rows = abs_ref[zz, pl.ds(row, 8), :]
            for slot in range(16 * core, 16 * core + 16):
                out_ref[slot, 4 + zz] = rows
    for zz in range(2):
        spectrum = real_transform([x_ref[n, zz] * decay**n for n in range(L)])
        out_ref[0, zz] = spectrum[0][0]
        out_ref[0, 2 + zz] = spectrum[PAIRS][0]
        for k in range(1, PAIRS):
            out_ref[k, zz] = spectrum[k][0]
            out_ref[k, 2 + zz] = spectrum[k][1]


def inverse_kernel(s_ref, out_ref, failed_ref):
    failed = jnp.zeros((8, 128), jnp.float32)
    for zz in range(2):
        ends = [s_ref[0, part, zz] for part in range(2)]
        spectrum = [(ends[0] + ends[0], None)]
        spectrum += [(s_ref[k, 0, zz], s_ref[k, 1, zz]) for k in range(1, PAIRS)]
        spectrum += [(ends[1] + ends[1], None)]
        values = real_inverse(spectrum)
        for n in range(L):
            out_ref[n, zz] = values[n] * (decay ** (-n) / (2 * L))
        failed = jnp.where(values[0] != values[0], 1.0, failed)
    failed_ref[0] = jnp.where(jnp.max(failed) > 0.0, 1, 0)


same = [(i, j) for i in range(STEPS + 1) for j in range(i, STEPS + 1)]
cross = [(i, j) for i in range(STEPS + 1) for j in range(i + 1, STEPS + 1)]
entry = {(kind, i, j): None for kind, ij in (("re", same), ("im", same), ("x", cross)) for i, j in ij}
for at, name in enumerate(entry):
    entry[name] = at


def tree_sum(terms):
    while len(terms) > 1:
        terms = [sum(terms[i : i + 2][1:], terms[i]) for i in range(0, len(terms), 2)]
    return terms[0]


def pick(slot, values):
    found = jnp.float32(values[0])
    for i in range(1, len(values)):
        found = jnp.where(slot == i, jnp.float32(values[i]), found)
    return found


def edges_kernel(own_ref, up_ref, down_ref, abs_ref):
    for sp in range(16):
        for i in range(4):
            up_ref[sp, pl.ds(HALO * i, HALO), :] = own_ref[1, sp, i, pl.ds(8 - HALO, HALO), :]
            down_ref[sp, pl.ds(HALO * i, HALO), :] = own_ref[0, sp, i, pl.ds(0, HALO), :]
        for side in range(2):
            for zz in range(2):
                abs_ref[side, sp, zz] = own_ref[side, sp, 4 + zz]


def basis_kernel(own_ref, left_ref, right_ref, swap_ref, v_ref, inv_ref, gram_ref, u, edge_inv, sums):
    slot, z, core = lax.axis_index(SLOTS), lax.axis_index("z"), lax.axis_index("core")
    shifts_here = slot_shifts()
    shift_a, shift_b, shift_im = (pick(slot, shifts_here[:, i]) for i in range(3))
    lanes = lax.broadcasted_iota(jnp.int32, (8, 128), 1)
    first_lane, last_lane = lanes == 0, lanes == 127
    blank = jnp.zeros((8, 128), jnp.float32)

    for turn in range(2):
        for part in range(2):
            for row in range(8, 40, 8):
                u[turn, part, 0, pl.ds(row, 8), :] = blank
                u[turn, part, NZ + 1, pl.ds(row, 8), :] = blank

    def put(turn, tile, layer, inverse, re, im):
        a, b, c = inverse
        u[turn, 0, layer, pl.ds(8 + 8 * tile, 8), :] = a * re - c * im
        u[turn, 1, layer, pl.ds(8 + 8 * tile, 8), :] = b * im + c * re

    def prepare(sp, _):
        for turn in range(2):
            for part in range(2):
                for zz in range(2):
                    u[turn, part, 2 * sp + zz + 1, pl.ds(0, 8), :] = blank
                    u[turn, part, 2 * sp + zz + 1, pl.ds(40, 8), :] = blank
        for tile in range(4):
            for zz in range(2):
                mine, other = own_ref[tile // 2, sp, 4 + zz], swap_ref[tile // 2, sp, zz]
                base = jnp.where(core == tile % 2, mine, other)
                da, db = (shift_a + 6.0) + base, (shift_b + 6.0) + base
                ra, rb = 1.0 / (da * da + shift_im * shift_im), 1.0 / (db * db + shift_im * shift_im)
                found = [da * ra, db * rb, -shift_im * ra]
                if tile in (1, 2):
                    for i in range(3):
                        inv_ref[i, tile - 1, sp, zz] = found[i]
                    re, im = (own_ref[tile - 1, sp, 2 * part + zz] for part in range(2))
                else:
                    inside = z > 0 if tile == 0 else z < lax.axis_size("z") - 1
                    found = [jnp.where(inside, f, 0.0) for f in found]
                    for i in range(3):
                        edge_inv[i, tile // 3, sp, zz] = found[i]
                    pair = []
                    for part in range(2):
                        at = HALO * (2 * part + zz)
                        if tile == 0:
                            start = max(at - (8 - HALO), 0)
                            rows = left_ref[sp, pl.ds(start, 8), :]
                            shift = start - (at - (8 - HALO))
                        else:
                            start = min(at, 4 * HALO - 8)
                            rows = right_ref[sp, pl.ds(start, 8), :]
                            shift = (start - at) % 8
                        pair.append(pltpu.roll(rows, shift, 0) if shift else rows)
                    re, im = pair
                put(0, tile, 2 * sp + zz + 1, found, re, im)
        return 0

    lax.fori_loop(0, NZ // 2, prepare, 0, unroll=4)

    def vector(j, side, sp, zz):
        if j == 0:
            return [own_ref[side, sp, 2 * part + zz] for part in range(2)]
        return [v_ref[j - 1, part, side, sp, zz] for part in range(2)]

    for j in range(STEPS):
        names = [name for name in entry if name[2] == j + 1 or (j == 0 and name[2] == 0)]

        def step(group, totals, j=j, names=names):
            by_layer = []
            for sp in [4 * group + s for s in range(4)]:
                found = {name: [] for name in names}
                for zz in range(2):
                    for tile in range(4) if j < STEPS - 1 else (1, 2):
                        layer, row = 2 * sp + zz + 1, 8 + 8 * tile
                        pair = []
                        for part in range(2):
                            old = u.at[j % 2, part]
                            here = old[layer, pl.ds(row, 8), :]
                            total = old[layer - 1, pl.ds(row, 8), :] + old[layer + 1, pl.ds(row, 8), :]
                            total = total + (old[layer, pl.ds(row - 1, 8), :] + old[layer, pl.ds(row + 1, 8), :])
                            total = total + (
                                jnp.where(first_lane, 0.0, pltpu.roll(here, 1, 1))
                                + jnp.where(last_lane, 0.0, pltpu.roll(here, 127, 1))
                            )
                            pair.append(total)
                        if tile in (1, 2):
                            side = tile - 1
                            if j < STEPS - 1:
                                for part in range(2):
                                    v_ref[j, part, side, sp, zz] = pair[part]
                            known = [vector(i, side, sp, zz) for i in range(j + 1)] + [pair]
                            for kind, i, k in names:
                                a, b = known[i], known[k]
                                if kind == "x":
                                    found[kind, i, k].append(a[0] * b[1] - a[1] * b[0])
                                else:
                                    part = ("re", "im").index(kind)
                                    found[kind, i, k].append(a[part] * b[part])
                        if j < STEPS - 1:
                            if tile in (1, 2):
                                inverse = [inv_ref[i, tile - 1, sp, zz] for i in range(3)]
                            else:
                                inverse = [edge_inv[i, tile // 3, sp, zz] for i in range(3)]
                            put((j + 1) % 2, tile, layer, inverse, *pair)
                by_layer.append([tree_sum(found[name]) for name in names])
            return tuple(t + tree_sum(list(parts)) for t, parts in zip(totals, zip(*by_layer)))

        totals = lax.fori_loop(0, NZ // 8, step, tuple(blank for _ in names), unroll=2)
        for name, total in zip(names, totals):
            sums[entry[name]] = total
    for spare in range(len(entry), sums.shape[0]):
        sums[spare] = blank

    rows = jnp.sum(sums[...], axis=1)
    column = jnp.sum(rows, axis=1, keepdims=True)
    where = lax.broadcasted_iota(jnp.int32, rows.shape, 0) == lax.broadcasted_iota(jnp.int32, rows.shape, 1)
    packed = jnp.sum(jnp.where(where, column, 0.0), axis=0, keepdims=True)
    gram_ref[...] = jnp.broadcast_to(packed[None], gram_ref.shape)


def multiplied(a, b):
    return (a[0] * b[0] - a[1] * b[1], a[0] * b[1] + a[1] * b[0])


def combine_kernel(count_ref, part_ref, own_ref, v_ref, inv_ref, out_ref):
    slot = lax.axis_index(SLOTS)
    ends = slot == 0
    low = lax.broadcasted_iota(jnp.int32, (8, 128), 1) < 64
    row = tree_sum([part_ref[i] for i in range(part_ref.shape[0])])

    def spread(name):
        return jnp.broadcast_to(row[:, entry[name] : entry[name] + 1], (8, 128))

    gram = {}
    for i, j in same:
        re, im = spread(("re", i, j)), spread(("im", i, j))
        real = jnp.where(ends, jnp.where(low, re, im), re + im)
        imag = jnp.where(ends, 0.0, spread(("x", i, j))) if j > i else jnp.zeros_like(real)
        gram[i, j] = (real, imag)

    count_lane = lax.broadcasted_iota(jnp.int32, (1, L), 1)
    count_a, count_b = (
        jnp.sum(jnp.where(count_lane == k, count_ref[...], 0).astype(jnp.float32), axis=1, keepdims=True)
        for k in (slot, jnp.where(ends, PAIRS, L - slot))
    )
    one, none = jnp.ones((8, 128), jnp.float32), jnp.zeros((8, 128), jnp.float32)
    poly, answer = [(one, none)], [(none, none) for _ in range(STEPS)]
    bound, doubt, scale = gram_rounding * gram[0, 0][0], none, None
    for m in range(STEPS):
        in_a, in_b = (jnp.broadcast_to(jnp.where(m < count, 1.0, 0.0), (8, 128)) for count in (count_a, count_b))
        weight = jnp.where(ends, jnp.where(low, in_a, in_b), in_a + in_b)
        g00, g01, g11 = gram[0, 0][0], gram[0, 1], gram[1, 1][0]
        denominator = (g00 - 2.0 * g01[0] + g11) + norm_floor
        inverse = 1.0 / denominator
        coef = ((g00 - g01[0]) * inverse, g01[1] * inverse)
        size = jnp.abs(coef[0]) + jnp.abs(coef[1])
        length = jnp.sqrt(jnp.maximum(g00, 0.0))
        if m == 0:
            scale = size * length
        step_doubt = bound * (2.0 + 4.0 * size) * jnp.abs(inverse) * length
        doubt = doubt + jnp.where(weight > 0.0, step_doubt, none)
        for j, p in enumerate(poly):
            term = multiplied(coef, p)
            answer[j] = (answer[j][0] + weight * term[0], answer[j][1] + weight * term[1])
        if m == STEPS - 1:
            break
        rest = (1.0 - coef[0], -coef[1])
        padded = [None] + poly + [None]
        following = []
        for j in range(len(poly) + 1):
            kept = multiplied(rest, poly[j]) if j < len(poly) else (none, none)
            moved = multiplied(coef, poly[j - 1]) if j > 0 else (none, none)
            following.append((kept[0] + moved[0], kept[1] + moved[1]))
        poly = following
        rr = rest[0] * rest[0] + rest[1] * rest[1]
        cc = coef[0] * coef[0] + coef[1] * coef[1]
        rc = multiplied((rest[0], -rest[1]), coef)
        cr = (rc[0], -rc[1])
        size_rest = jnp.abs(rest[0]) + jnp.abs(rest[1])
        bound = bound * (size + size_rest) * (size + size_rest)

        def at(i, j):
            return gram[i, j] if i <= j else (gram[j, i][0], -gram[j, i][1])

        shrunk = {}
        top = STEPS - m
        for i in range(top):
            for j in range(i, top):
                a, b, d = at(i, j), at(i, j + 1), at(i + 1, j + 1)
                if i == j:
                    ab = multiplied(rc, b)
                    shrunk[i, j] = (rr * a[0] + 2.0 * ab[0] + cc * d[0], none)
                else:
                    ab, ac = multiplied(rc, b), multiplied(cr, at(i + 1, j))
                    shrunk[i, j] = tuple(rr * a[x] + (ab[x] + ac[x]) + cc * d[x] for x in range(2))
        gram = shrunk

    trusted = doubt <= error_allowed * scale
    weights = []
    for re, im in answer:
        re = jnp.where(trusted, re, jnp.nan)
        weights.append(
            (
                jnp.broadcast_to(re[:, 0:1], (8, 128)),
                jnp.broadcast_to(re[:, 127:128], (8, 128)),
                jnp.broadcast_to(im[:, 0:1], (8, 128)),
            )
        )

    def finish(sp, _):
        for side in range(2):
            for zz in range(2):
                res, ims = [], []
                for j, (wa, wb, wi) in enumerate(weights):
                    re, im = ((own_ref[side, sp, 2 * part + zz] if j == 0 else v_ref[j - 1, part, side, sp, zz]) for part in range(2))
                    res.append(wa * re - wi * im)
                    ims.append(wb * im + wi * re)
                re, im = tree_sum(res), tree_sum(ims)
                a, b, c = (inv_ref[i, side, sp, zz] for i in range(3))
                out_ref[side, sp, 0, zz] = a * re - c * im
                out_ref[side, sp, 1, zz] = b * im + c * re
        return 0

    lax.fori_loop(0, NZ // 2, finish, 0, unroll=2)


def slot_shifts():
    table = np.zeros((PAIRS, 4), np.float32)
    for slot in range(PAIRS):
        angle = 2 * math.pi * slot / L
        table[slot, :2] = (1 - decay * math.cos(angle)) / step_size
        table[slot, 2] = decay * math.sin(angle) / step_size
    table[0, 1] = (1 + decay) / step_size
    return table


def exchanged(blocks, axes):
    return lax.all_to_all(blocks, axes, split_axis=0, concat_axis=0, tiled=True)


VMEM = pl.BlockSpec(memory_space=pltpu.VMEM)
SMEM = pl.BlockSpec(memory_space=pltpu.SMEM)


def f32(*shape):
    return pltpu.VMEM(shape, jnp.float32)


def held(x):
    return pltpu.with_memory_space_constraint(x, pltpu.MemorySpace.VMEM)


def room(mebibytes):
    return pltpu.CompilerParams(vmem_limit_bytes=mebibytes * 2**20)


def together(residual, absorption, counts):
    chips = lax.axis_size("z")
    bands = residual.reshape(4, 2, 16, 8, 128).transpose(2, 0, 1, 3, 4)
    series = exchanged(bands, TM).reshape(L, 2, 8, 128)
    spectrum = pl.pallas_call(
        forward_kernel,
        out_shape=f32(PAIRS, 6, 8, 128),
        in_specs=[VMEM, VMEM],
        out_specs=VMEM,
        compiler_params=room(4),
        name="forward",
    )(held(series), held(absorption))
    own = held(exchanged(spectrum, SLOTS).reshape(2, 16, 6, 8, 128))
    up, down, swap = pl.pallas_call(
        edges_kernel,
        out_shape=(f32(16, 4 * HALO, 128), f32(16, 4 * HALO, 128), f32(2, 16, 2, 8, 128)),
        in_specs=[VMEM],
        out_specs=(VMEM, VMEM, VMEM),
        compiler_params=room(2),
        name="edges",
    )(own)
    left = lax.ppermute(up, "z", [(i, i + 1) for i in range(chips - 1)])
    right = lax.ppermute(down, "z", [(i + 1, i) for i in range(chips - 1)])
    swap = lax.ppermute(swap, "core", [(0, 1), (1, 0)])
    basis, inverses, partial = pl.pallas_call(
        basis_kernel,
        out_shape=(f32(STEPS - 1, 2, 2, 16, 2, 8, 128), f32(3, 2, 16, 2, 8, 128), f32(8, 8, 128)),
        in_specs=[VMEM, VMEM, VMEM, VMEM],
        out_specs=(VMEM, VMEM, VMEM),
        scratch_shapes=[
            pltpu.VMEM((2, 2, NZ + 2, 48, 128), jnp.float32),
            pltpu.VMEM((3, 2, 16, 2, 8, 128), jnp.float32),
            pltpu.VMEM((80, 8, 128), jnp.float32),
        ],
        compiler_params=room(10),
        name="basis",
    )(own, held(left), held(right), held(swap))
    partials = exchanged(partial, "z")
    solved = pl.pallas_call(
        combine_kernel,
        out_shape=f32(2, 16, 2, 2, 8, 128),
        in_specs=[VMEM, VMEM, VMEM, VMEM, VMEM],
        out_specs=VMEM,
        compiler_params=room(6),
        name="combine",
    )(held(counts.reshape(1, L)), held(partials), own, held(basis), held(inverses))
    gathered = exchanged(solved.reshape(32, 2, 2, 8, 128), SLOTS)
    values, failed = pl.pallas_call(
        inverse_kernel,
        out_shape=(f32(L, 2, 8, 128), jax.ShapeDtypeStruct((1,), jnp.int32)),
        in_specs=[VMEM],
        out_specs=(VMEM, SMEM),
        compiler_params=room(4),
        name="inverse",
    )(held(gathered))
    return values, failed


def to_steps(values, shape):
    bands = exchanged(values.reshape(16, 4, 2, 8, 128), TM)
    return bands.transpose(1, 2, 0, 3, 4).reshape(shape)


def body(residual, absorption, counts):
    values, failed = together(residual, absorption, counts)
    return lax.cond(
        failed[0] > 0,
        lambda r, a, c, v: stepwise(r, a, c),
        lambda r, a, c, v: to_steps(v, r.shape),
        residual, absorption, counts, values,
    )


def solution(mesh):
    chips, cores = mesh.shape["tm"] // 2, 2
    devices = mesh.devices.reshape(chips, cores, 4, 4)
    inner = Mesh(devices, ("z", "core", "y", "x"))
    in_specs = (P(TM, SPACE, None, None), P(SPACE, None, None), P())
    out_specs = P(TM, SPACE, None, None)
    return jax.shard_map(body, mesh=inner, in_specs=in_specs, out_specs=out_specs, check_vma=False)
```

```python
import math

import jax
import jax.numpy as jnp
import numpy as np
from jax import lax
from jax.experimental import pallas as pl
from jax.experimental.pallas import tpu as pltpu
from jax.sharding import Mesh
from jax.sharding import PartitionSpec as P

L = 64
STEPS = 6
HALO = 6
NX = 128
NZ = 32
PAIRS = L // 2
TM = ("z", "core")
SPACE = ("y", "x")
SLOTS = ("core", "y", "x")

wrap_factor = 0.1
step_size = 1.0
norm_floor = 1e-06
highest = lax.Precision.HIGHEST
decay = wrap_factor ** (1.0 / L)

gram_rounding = 2.5e-7
error_allowed = 5e-4


def with_halo(cells, sides, width):
    for axis, dim in sides:
        count = lax.axis_size(axis)
        ends = count - 1
        head = lax.slice_in_dim(cells, 0, width, axis=dim)
        tail = lax.slice_in_dim(cells, cells.shape[dim] - width, cells.shape[dim], axis=dim)
        cells = jnp.concatenate(
            [
                lax.ppermute(tail, axis, [(i, (i + 1) % count) for i in range(ends)]),
                cells,
                lax.ppermute(head, axis, [((i + 1) % count, i) for i in range(ends)]),
            ],
            axis=dim,
        )
    return cells


def copy_for_each(shard, axis):
    copies = jnp.broadcast_to(shard, (lax.axis_size(axis), *shard.shape))
    return lax.all_to_all(copies, axis, split_axis=0, concat_axis=0, tiled=True)


def taken_together(shard, axis):
    return copy_for_each(shard, axis).sum(axis=0)


def packed_total(arrays, axis):
    vector, at, finished = (jnp.concatenate([a.reshape(-1) for a in arrays]), 0, [])
    so_far = taken_together(vector, axis)
    for a in arrays:
        finished.append(so_far[at : at + a.size].reshape(a.shape))
        at += a.size
    return tuple(finished)


def shifts(frequency):
    angles = frequency.astype(jnp.float32) * (2.0 * math.pi / L)
    decay_rate = wrap_factor ** (1.0 / L)
    shift_re = (1.0 - decay_rate * jnp.cos(angles)) / step_size
    shift_im = decay_rate * jnp.sin(angles) / step_size
    return (shift_re, shift_im)


def near_sum(padded):
    interior = padded[..., 1:-1, :, :]
    widths = [(0, 0)] * (interior.ndim - 2) + [(1, 1), (1, 1)]
    padded_xy = jnp.pad(interior, widths)
    summed = padded[..., 2:, :, :] + padded[..., :-2, :, :]
    summed = summed + padded_xy[..., 2:, 1:-1] + padded_xy[..., :-2, 1:-1]
    summed = summed + padded_xy[..., 1:-1, 2:] + padded_xy[..., 1:-1, :-2]
    return summed


def advance(carried, dir_re, dir_im, img_re, img_im, coef_re, coef_im):
    sol_re, sol_im, res_re, res_im = carried
    sol_re = sol_re + coef_re * dir_re - coef_im * dir_im
    sol_im = sol_im + coef_re * dir_im + coef_im * dir_re
    res_re = res_re - (coef_re * img_re - coef_im * img_im)
    res_im = res_im - (coef_re * img_im + coef_im * img_re)
    return (sol_re, sol_im, res_re, res_im)


def solve_together(spectrum, absorption, frequencies, step_counts, longest):
    shift_re, shift_im = shifts(frequencies)
    shift_re = shift_re[:, None, None, None]
    shift_im = shift_im[:, None, None, None]
    diag_re = shift_re + 6.0 + absorption[None]
    magnitude = diag_re * diag_re + shift_im * shift_im
    inv_re = diag_re / magnitude
    inv_im = -shift_im / magnitude

    def iterate(iteration, carried):
        res_re, res_im = (carried[2], carried[3])
        dir_re = inv_re * res_re - inv_im * res_im
        dir_im = inv_re * res_im + inv_im * res_re
        padded = with_halo(jnp.stack([dir_re, dir_im], axis=1), ((SPACE, 2),), 1)
        nearby = near_sum(padded)
        img_re = diag_re * dir_re - shift_im * dir_im - nearby[:, 0]
        img_im = diag_re * dir_im + shift_im * dir_re - nearby[:, 1]
        totals = packed_total(
            (
                jnp.sum(img_re * res_re + img_im * res_im, axis=(1, 2, 3)),
                jnp.sum(img_re * res_im - img_im * res_re, axis=(1, 2, 3)),
                jnp.sum(img_re * img_re + img_im * img_im, axis=(1, 2, 3)),
            ),
            SPACE,
        )
        active = iteration < step_counts
        denominator = totals[2] + norm_floor
        coef_re = jnp.where(active, totals[0] / denominator, 0.0)[:, None, None, None]
        coef_im = jnp.where(active, totals[1] / denominator, 0.0)[:, None, None, None]
        return advance(carried, dir_re, dir_im, img_re, img_im, coef_re, coef_im)

    blank = jnp.zeros_like(spectrum[:, 0])
    finished = lax.fori_loop(0, longest, iterate, (blank, blank, spectrum[:, 0], spectrum[:, 1]))
    return jnp.stack([finished[0], finished[1]], axis=1)


def slot_order():
    return jnp.arange(L, dtype=jnp.int32)


def phase_table(left, right):
    return (left[:, None] * right[None, :] % L).astype(jnp.float32) * (2.0 * math.pi / L)


def stepwise(residual, absorption, counts):
    per_device = residual.shape[0]
    decay_rate = wrap_factor ** (1.0 / L)
    first_step = lax.axis_index(TM) * per_device
    times_here = first_step + jnp.arange(per_device, dtype=jnp.int32)
    scaled = residual * jnp.power(decay_rate, times_here.astype(jnp.float32))[:, None, None, None]
    slot_freqs = slot_order()
    own_freqs = lax.dynamic_slice_in_dim(slot_freqs, first_step, per_device)
    own_counts = counts[own_freqs]
    longest = jnp.max(counts)
    all_times = jnp.arange(L, dtype=jnp.int32)
    series = lax.all_to_all(scaled, TM, split_axis=2, concat_axis=0, tiled=True)
    phases = phase_table(slot_freqs, all_times)
    real_part = jnp.einsum("sn,nzxy->szxy", jnp.cos(phases), series, precision=highest)
    imag_part = -jnp.einsum("sn,nzxy->szxy", jnp.sin(phases), series, precision=highest)
    spectrum = lax.all_to_all(
        jnp.stack([real_part, imag_part], axis=1), TM, split_axis=0, concat_axis=3, tiled=True
    )
    solved = solve_together(spectrum, absorption, own_freqs, own_counts, longest)
    gathered = lax.all_to_all(solved, TM, split_axis=3, concat_axis=0, tiled=True)
    phases = phase_table(all_times, slot_freqs)
    values = jnp.einsum("ns,szxy->nzxy", jnp.cos(phases), gathered[:, 0], precision=highest)
    values = values - jnp.einsum(
        "ns,szxy->nzxy", jnp.sin(phases), gathered[:, 1], precision=highest
    )
    weight = jnp.power(decay_rate, -all_times.astype(jnp.float32)) / L
    values = values * weight[:, None, None, None]
    return lax.all_to_all(values, TM, split_axis=0, concat_axis=2, tiled=True)


def real_transform(x):
    n = len(x)
    if n == 2:
        return [(x[0] + x[1], None), (x[0] - x[1], None)]
    even, odd = real_transform(x[0::2]), real_transform(x[1::2])
    out = [None] * (n // 2 + 1)
    out[0] = (even[0][0] + odd[0][0], None)
    out[n // 2] = (even[0][0] - odd[0][0], None)
    out[n // 4] = (even[n // 4][0], -odd[n // 4][0])
    for k in range(1, n // 4):
        cos, sin = math.cos(2 * math.pi * k / n), math.sin(2 * math.pi * k / n)
        (er, ei), (cr, ci) = even[k], odd[k]
        tr, ti = cos * cr + sin * ci, cos * ci - sin * cr
        out[k] = (er + tr, ei + ti)
        out[n // 2 - k] = (er - tr, ti - ei)
    return out


def real_inverse(spectrum):
    n = 2 * (len(spectrum) - 1)
    first, last = spectrum[0][0], spectrum[n // 2][0]
    if n == 2:
        return [first + last, first - last]
    even, odd = [None] * (n // 4 + 1), [None] * (n // 4 + 1)
    even[0], odd[0] = (first + last, None), (first - last, None)
    mid_re, mid_im = spectrum[n // 4]
    even[n // 4], odd[n // 4] = (mid_re + mid_re, None), (-(mid_im + mid_im), None)
    for k in range(1, n // 4):
        cos, sin = math.cos(2 * math.pi * k / n), math.sin(2 * math.pi * k / n)
        (ar, ai), (br, bi) = spectrum[k], spectrum[n // 2 - k]
        even[k] = (ar + br, ai - bi)
        tr, ti = ar - br, ai + bi
        odd[k] = (cos * tr - sin * ti, cos * ti + sin * tr)
    halves = real_inverse(even), real_inverse(odd)
    return [halves[i % 2][i // 2] for i in range(n)]


def bands_kernel(x_ref, a_ref, out_ref, rows_ref, sems):
    copies = [
        pltpu.make_async_copy(x_ref.at[:, :, pl.ds(8 * band, 8), :], out_ref.at[band], sems.at[band]) for band in range(16)
    ]
    first = 16 * lax.axis_index("z") + 16 * lax.axis_index("core") - 8
    for core in range(2):
        row = pl.multiple_of(jnp.clip(first + 8 * core, 0, NX - 8), 8)
        copies.append(pltpu.make_async_copy(a_ref.at[:, pl.ds(row, 8), :], rows_ref.at[core], sems.at[16 + core]))
    for copy in copies:
        copy.start()
    for copy in copies:
        copy.wait()


def forward_kernel(x_ref, rows_ref, out_ref):
    for core in range(2):
        for zz in range(2):
            rows = rows_ref[core, zz]
            for slot in range(16 * core, 16 * core + 16):
                out_ref[slot, 4 + zz] = rows
    for zz in range(2):
        spectrum = real_transform([x_ref[n, zz] * decay**n for n in range(L)])
        out_ref[0, zz] = spectrum[0][0]
        out_ref[0, 2 + zz] = spectrum[PAIRS][0]
        for k in range(1, PAIRS):
            out_ref[k, zz] = spectrum[k][0]
            out_ref[k, 2 + zz] = spectrum[k][1]


def inverse_kernel(s_ref, out_ref, failed_ref):
    failed = jnp.zeros((8, 128), jnp.float32)
    for zz in range(2):
        ends = [s_ref[0, part, zz] for part in range(2)]
        spectrum = [(ends[0] + ends[0], None)]
        spectrum += [(s_ref[k, 0, zz], s_ref[k, 1, zz]) for k in range(1, PAIRS)]
        spectrum += [(ends[1] + ends[1], None)]
        values = real_inverse(spectrum)
        for n in range(L):
            out_ref[n, zz] = values[n] * (decay ** (-n) / (2 * L))
        failed = jnp.where(values[0] != values[0], 1.0, failed)
    failed_ref[0] = jnp.where(jnp.max(failed) > 0.0, 1, 0)


same = [(i, j) for i in range(STEPS + 1) for j in range(i, STEPS + 1)]
cross = [(i, j) for i in range(STEPS + 1) for j in range(i + 1, STEPS + 1)]
entry = {(kind, i, j): None for kind, ij in (("re", same), ("im", same), ("x", cross)) for i, j in ij}
for at, name in enumerate(entry):
    entry[name] = at


def tree_sum(terms):
    while len(terms) > 1:
        terms = [sum(terms[i : i + 2][1:], terms[i]) for i in range(0, len(terms), 2)]
    return terms[0]


def pick(slot, values):
    found = jnp.float32(values[0])
    for i in range(1, len(values)):
        found = jnp.where(slot == i, jnp.float32(values[i]), found)
    return found


def edges_kernel(own_ref, first_ref, second_ref, abs_ref):
    low = lax.axis_index("core") == 0
    for sp in range(16):
        for i in range(4):
            up, down = own_ref[1, sp, i, pl.ds(8 - HALO, HALO), :], own_ref[0, sp, i, pl.ds(0, HALO), :]
            first_ref[sp, pl.ds(HALO * i, HALO), :] = jnp.where(low, up, down)
            second_ref[sp, pl.ds(HALO * i, HALO), :] = jnp.where(low, down, up)
        for side in range(2):
            for zz in range(2):
                abs_ref[side, sp, zz] = own_ref[side, sp, 4 + zz]


def basis_kernel(own_ref, first_ref, second_ref, swap_ref, v_ref, inv_ref, gram_ref, u, edge_inv, sums):
    slot, z, core = lax.axis_index(SLOTS), lax.axis_index("z"), lax.axis_index("core")
    shifts_here = slot_shifts()
    shift_a, shift_b, shift_im = (pick(slot, shifts_here[:, i]) for i in range(3))
    lanes = lax.broadcasted_iota(jnp.int32, (8, 128), 1)
    first_lane, last_lane = lanes == 0, lanes == 127
    blank = jnp.zeros((8, 128), jnp.float32)

    for turn in range(2):
        for part in range(2):
            for row in range(8, 40, 8):
                u[turn, part, 0, pl.ds(row, 8), :] = blank
                u[turn, part, NZ + 1, pl.ds(row, 8), :] = blank

    def put(turn, tile, layer, inverse, re, im):
        a, b, c = inverse
        u[turn, 0, layer, pl.ds(8 + 8 * tile, 8), :] = a * re - c * im
        u[turn, 1, layer, pl.ds(8 + 8 * tile, 8), :] = b * im + c * re

    def prepare(sp, _):
        for turn in range(2):
            for part in range(2):
                for zz in range(2):
                    u[turn, part, 2 * sp + zz + 1, pl.ds(0, 8), :] = blank
                    u[turn, part, 2 * sp + zz + 1, pl.ds(40, 8), :] = blank
        for tile in range(4):
            for zz in range(2):
                mine, other = own_ref[tile // 2, sp, 4 + zz], swap_ref[tile // 2, sp, zz]
                base = jnp.where(core == tile % 2, mine, other)
                da, db = (shift_a + 6.0) + base, (shift_b + 6.0) + base
                ra, rb = 1.0 / (da * da + shift_im * shift_im), 1.0 / (db * db + shift_im * shift_im)
                found = [da * ra, db * rb, -shift_im * ra]
                if tile in (1, 2):
                    for i in range(3):
                        inv_ref[i, tile - 1, sp, zz] = found[i]
                    re, im = (own_ref[tile - 1, sp, 2 * part + zz] for part in range(2))
                else:
                    inside = z > 0 if tile == 0 else z < lax.axis_size("z") - 1
                    found = [jnp.where(inside, f, 0.0) for f in found]
                    for i in range(3):
                        edge_inv[i, tile // 3, sp, zz] = found[i]
                    pair = []
                    for part in range(2):
                        at = HALO * (2 * part + zz)
                        wanted = at - (8 - HALO) if tile == 0 else at
                        start = min(max(wanted, 0), 4 * HALO - 8)
                        first, second = (ref[sp, pl.ds(start, 8), :] for ref in (first_ref, second_ref))
                        rows = jnp.where((core == 0) == (tile == 0), first, second)
                        shift = (start - wanted) % 8
                        pair.append(pltpu.roll(rows, shift, 0) if shift else rows)
                    re, im = pair
                put(0, tile, 2 * sp + zz + 1, found, re, im)
        return 0

    lax.fori_loop(0, NZ // 2, prepare, 0, unroll=4)

    def vector(j, side, sp, zz):
        if j == 0:
            return [own_ref[side, sp, 2 * part + zz] for part in range(2)]
        return [v_ref[j - 1, part, side, sp, zz] for part in range(2)]

    for j in range(STEPS):
        names = [name for name in entry if name[2] == j + 1 or (j == 0 and name[2] == 0)]

        def step(group, totals, j=j, names=names):
            by_layer = []
            for sp in [4 * group + s for s in range(4)]:
                found = {name: [] for name in names}
                for zz in range(2):
                    for tile in range(4) if j < STEPS - 1 else (1, 2):
                        layer, row = 2 * sp + zz + 1, 8 + 8 * tile
                        pair = []
                        for part in range(2):
                            old = u.at[j % 2, part]
                            here = old[layer, pl.ds(row, 8), :]
                            total = old[layer - 1, pl.ds(row, 8), :] + old[layer + 1, pl.ds(row, 8), :]
                            total = total + (old[layer, pl.ds(row - 1, 8), :] + old[layer, pl.ds(row + 1, 8), :])
                            total = total + (
                                jnp.where(first_lane, 0.0, pltpu.roll(here, 1, 1))
                                + jnp.where(last_lane, 0.0, pltpu.roll(here, 127, 1))
                            )
                            pair.append(total)
                        if tile in (1, 2):
                            side = tile - 1
                            if j < STEPS - 1:
                                for part in range(2):
                                    v_ref[j, part, side, sp, zz] = pair[part]
                            known = [vector(i, side, sp, zz) for i in range(j + 1)] + [pair]
                            for kind, i, k in names:
                                a, b = known[i], known[k]
                                if kind == "x":
                                    found[kind, i, k].append(a[0] * b[1] - a[1] * b[0])
                                else:
                                    part = ("re", "im").index(kind)
                                    found[kind, i, k].append(a[part] * b[part])
                        if j < STEPS - 1:
                            if tile in (1, 2):
                                inverse = [inv_ref[i, tile - 1, sp, zz] for i in range(3)]
                            else:
                                inverse = [edge_inv[i, tile // 3, sp, zz] for i in range(3)]
                            put((j + 1) % 2, tile, layer, inverse, *pair)
                by_layer.append([tree_sum(found[name]) for name in names])
            return tuple(t + tree_sum(list(parts)) for t, parts in zip(totals, zip(*by_layer)))

        totals = lax.fori_loop(0, NZ // 8, step, tuple(blank for _ in names), unroll=2)
        for name, total in zip(names, totals):
            sums[entry[name]] = total
    for spare in range(len(entry), sums.shape[0]):
        sums[spare] = blank

    rows = jnp.sum(sums[...], axis=1)
    column = jnp.sum(rows, axis=1, keepdims=True)
    where = lax.broadcasted_iota(jnp.int32, rows.shape, 0) == lax.broadcasted_iota(jnp.int32, rows.shape, 1)
    packed = jnp.sum(jnp.where(where, column, 0.0), axis=0, keepdims=True)
    gram_ref[...] = jnp.broadcast_to(packed[None], gram_ref.shape)


def multiplied(a, b):
    return (a[0] * b[0] - a[1] * b[1], a[0] * b[1] + a[1] * b[0])


def combine_kernel(count_ref, part_ref, own_ref, v_ref, inv_ref, out_ref):
    slot = lax.axis_index(SLOTS)
    ends = slot == 0
    low = lax.broadcasted_iota(jnp.int32, (8, 128), 1) < 64
    row = tree_sum([part_ref[i] for i in range(part_ref.shape[0])])

    def spread(name):
        return jnp.broadcast_to(row[:, entry[name] : entry[name] + 1], (8, 128))

    gram = {}
    for i, j in same:
        re, im = spread(("re", i, j)), spread(("im", i, j))
        real = jnp.where(ends, jnp.where(low, re, im), re + im)
        imag = jnp.where(ends, 0.0, spread(("x", i, j))) if j > i else jnp.zeros_like(real)
        gram[i, j] = (real, imag)

    count_lane = lax.broadcasted_iota(jnp.int32, (1, L), 1)
    count_a, count_b = (
        jnp.sum(jnp.where(count_lane == k, count_ref[...], 0).astype(jnp.float32), axis=1, keepdims=True)
        for k in (slot, jnp.where(ends, PAIRS, L - slot))
    )
    one, none = jnp.ones((8, 128), jnp.float32), jnp.zeros((8, 128), jnp.float32)
    poly, answer = [(one, none)], [(none, none) for _ in range(STEPS)]
    bound, doubt, scale = gram_rounding * gram[0, 0][0], none, None
    for m in range(STEPS):
        in_a, in_b = (jnp.broadcast_to(jnp.where(m < count, 1.0, 0.0), (8, 128)) for count in (count_a, count_b))
        weight = jnp.where(ends, jnp.where(low, in_a, in_b), in_a + in_b)
        g00, g01, g11 = gram[0, 0][0], gram[0, 1], gram[1, 1][0]
        denominator = (g00 - 2.0 * g01[0] + g11) + norm_floor
        inverse = 1.0 / denominator
        coef = ((g00 - g01[0]) * inverse, g01[1] * inverse)
        size = jnp.abs(coef[0]) + jnp.abs(coef[1])
        length = jnp.sqrt(jnp.maximum(g00, 0.0))
        if m == 0:
            scale = size * length
        step_doubt = bound * (2.0 + 4.0 * size) * jnp.abs(inverse) * length
        doubt = doubt + jnp.where(weight > 0.0, step_doubt, none)
        for j, p in enumerate(poly):
            term = multiplied(coef, p)
            answer[j] = (answer[j][0] + weight * term[0], answer[j][1] + weight * term[1])
        if m == STEPS - 1:
            break
        rest = (1.0 - coef[0], -coef[1])
        padded = [None] + poly + [None]
        following = []
        for j in range(len(poly) + 1):
            kept = multiplied(rest, poly[j]) if j < len(poly) else (none, none)
            moved = multiplied(coef, poly[j - 1]) if j > 0 else (none, none)
            following.append((kept[0] + moved[0], kept[1] + moved[1]))
        poly = following
        rr = rest[0] * rest[0] + rest[1] * rest[1]
        cc = coef[0] * coef[0] + coef[1] * coef[1]
        rc = multiplied((rest[0], -rest[1]), coef)
        cr = (rc[0], -rc[1])
        size_rest = jnp.abs(rest[0]) + jnp.abs(rest[1])
        bound = bound * (size + size_rest) * (size + size_rest)

        def at(i, j):
            return gram[i, j] if i <= j else (gram[j, i][0], -gram[j, i][1])

        shrunk = {}
        top = STEPS - m
        for i in range(top):
            for j in range(i, top):
                a, b, d = at(i, j), at(i, j + 1), at(i + 1, j + 1)
                if i == j:
                    ab = multiplied(rc, b)
                    shrunk[i, j] = (rr * a[0] + 2.0 * ab[0] + cc * d[0], none)
                else:
                    ab, ac = multiplied(rc, b), multiplied(cr, at(i + 1, j))
                    shrunk[i, j] = tuple(rr * a[x] + (ab[x] + ac[x]) + cc * d[x] for x in range(2))
        gram = shrunk

    trusted = doubt <= error_allowed * scale
    weights = []
    for re, im in answer:
        re = jnp.where(trusted, re, jnp.nan)
        weights.append(
            (
                jnp.broadcast_to(re[:, 0:1], (8, 128)),
                jnp.broadcast_to(re[:, 127:128], (8, 128)),
                jnp.broadcast_to(im[:, 0:1], (8, 128)),
            )
        )

    def finish(sp, _):
        for side in range(2):
            for zz in range(2):
                res, ims = [], []
                for j, (wa, wb, wi) in enumerate(weights):
                    re, im = ((own_ref[side, sp, 2 * part + zz] if j == 0 else v_ref[j - 1, part, side, sp, zz]) for part in range(2))
                    res.append(wa * re - wi * im)
                    ims.append(wb * im + wi * re)
                re, im = tree_sum(res), tree_sum(ims)
                a, b, c = (inv_ref[i, side, sp, zz] for i in range(3))
                out_ref[side, sp, 0, zz] = a * re - c * im
                out_ref[side, sp, 1, zz] = b * im + c * re
        return 0

    lax.fori_loop(0, NZ // 2, finish, 0, unroll=2)


def slot_shifts():
    table = np.zeros((PAIRS, 4), np.float32)
    for slot in range(PAIRS):
        angle = 2 * math.pi * slot / L
        table[slot, :2] = (1 - decay * math.cos(angle)) / step_size
        table[slot, 2] = decay * math.sin(angle) / step_size
    table[0, 1] = (1 + decay) / step_size
    return table


def exchanged(blocks, axes):
    return lax.all_to_all(blocks, axes, split_axis=0, concat_axis=0, tiled=True)


VMEM = pl.BlockSpec(memory_space=pltpu.VMEM)
SMEM = pl.BlockSpec(memory_space=pltpu.SMEM)
ANY = pl.BlockSpec(memory_space=pl.ANY)


def f32(*shape):
    return pltpu.VMEM(shape, jnp.float32)


def held(x):
    return pltpu.with_memory_space_constraint(x, pltpu.MemorySpace.VMEM)


def in_hbm(x):
    return pltpu.with_memory_space_constraint(x, pltpu.MemorySpace.HBM)


def room(mebibytes):
    return pltpu.CompilerParams(vmem_limit_bytes=mebibytes * 2**20)


def together(residual, absorption, counts):
    chips = lax.axis_size("z")
    bands, rows = pl.pallas_call(
        bands_kernel,
        out_shape=(f32(16, 4, 2, 8, 128), f32(2, 2, 8, 128)),
        in_specs=[ANY, ANY],
        out_specs=(VMEM, VMEM),
        scratch_shapes=[pltpu.SemaphoreType.DMA((18,))],
        compiler_params=room(2),
        name="bands",
    )(in_hbm(residual), in_hbm(absorption))
    series = exchanged(bands, TM).reshape(L, 2, 8, 128)
    spectrum = pl.pallas_call(
        forward_kernel,
        out_shape=f32(PAIRS, 6, 8, 128),
        in_specs=[VMEM, VMEM],
        out_specs=VMEM,
        compiler_params=room(4),
        name="forward",
    )(held(series), held(rows))
    own = held(exchanged(spectrum, SLOTS).reshape(2, 16, 6, 8, 128))
    first, second, swap = pl.pallas_call(
        edges_kernel,
        out_shape=(f32(16, 4 * HALO, 128), f32(16, 4 * HALO, 128), f32(2, 16, 2, 8, 128)),
        in_specs=[VMEM],
        out_specs=(VMEM, VMEM, VMEM),
        compiler_params=room(2),
        name="edges",
    )(own)
    ups = [[(2 * i + core, 2 * i + 2 + core) for i in range(chips - 1)] for core in range(2)]
    downs = [[(b, a) for a, b in pairs] for pairs in ups]
    swap = lax.ppermute(swap, "core", [(0, 1), (1, 0)])
    first = lax.ppermute(first, TM, ups[0] + downs[1])
    second = lax.ppermute(second, TM, downs[0] + ups[1])
    basis, inverses, partial = pl.pallas_call(
        basis_kernel,
        out_shape=(f32(STEPS - 1, 2, 2, 16, 2, 8, 128), f32(3, 2, 16, 2, 8, 128), f32(8, 8, 128)),
        in_specs=[VMEM, VMEM, VMEM, VMEM],
        out_specs=(VMEM, VMEM, VMEM),
        scratch_shapes=[
            pltpu.VMEM((2, 2, NZ + 2, 48, 128), jnp.float32),
            pltpu.VMEM((3, 2, 16, 2, 8, 128), jnp.float32),
            pltpu.VMEM((80, 8, 128), jnp.float32),
        ],
        compiler_params=room(10),
        name="basis",
    )(own, held(first), held(second), held(swap))
    partials = exchanged(partial, "z")
    solved = pl.pallas_call(
        combine_kernel,
        out_shape=f32(2, 16, 2, 2, 8, 128),
        in_specs=[VMEM, VMEM, VMEM, VMEM, VMEM],
        out_specs=VMEM,
        compiler_params=room(6),
        name="combine",
    )(held(counts.reshape(1, L)), held(partials), own, held(basis), held(inverses))
    gathered = exchanged(solved.reshape(32, 2, 2, 8, 128), SLOTS)
    values, failed = pl.pallas_call(
        inverse_kernel,
        out_shape=(f32(L, 2, 8, 128), pltpu.SMEM((1,), jnp.int32)),
        in_specs=[VMEM],
        out_specs=(VMEM, SMEM),
        compiler_params=room(4),
        name="inverse",
    )(held(gathered))
    return values, failed


def to_steps(values, shape):
    bands = exchanged(values.reshape(16, 4, 2, 8, 128), TM)
    return bands.transpose(1, 2, 0, 3, 4).reshape(shape)


def body(residual, absorption, counts):
    values, failed = together(residual, absorption, counts)
    return lax.cond(
        failed[0] > 0,
        lambda r, a, c, v: stepwise(r, a, c),
        lambda r, a, c, v: to_steps(v, r.shape),
        residual, absorption, counts, values,
    )


def solution(mesh):
    chips, cores = mesh.shape["tm"] // 2, 2
    devices = mesh.devices.reshape(chips, cores, 4, 4)
    inner = Mesh(devices, ("z", "core", "y", "x"))
    in_specs = (P(TM, SPACE, None, None), P(SPACE, None, None), P())
    out_specs = P(TM, SPACE, None, None)
    return jax.shard_map(body, mesh=inner, in_specs=in_specs, out_specs=out_specs, check_vma=False)
```

```python
import math

import jax
import jax.numpy as jnp
import numpy as np
from jax import lax
from jax.experimental import pallas as pl
from jax.experimental.pallas import tpu as pltpu
from jax.sharding import Mesh
from jax.sharding import PartitionSpec as P

L = 64
STEPS = 6
HALO = 6
NX = 128
NZ = 32
PAIRS = L // 2
TM = ("z", "core")
SPACE = ("y", "x")
SLOTS = ("core", "y", "x")

wrap_factor = 0.1
step_size = 1.0
norm_floor = 1e-06
highest = lax.Precision.HIGHEST
decay = wrap_factor ** (1.0 / L)

gram_rounding = 1e-6
error_allowed = 1.5e-4


def with_halo(cells, sides, width):
    for axis, dim in sides:
        count = lax.axis_size(axis)
        ends = count - 1
        head = lax.slice_in_dim(cells, 0, width, axis=dim)
        tail = lax.slice_in_dim(cells, cells.shape[dim] - width, cells.shape[dim], axis=dim)
        cells = jnp.concatenate(
            [
                lax.ppermute(tail, axis, [(i, (i + 1) % count) for i in range(ends)]),
                cells,
                lax.ppermute(head, axis, [((i + 1) % count, i) for i in range(ends)]),
            ],
            axis=dim,
        )
    return cells


def copy_for_each(shard, axis):
    copies = jnp.broadcast_to(shard, (lax.axis_size(axis), *shard.shape))
    return lax.all_to_all(copies, axis, split_axis=0, concat_axis=0, tiled=True)


def taken_together(shard, axis):
    return copy_for_each(shard, axis).sum(axis=0)


def packed_total(arrays, axis):
    vector, at, finished = (jnp.concatenate([a.reshape(-1) for a in arrays]), 0, [])
    so_far = taken_together(vector, axis)
    for a in arrays:
        finished.append(so_far[at : at + a.size].reshape(a.shape))
        at += a.size
    return tuple(finished)


def shifts(frequency):
    angles = frequency.astype(jnp.float32) * (2.0 * math.pi / L)
    decay_rate = wrap_factor ** (1.0 / L)
    shift_re = (1.0 - decay_rate * jnp.cos(angles)) / step_size
    shift_im = decay_rate * jnp.sin(angles) / step_size
    return (shift_re, shift_im)


def near_sum(padded):
    interior = padded[..., 1:-1, :, :]
    widths = [(0, 0)] * (interior.ndim - 2) + [(1, 1), (1, 1)]
    padded_xy = jnp.pad(interior, widths)
    summed = padded[..., 2:, :, :] + padded[..., :-2, :, :]
    summed = summed + padded_xy[..., 2:, 1:-1] + padded_xy[..., :-2, 1:-1]
    summed = summed + padded_xy[..., 1:-1, 2:] + padded_xy[..., 1:-1, :-2]
    return summed


def advance(carried, dir_re, dir_im, img_re, img_im, coef_re, coef_im):
    sol_re, sol_im, res_re, res_im = carried
    sol_re = sol_re + coef_re * dir_re - coef_im * dir_im
    sol_im = sol_im + coef_re * dir_im + coef_im * dir_re
    res_re = res_re - (coef_re * img_re - coef_im * img_im)
    res_im = res_im - (coef_re * img_im + coef_im * img_re)
    return (sol_re, sol_im, res_re, res_im)


def solve_together(spectrum, absorption, frequencies, step_counts, longest):
    shift_re, shift_im = shifts(frequencies)
    shift_re = shift_re[:, None, None, None]
    shift_im = shift_im[:, None, None, None]
    diag_re = shift_re + 6.0 + absorption[None]
    magnitude = diag_re * diag_re + shift_im * shift_im
    inv_re = diag_re / magnitude
    inv_im = -shift_im / magnitude

    def iterate(iteration, carried):
        res_re, res_im = (carried[2], carried[3])
        dir_re = inv_re * res_re - inv_im * res_im
        dir_im = inv_re * res_im + inv_im * res_re
        padded = with_halo(jnp.stack([dir_re, dir_im], axis=1), ((SPACE, 2),), 1)
        nearby = near_sum(padded)
        img_re = diag_re * dir_re - shift_im * dir_im - nearby[:, 0]
        img_im = diag_re * dir_im + shift_im * dir_re - nearby[:, 1]
        totals = packed_total(
            (
                jnp.sum(img_re * res_re + img_im * res_im, axis=(1, 2, 3)),
                jnp.sum(img_re * res_im - img_im * res_re, axis=(1, 2, 3)),
                jnp.sum(img_re * img_re + img_im * img_im, axis=(1, 2, 3)),
            ),
            SPACE,
        )
        active = iteration < step_counts
        denominator = totals[2] + norm_floor
        coef_re = jnp.where(active, totals[0] / denominator, 0.0)[:, None, None, None]
        coef_im = jnp.where(active, totals[1] / denominator, 0.0)[:, None, None, None]
        return advance(carried, dir_re, dir_im, img_re, img_im, coef_re, coef_im)

    blank = jnp.zeros_like(spectrum[:, 0])
    finished = lax.fori_loop(0, longest, iterate, (blank, blank, spectrum[:, 0], spectrum[:, 1]))
    return jnp.stack([finished[0], finished[1]], axis=1)


def slot_order():
    return jnp.arange(L, dtype=jnp.int32)


def phase_table(left, right):
    return (left[:, None] * right[None, :] % L).astype(jnp.float32) * (2.0 * math.pi / L)


def stepwise(residual, absorption, counts):
    per_device = residual.shape[0]
    decay_rate = wrap_factor ** (1.0 / L)
    first_step = lax.axis_index(TM) * per_device
    times_here = first_step + jnp.arange(per_device, dtype=jnp.int32)
    scaled = residual * jnp.power(decay_rate, times_here.astype(jnp.float32))[:, None, None, None]
    slot_freqs = slot_order()
    own_freqs = lax.dynamic_slice_in_dim(slot_freqs, first_step, per_device)
    own_counts = counts[own_freqs]
    longest = jnp.max(counts)
    all_times = jnp.arange(L, dtype=jnp.int32)
    series = lax.all_to_all(scaled, TM, split_axis=2, concat_axis=0, tiled=True)
    phases = phase_table(slot_freqs, all_times)
    real_part = jnp.einsum("sn,nzxy->szxy", jnp.cos(phases), series, precision=highest)
    imag_part = -jnp.einsum("sn,nzxy->szxy", jnp.sin(phases), series, precision=highest)
    spectrum = lax.all_to_all(
        jnp.stack([real_part, imag_part], axis=1), TM, split_axis=0, concat_axis=3, tiled=True
    )
    solved = solve_together(spectrum, absorption, own_freqs, own_counts, longest)
    gathered = lax.all_to_all(solved, TM, split_axis=3, concat_axis=0, tiled=True)
    phases = phase_table(all_times, slot_freqs)
    values = jnp.einsum("ns,szxy->nzxy", jnp.cos(phases), gathered[:, 0], precision=highest)
    values = values - jnp.einsum(
        "ns,szxy->nzxy", jnp.sin(phases), gathered[:, 1], precision=highest
    )
    weight = jnp.power(decay_rate, -all_times.astype(jnp.float32)) / L
    values = values * weight[:, None, None, None]
    return lax.all_to_all(values, TM, split_axis=0, concat_axis=2, tiled=True)


def real_transform(x):
    n = len(x)
    if n == 2:
        return [(x[0] + x[1], None), (x[0] - x[1], None)]
    even, odd = real_transform(x[0::2]), real_transform(x[1::2])
    out = [None] * (n // 2 + 1)
    out[0] = (even[0][0] + odd[0][0], None)
    out[n // 2] = (even[0][0] - odd[0][0], None)
    out[n // 4] = (even[n // 4][0], -odd[n // 4][0])
    for k in range(1, n // 4):
        cos, sin = math.cos(2 * math.pi * k / n), math.sin(2 * math.pi * k / n)
        (er, ei), (cr, ci) = even[k], odd[k]
        tr, ti = cos * cr + sin * ci, cos * ci - sin * cr
        out[k] = (er + tr, ei + ti)
        out[n // 2 - k] = (er - tr, ti - ei)
    return out


def real_inverse(spectrum):
    n = 2 * (len(spectrum) - 1)
    first, last = spectrum[0][0], spectrum[n // 2][0]
    if n == 2:
        return [first + last, first - last]
    even, odd = [None] * (n // 4 + 1), [None] * (n // 4 + 1)
    even[0], odd[0] = (first + last, None), (first - last, None)
    mid_re, mid_im = spectrum[n // 4]
    even[n // 4], odd[n // 4] = (mid_re + mid_re, None), (-(mid_im + mid_im), None)
    for k in range(1, n // 4):
        cos, sin = math.cos(2 * math.pi * k / n), math.sin(2 * math.pi * k / n)
        (ar, ai), (br, bi) = spectrum[k], spectrum[n // 2 - k]
        even[k] = (ar + br, ai - bi)
        tr, ti = ar - br, ai + bi
        odd[k] = (cos * tr - sin * ti, cos * ti + sin * tr)
    halves = real_inverse(even), real_inverse(odd)
    return [halves[i % 2][i // 2] for i in range(n)]


def bands_kernel(x_ref, a_ref, out_ref, rows_ref, sems):
    copies = [
        pltpu.make_async_copy(x_ref.at[:, :, pl.ds(8 * band, 8), :], out_ref.at[band], sems.at[band]) for band in range(16)
    ]
    first = 16 * lax.axis_index("z") + 16 * lax.axis_index("core") - 8
    for core in range(2):
        row = pl.multiple_of(jnp.clip(first + 8 * core, 0, NX - 8), 8)
        copies.append(pltpu.make_async_copy(a_ref.at[:, pl.ds(row, 8), :], rows_ref.at[core], sems.at[16 + core]))
    for copy in copies:
        copy.start()
    for copy in copies:
        copy.wait()


def forward_kernel(x_ref, rows_ref, out_ref):
    for core in range(2):
        for zz in range(2):
            rows = rows_ref[core, zz]
            for slot in range(16 * core, 16 * core + 16):
                out_ref[slot, 4 + zz] = rows
    for zz in range(2):
        spectrum = real_transform([x_ref[n, zz] * decay**n for n in range(L)])
        out_ref[0, zz] = spectrum[0][0]
        out_ref[0, 2 + zz] = spectrum[PAIRS][0]
        for k in range(1, PAIRS):
            out_ref[k, zz] = spectrum[k][0]
            out_ref[k, 2 + zz] = spectrum[k][1]


def inverse_kernel(s_ref, out_ref, failed_ref):
    failed = jnp.zeros((8, 128), jnp.float32)
    for zz in range(2):
        ends = [s_ref[0, part, zz] for part in range(2)]
        spectrum = [(ends[0] + ends[0], None)]
        spectrum += [(s_ref[k, 0, zz], s_ref[k, 1, zz]) for k in range(1, PAIRS)]
        spectrum += [(ends[1] + ends[1], None)]
        values = real_inverse(spectrum)
        for n in range(L):
            out_ref[n, zz] = values[n] * (decay ** (-n) / (2 * L))
        failed = jnp.where(values[0] != values[0], 1.0, failed)
    failed_ref[0] = jnp.where(jnp.max(failed) > 0.0, 1, 0)


same = [(i, j) for i in range(STEPS + 1) for j in range(i, STEPS + 1)]
cross = [(i, j) for i in range(STEPS + 1) for j in range(i + 1, STEPS + 1)]
entry = {(kind, i, j): None for kind, ij in (("re", same), ("im", same), ("x", cross)) for i, j in ij}
for at, name in enumerate(entry):
    entry[name] = at


def tree_sum(terms):
    while len(terms) > 1:
        terms = [sum(terms[i : i + 2][1:], terms[i]) for i in range(0, len(terms), 2)]
    return terms[0]


def pick(slot, values):
    found = jnp.float32(values[0])
    for i in range(1, len(values)):
        found = jnp.where(slot == i, jnp.float32(values[i]), found)
    return found


def edges_kernel(own_ref, first_ref, second_ref, abs_ref):
    low = lax.axis_index("core") == 0
    for sp in range(16):
        for i in range(4):
            up, down = own_ref[1, sp, i, pl.ds(8 - HALO, HALO), :], own_ref[0, sp, i, pl.ds(0, HALO), :]
            first_ref[sp, pl.ds(HALO * i, HALO), :] = jnp.where(low, up, down)
            second_ref[sp, pl.ds(HALO * i, HALO), :] = jnp.where(low, down, up)
        for side in range(2):
            for zz in range(2):
                abs_ref[side, sp, zz] = own_ref[side, sp, 4 + zz]


def basis_kernel(own_ref, first_ref, second_ref, swap_ref, v_ref, inv_ref, gram_ref, u, edge_inv, sums):
    slot, z, core = lax.axis_index(SLOTS), lax.axis_index("z"), lax.axis_index("core")
    shifts_here = slot_shifts()
    shift_a, shift_b, shift_im = (pick(slot, shifts_here[:, i]) for i in range(3))
    lanes = lax.broadcasted_iota(jnp.int32, (8, 128), 1)
    first_lane, last_lane = lanes == 0, lanes == 127
    blank = jnp.zeros((8, 128), jnp.float32)

    for turn in range(2):
        for part in range(2):
            for row in range(8, 40, 8):
                u[turn, part, 0, pl.ds(row, 8), :] = blank
                u[turn, part, NZ + 1, pl.ds(row, 8), :] = blank

    def put(turn, tile, layer, inverse, re, im):
        a, b, c = inverse
        u[turn, 0, layer, pl.ds(8 + 8 * tile, 8), :] = a * re - c * im
        u[turn, 1, layer, pl.ds(8 + 8 * tile, 8), :] = b * im + c * re

    def prepare(sp, _):
        for turn in range(2):
            for part in range(2):
                for zz in range(2):
                    u[turn, part, 2 * sp + zz + 1, pl.ds(0, 8), :] = blank
                    u[turn, part, 2 * sp + zz + 1, pl.ds(40, 8), :] = blank
        for tile in range(4):
            for zz in range(2):
                mine, other = own_ref[tile // 2, sp, 4 + zz], swap_ref[tile // 2, sp, zz]
                base = jnp.where(core == tile % 2, mine, other)
                da, db = (shift_a + 6.0) + base, (shift_b + 6.0) + base
                ra, rb = 1.0 / (da * da + shift_im * shift_im), 1.0 / (db * db + shift_im * shift_im)
                found = [da * ra, db * rb, -shift_im * ra]
                if tile in (1, 2):
                    for i in range(3):
                        inv_ref[i, tile - 1, sp, zz] = found[i]
                    re, im = (own_ref[tile - 1, sp, 2 * part + zz] for part in range(2))
                else:
                    inside = z > 0 if tile == 0 else z < lax.axis_size("z") - 1
                    found = [jnp.where(inside, f, 0.0) for f in found]
                    for i in range(3):
                        edge_inv[i, tile // 3, sp, zz] = found[i]
                    pair = []
                    for part in range(2):
                        at = HALO * (2 * part + zz)
                        wanted = at - (8 - HALO) if tile == 0 else at
                        start = min(max(wanted, 0), 4 * HALO - 8)
                        first, second = (ref[sp, pl.ds(start, 8), :] for ref in (first_ref, second_ref))
                        rows = jnp.where((core == 0) == (tile == 0), first, second)
                        shift = (start - wanted) % 8
                        pair.append(pltpu.roll(rows, shift, 0) if shift else rows)
                    re, im = pair
                put(0, tile, 2 * sp + zz + 1, found, re, im)
        return 0

    lax.fori_loop(0, NZ // 2, prepare, 0, unroll=4)

    def vector(j, side, sp, zz):
        if j == 0:
            return [own_ref[side, sp, 2 * part + zz] for part in range(2)]
        return [v_ref[j - 1, part, side, sp, zz] for part in range(2)]

    for j in range(STEPS):
        names = [name for name in entry if name[2] == j + 1 or (j == 0 and name[2] == 0)]

        def step(group, totals, j=j, names=names):
            by_layer = []
            for sp in [4 * group + s for s in range(4)]:
                found = {name: [] for name in names}
                for zz in range(2):
                    for tile in range(4) if j < STEPS - 1 else (1, 2):
                        layer, row = 2 * sp + zz + 1, 8 + 8 * tile
                        pair = []
                        for part in range(2):
                            old = u.at[j % 2, part]
                            here = old[layer, pl.ds(row, 8), :]
                            total = old[layer - 1, pl.ds(row, 8), :] + old[layer + 1, pl.ds(row, 8), :]
                            total = total + (old[layer, pl.ds(row - 1, 8), :] + old[layer, pl.ds(row + 1, 8), :])
                            total = total + (
                                jnp.where(first_lane, 0.0, pltpu.roll(here, 1, 1))
                                + jnp.where(last_lane, 0.0, pltpu.roll(here, 127, 1))
                            )
                            pair.append(total)
                        if tile in (1, 2):
                            side = tile - 1
                            if j < STEPS - 1:
                                for part in range(2):
                                    v_ref[j, part, side, sp, zz] = pair[part]
                            known = [vector(i, side, sp, zz) for i in range(j + 1)] + [pair]
                            for kind, i, k in names:
                                a, b = known[i], known[k]
                                if kind == "x":
                                    found[kind, i, k].append(a[0] * b[1] - a[1] * b[0])
                                else:
                                    part = ("re", "im").index(kind)
                                    found[kind, i, k].append(a[part] * b[part])
                        if j < STEPS - 1:
                            if tile in (1, 2):
                                inverse = [inv_ref[i, tile - 1, sp, zz] for i in range(3)]
                            else:
                                inverse = [edge_inv[i, tile // 3, sp, zz] for i in range(3)]
                            put((j + 1) % 2, tile, layer, inverse, *pair)
                by_layer.append([tree_sum(found[name]) for name in names])
            return tuple(t + tree_sum(list(parts)) for t, parts in zip(totals, zip(*by_layer)))

        totals = lax.fori_loop(0, NZ // 8, step, tuple(blank for _ in names), unroll=2)
        for name, total in zip(names, totals):
            sums[entry[name]] = total
    for spare in range(len(entry), sums.shape[0]):
        sums[spare] = blank

    rows = jnp.sum(sums[...], axis=1)
    column = jnp.sum(rows, axis=1, keepdims=True)
    where = lax.broadcasted_iota(jnp.int32, rows.shape, 0) == lax.broadcasted_iota(jnp.int32, rows.shape, 1)
    packed = jnp.sum(jnp.where(where, column, 0.0), axis=0, keepdims=True)
    gram_ref[...] = jnp.broadcast_to(packed[None], gram_ref.shape)


def multiplied(a, b):
    return (a[0] * b[0] - a[1] * b[1], a[0] * b[1] + a[1] * b[0])


def combine_kernel(count_ref, part_ref, own_ref, v_ref, inv_ref, out_ref):
    slot = lax.axis_index(SLOTS)
    ends = slot == 0
    low = lax.broadcasted_iota(jnp.int32, (8, 128), 1) < 64
    row = tree_sum([part_ref[i] for i in range(part_ref.shape[0])])

    def spread(name):
        return jnp.broadcast_to(row[:, entry[name] : entry[name] + 1], (8, 128))

    gram = {}
    for i, j in same:
        re, im = spread(("re", i, j)), spread(("im", i, j))
        real = jnp.where(ends, jnp.where(low, re, im), re + im)
        imag = jnp.where(ends, 0.0, spread(("x", i, j))) if j > i else jnp.zeros_like(real)
        gram[i, j] = (real, imag)

    count_lane = lax.broadcasted_iota(jnp.int32, (1, L), 1)
    count_a, count_b = (
        jnp.sum(jnp.where(count_lane == k, count_ref[...], 0).astype(jnp.float32), axis=1, keepdims=True)
        for k in (slot, jnp.where(ends, PAIRS, L - slot))
    )
    one, none = jnp.ones((8, 128), jnp.float32), jnp.zeros((8, 128), jnp.float32)
    poly, answer = [(one, none)], [(none, none) for _ in range(STEPS)]
    sizes = [jnp.sqrt(jnp.maximum(gram[i, i][0], 0.0)) for i in range(STEPS + 1)]
    doubt, scale = none, None
    for m in range(STEPS):
        in_a, in_b = (jnp.broadcast_to(jnp.where(m < count, 1.0, 0.0), (8, 128)) for count in (count_a, count_b))
        weight = jnp.where(ends, jnp.where(low, in_a, in_b), in_a + in_b)
        g00, g01, g11 = gram[0, 0][0], gram[0, 1], gram[1, 1][0]
        denominator = (g00 - 2.0 * g01[0] + g11) + norm_floor
        inverse = 1.0 / denominator
        coef = ((g00 - g01[0]) * inverse, g01[1] * inverse)
        size = jnp.abs(coef[0]) + jnp.abs(coef[1])
        length = jnp.sqrt(jnp.maximum(g00, 0.0))
        if m == 0:
            scale = size * length
        pair = sizes[0] + sizes[1]
        step_doubt = (gram_rounding * (1 + m / 2)) * pair * (sizes[0] + size * pair) * jnp.abs(inverse) * length
        doubt = doubt + jnp.where(weight > 0.0, step_doubt, none)
        for j, p in enumerate(poly):
            term = multiplied(coef, p)
            answer[j] = (answer[j][0] + weight * term[0], answer[j][1] + weight * term[1])
        if m == STEPS - 1:
            break
        rest = (1.0 - coef[0], -coef[1])
        padded = [None] + poly + [None]
        following = []
        for j in range(len(poly) + 1):
            kept = multiplied(rest, poly[j]) if j < len(poly) else (none, none)
            moved = multiplied(coef, poly[j - 1]) if j > 0 else (none, none)
            following.append((kept[0] + moved[0], kept[1] + moved[1]))
        poly = following
        rr = rest[0] * rest[0] + rest[1] * rest[1]
        cc = coef[0] * coef[0] + coef[1] * coef[1]
        rc = multiplied((rest[0], -rest[1]), coef)
        cr = (rc[0], -rc[1])
        size_rest = jnp.abs(rest[0]) + jnp.abs(rest[1])
        sizes = [size_rest * a + size * b for a, b in zip(sizes[:-1], sizes[1:])]

        def at(i, j):
            return gram[i, j] if i <= j else (gram[j, i][0], -gram[j, i][1])

        shrunk = {}
        top = STEPS - m
        for i in range(top):
            for j in range(i, top):
                a, b, d = at(i, j), at(i, j + 1), at(i + 1, j + 1)
                if i == j:
                    ab = multiplied(rc, b)
                    shrunk[i, j] = (rr * a[0] + 2.0 * ab[0] + cc * d[0], none)
                else:
                    ab, ac = multiplied(rc, b), multiplied(cr, at(i + 1, j))
                    shrunk[i, j] = tuple(rr * a[x] + (ab[x] + ac[x]) + cc * d[x] for x in range(2))
        gram = shrunk

    trusted = doubt <= error_allowed * scale
    weights = []
    for re, im in answer:
        re = jnp.where(trusted, re, jnp.nan)
        weights.append(
            (
                jnp.broadcast_to(re[:, 0:1], (8, 128)),
                jnp.broadcast_to(re[:, 127:128], (8, 128)),
                jnp.broadcast_to(im[:, 0:1], (8, 128)),
            )
        )

    def finish(sp, _):
        for side in range(2):
            for zz in range(2):
                res, ims = [], []
                for j, (wa, wb, wi) in enumerate(weights):
                    re, im = ((own_ref[side, sp, 2 * part + zz] if j == 0 else v_ref[j - 1, part, side, sp, zz]) for part in range(2))
                    res.append(wa * re - wi * im)
                    ims.append(wb * im + wi * re)
                re, im = tree_sum(res), tree_sum(ims)
                a, b, c = (inv_ref[i, side, sp, zz] for i in range(3))
                out_ref[16 * side + sp, 0, zz] = a * re - c * im
                out_ref[16 * side + sp, 1, zz] = b * im + c * re
        return 0

    lax.fori_loop(0, NZ // 2, finish, 0, unroll=2)


def slot_shifts():
    table = np.zeros((PAIRS, 4), np.float32)
    for slot in range(PAIRS):
        angle = 2 * math.pi * slot / L
        table[slot, :2] = (1 - decay * math.cos(angle)) / step_size
        table[slot, 2] = decay * math.sin(angle) / step_size
    table[0, 1] = (1 + decay) / step_size
    return table


def exchanged(blocks, axes):
    return lax.all_to_all(blocks, axes, split_axis=0, concat_axis=0, tiled=True)


VMEM = pl.BlockSpec(memory_space=pltpu.VMEM)
SMEM = pl.BlockSpec(memory_space=pltpu.SMEM)
ANY = pl.BlockSpec(memory_space=pl.ANY)


def f32(*shape):
    return pltpu.VMEM(shape, jnp.float32)


def held(x):
    return pltpu.with_memory_space_constraint(x, pltpu.MemorySpace.VMEM)


def in_hbm(x):
    return pltpu.with_memory_space_constraint(x, pltpu.MemorySpace.HBM)


def room(mebibytes):
    return pltpu.CompilerParams(vmem_limit_bytes=mebibytes * 2**20)


def together(residual, absorption, counts):
    chips = lax.axis_size("z")
    bands, rows = pl.pallas_call(
        bands_kernel,
        out_shape=(f32(16, 4, 2, 8, 128), f32(2, 2, 8, 128)),
        in_specs=[ANY, ANY],
        out_specs=(VMEM, VMEM),
        scratch_shapes=[pltpu.SemaphoreType.DMA((18,))],
        compiler_params=room(2),
        name="bands",
    )(in_hbm(residual), in_hbm(absorption))
    series = exchanged(bands, TM).reshape(L, 2, 8, 128)
    spectrum = pl.pallas_call(
        forward_kernel,
        out_shape=f32(PAIRS, 6, 8, 128),
        in_specs=[VMEM, VMEM],
        out_specs=VMEM,
        compiler_params=room(4),
        name="forward",
    )(held(series), held(rows))
    own = held(exchanged(spectrum, SLOTS).reshape(2, 16, 6, 8, 128))
    first, second, swap = pl.pallas_call(
        edges_kernel,
        out_shape=(f32(16, 4 * HALO, 128), f32(16, 4 * HALO, 128), f32(2, 16, 2, 8, 128)),
        in_specs=[VMEM],
        out_specs=(VMEM, VMEM, VMEM),
        compiler_params=room(2),
        name="edges",
    )(own)
    ups = [[(2 * i + core, 2 * i + 2 + core) for i in range(chips - 1)] for core in range(2)]
    downs = [[(b, a) for a, b in pairs] for pairs in ups]
    swap = lax.ppermute(swap, "core", [(0, 1), (1, 0)])
    first = lax.ppermute(first, TM, ups[0] + downs[1])
    second = lax.ppermute(second, TM, downs[0] + ups[1])
    basis, inverses, partial = pl.pallas_call(
        basis_kernel,
        out_shape=(f32(STEPS - 1, 2, 2, 16, 2, 8, 128), f32(3, 2, 16, 2, 8, 128), f32(8, 8, 128)),
        in_specs=[VMEM, VMEM, VMEM, VMEM],
        out_specs=(VMEM, VMEM, VMEM),
        scratch_shapes=[
            pltpu.VMEM((2, 2, NZ + 2, 48, 128), jnp.float32),
            pltpu.VMEM((3, 2, 16, 2, 8, 128), jnp.float32),
            pltpu.VMEM((80, 8, 128), jnp.float32),
        ],
        compiler_params=room(10),
        name="basis",
    )(own, held(first), held(second), held(swap))
    partials = exchanged(partial, "z")
    solved = pl.pallas_call(
        combine_kernel,
        out_shape=f32(PAIRS, 2, 2, 8, 128),
        in_specs=[VMEM, VMEM, VMEM, VMEM, VMEM],
        out_specs=VMEM,
        compiler_params=room(6),
        name="combine",
    )(held(counts.reshape(1, L)), held(partials), own, held(basis), held(inverses))
    gathered = exchanged(solved, SLOTS)
    values, failed = pl.pallas_call(
        inverse_kernel,
        out_shape=(f32(L, 2, 8, 128), pltpu.SMEM((1,), jnp.int32)),
        in_specs=[VMEM],
        out_specs=(VMEM, SMEM),
        compiler_params=room(4),
        name="inverse",
    )(held(gathered))
    return values, failed


def taken_kernel(*refs):
    count = len(refs) // 2
    copies = [pltpu.make_async_copy(refs[i], refs[count + i], refs[-1].at[i]) for i in range(count)]
    for copy in copies:
        copy.start()
    for copy in copies:
        copy.wait()


def taken(*arrays):
    return pl.pallas_call(
        taken_kernel,
        out_shape=tuple(f32(*a.shape) for a in arrays),
        in_specs=[ANY] * len(arrays),
        out_specs=(VMEM,) * len(arrays),
        scratch_shapes=[pltpu.SemaphoreType.DMA((len(arrays),))],
        compiler_params=room(2),
        name="taken",
    )(*(in_hbm(a) for a in arrays))


def to_steps(values, shape):
    bands = exchanged(values.reshape(16, 4, 2, 8, 128), TM)
    return bands.transpose(1, 2, 0, 3, 4).reshape(shape)


def body(residual, absorption, counts):
    values, failed = together(residual, absorption, counts)
    return lax.cond(
        failed[0] > 0,
        lambda r, a, c, v: stepwise(*taken(r, a), c),
        lambda r, a, c, v: to_steps(v, r.shape),
        residual, absorption, counts, values,
    )


def solution(mesh):
    chips, cores = mesh.shape["tm"] // 2, 2
    devices = mesh.devices.reshape(chips, cores, 4, 4)
    inner = Mesh(devices, ("z", "core", "y", "x"))
    in_specs = (P(TM, SPACE, None, None), P(SPACE, None, None), P())
    out_specs = P(TM, SPACE, None, None)
    return jax.shard_map(body, mesh=inner, in_specs=in_specs, out_specs=out_specs, check_vma=False)
```

```python
import math

import jax
import jax.numpy as jnp
import numpy as np
from jax import lax
from jax.experimental import pallas as pl
from jax.experimental.pallas import tpu as pltpu
from jax.sharding import Mesh
from jax.sharding import PartitionSpec as P

L = 64
STEPS = 6
HALO = 6
NX = 128
NZ = 32
PAIRS = L // 2
TM = ("z", "core")
SPACE = ("y", "x")
SLOTS = ("core", "y", "x")

wrap_factor = 0.1
step_size = 1.0
norm_floor = 1e-06
highest = lax.Precision.HIGHEST
decay = wrap_factor ** (1.0 / L)

gram_rounding = 1e-6
error_allowed = 1.5e-4


def with_halo(cells, sides, width):
    for axis, dim in sides:
        count = lax.axis_size(axis)
        ends = count - 1
        head = lax.slice_in_dim(cells, 0, width, axis=dim)
        tail = lax.slice_in_dim(cells, cells.shape[dim] - width, cells.shape[dim], axis=dim)
        cells = jnp.concatenate(
            [
                lax.ppermute(tail, axis, [(i, (i + 1) % count) for i in range(ends)]),
                cells,
                lax.ppermute(head, axis, [((i + 1) % count, i) for i in range(ends)]),
            ],
            axis=dim,
        )
    return cells


def copy_for_each(shard, axis):
    copies = jnp.broadcast_to(shard, (lax.axis_size(axis), *shard.shape))
    return lax.all_to_all(copies, axis, split_axis=0, concat_axis=0, tiled=True)


def taken_together(shard, axis):
    return copy_for_each(shard, axis).sum(axis=0)


def packed_total(arrays, axis):
    vector, at, finished = (jnp.concatenate([a.reshape(-1) for a in arrays]), 0, [])
    so_far = taken_together(vector, axis)
    for a in arrays:
        finished.append(so_far[at : at + a.size].reshape(a.shape))
        at += a.size
    return tuple(finished)


def shifts(frequency):
    angles = frequency.astype(jnp.float32) * (2.0 * math.pi / L)
    decay_rate = wrap_factor ** (1.0 / L)
    shift_re = (1.0 - decay_rate * jnp.cos(angles)) / step_size
    shift_im = decay_rate * jnp.sin(angles) / step_size
    return (shift_re, shift_im)


def near_sum(padded):
    interior = padded[..., 1:-1, :, :]
    widths = [(0, 0)] * (interior.ndim - 2) + [(1, 1), (1, 1)]
    padded_xy = jnp.pad(interior, widths)
    summed = padded[..., 2:, :, :] + padded[..., :-2, :, :]
    summed = summed + padded_xy[..., 2:, 1:-1] + padded_xy[..., :-2, 1:-1]
    summed = summed + padded_xy[..., 1:-1, 2:] + padded_xy[..., 1:-1, :-2]
    return summed


def advance(carried, dir_re, dir_im, img_re, img_im, coef_re, coef_im):
    sol_re, sol_im, res_re, res_im = carried
    sol_re = sol_re + coef_re * dir_re - coef_im * dir_im
    sol_im = sol_im + coef_re * dir_im + coef_im * dir_re
    res_re = res_re - (coef_re * img_re - coef_im * img_im)
    res_im = res_im - (coef_re * img_im + coef_im * img_re)
    return (sol_re, sol_im, res_re, res_im)


def solve_together(spectrum, absorption, frequencies, step_counts, longest):
    shift_re, shift_im = shifts(frequencies)
    shift_re = shift_re[:, None, None, None]
    shift_im = shift_im[:, None, None, None]
    diag_re = shift_re + 6.0 + absorption[None]
    magnitude = diag_re * diag_re + shift_im * shift_im
    inv_re = diag_re / magnitude
    inv_im = -shift_im / magnitude

    def iterate(iteration, carried):
        res_re, res_im = (carried[2], carried[3])
        dir_re = inv_re * res_re - inv_im * res_im
        dir_im = inv_re * res_im + inv_im * res_re
        padded = with_halo(jnp.stack([dir_re, dir_im], axis=1), ((SPACE, 2),), 1)
        nearby = near_sum(padded)
        img_re = diag_re * dir_re - shift_im * dir_im - nearby[:, 0]
        img_im = diag_re * dir_im + shift_im * dir_re - nearby[:, 1]
        totals = packed_total(
            (
                jnp.sum(img_re * res_re + img_im * res_im, axis=(1, 2, 3)),
                jnp.sum(img_re * res_im - img_im * res_re, axis=(1, 2, 3)),
                jnp.sum(img_re * img_re + img_im * img_im, axis=(1, 2, 3)),
            ),
            SPACE,
        )
        active = iteration < step_counts
        denominator = totals[2] + norm_floor
        coef_re = jnp.where(active, totals[0] / denominator, 0.0)[:, None, None, None]
        coef_im = jnp.where(active, totals[1] / denominator, 0.0)[:, None, None, None]
        return advance(carried, dir_re, dir_im, img_re, img_im, coef_re, coef_im)

    blank = jnp.zeros_like(spectrum[:, 0])
    finished = lax.fori_loop(0, longest, iterate, (blank, blank, spectrum[:, 0], spectrum[:, 1]))
    return jnp.stack([finished[0], finished[1]], axis=1)


def slot_order():
    return jnp.arange(L, dtype=jnp.int32)


def phase_table(left, right):
    return (left[:, None] * right[None, :] % L).astype(jnp.float32) * (2.0 * math.pi / L)


def stepwise(residual, absorption, counts):
    per_device = residual.shape[0]
    decay_rate = wrap_factor ** (1.0 / L)
    first_step = lax.axis_index(TM) * per_device
    times_here = first_step + jnp.arange(per_device, dtype=jnp.int32)
    scaled = residual * jnp.power(decay_rate, times_here.astype(jnp.float32))[:, None, None, None]
    slot_freqs = slot_order()
    own_freqs = lax.dynamic_slice_in_dim(slot_freqs, first_step, per_device)
    own_counts = counts[own_freqs]
    longest = jnp.max(counts)
    all_times = jnp.arange(L, dtype=jnp.int32)
    series = lax.all_to_all(scaled, TM, split_axis=2, concat_axis=0, tiled=True)
    phases = phase_table(slot_freqs, all_times)
    real_part = jnp.einsum("sn,nzxy->szxy", jnp.cos(phases), series, precision=highest)
    imag_part = -jnp.einsum("sn,nzxy->szxy", jnp.sin(phases), series, precision=highest)
    spectrum = lax.all_to_all(
        jnp.stack([real_part, imag_part], axis=1), TM, split_axis=0, concat_axis=3, tiled=True
    )
    solved = solve_together(spectrum, absorption, own_freqs, own_counts, longest)
    gathered = lax.all_to_all(solved, TM, split_axis=3, concat_axis=0, tiled=True)
    phases = phase_table(all_times, slot_freqs)
    values = jnp.einsum("ns,szxy->nzxy", jnp.cos(phases), gathered[:, 0], precision=highest)
    values = values - jnp.einsum(
        "ns,szxy->nzxy", jnp.sin(phases), gathered[:, 1], precision=highest
    )
    weight = jnp.power(decay_rate, -all_times.astype(jnp.float32)) / L
    values = values * weight[:, None, None, None]
    return lax.all_to_all(values, TM, split_axis=0, concat_axis=2, tiled=True)


def real_transform(x):
    n = len(x)
    if n == 2:
        return [(x[0] + x[1], None), (x[0] - x[1], None)]
    even, odd = real_transform(x[0::2]), real_transform(x[1::2])
    out = [None] * (n // 2 + 1)
    out[0] = (even[0][0] + odd[0][0], None)
    out[n // 2] = (even[0][0] - odd[0][0], None)
    out[n // 4] = (even[n // 4][0], -odd[n // 4][0])
    for k in range(1, n // 4):
        cos, sin = math.cos(2 * math.pi * k / n), math.sin(2 * math.pi * k / n)
        (er, ei), (cr, ci) = even[k], odd[k]
        tr, ti = cos * cr + sin * ci, cos * ci - sin * cr
        out[k] = (er + tr, ei + ti)
        out[n // 2 - k] = (er - tr, ti - ei)
    return out


def real_inverse(spectrum):
    n = 2 * (len(spectrum) - 1)
    first, last = spectrum[0][0], spectrum[n // 2][0]
    if n == 2:
        return [first + last, first - last]
    even, odd = [None] * (n // 4 + 1), [None] * (n // 4 + 1)
    even[0], odd[0] = (first + last, None), (first - last, None)
    mid_re, mid_im = spectrum[n // 4]
    even[n // 4], odd[n // 4] = (mid_re + mid_re, None), (-(mid_im + mid_im), None)
    for k in range(1, n // 4):
        cos, sin = math.cos(2 * math.pi * k / n), math.sin(2 * math.pi * k / n)
        (ar, ai), (br, bi) = spectrum[k], spectrum[n // 2 - k]
        even[k] = (ar + br, ai - bi)
        tr, ti = ar - br, ai + bi
        odd[k] = (cos * tr - sin * ti, cos * ti + sin * tr)
    halves = real_inverse(even), real_inverse(odd)
    return [halves[i % 2][i // 2] for i in range(n)]


def bands_kernel(x_ref, a_ref, out_ref, rows_ref, sems):
    copies = [
        pltpu.make_async_copy(x_ref.at[:, :, pl.ds(8 * band, 8), :], out_ref.at[band], sems.at[band]) for band in range(16)
    ]
    first = 16 * lax.axis_index("z") + 16 * lax.axis_index("core") - 8
    for core in range(2):
        row = pl.multiple_of(jnp.clip(first + 8 * core, 0, NX - 8), 8)
        copies.append(pltpu.make_async_copy(a_ref.at[:, pl.ds(row, 8), :], rows_ref.at[core], sems.at[16 + core]))
    for copy in copies:
        copy.start()
    for copy in copies:
        copy.wait()


def forward_kernel(x_ref, out_ref):
    for zz in range(2):
        spectrum = real_transform([x_ref[n, zz] * decay**n for n in range(L)])
        out_ref[0, zz] = spectrum[0][0]
        out_ref[0, 2 + zz] = spectrum[PAIRS][0]
        for k in range(1, PAIRS):
            out_ref[k, zz] = spectrum[k][0]
            out_ref[k, 2 + zz] = spectrum[k][1]


def inverse_kernel(s_ref, out_ref, failed_ref):
    failed = jnp.zeros((8, 128), jnp.float32)
    for zz in range(2):
        ends = [s_ref[0, part, zz] for part in range(2)]
        spectrum = [(ends[0] + ends[0], None)]
        spectrum += [(s_ref[k, 0, zz], s_ref[k, 1, zz]) for k in range(1, PAIRS)]
        spectrum += [(ends[1] + ends[1], None)]
        values = real_inverse(spectrum)
        for n in range(L):
            out_ref[n, zz] = values[n] * (decay ** (-n) / (2 * L))
        failed = jnp.where(values[0] != values[0], 1.0, failed)
    failed_ref[0] = jnp.where(jnp.max(failed) > 0.0, 1, 0)


same = [(i, j) for i in range(STEPS + 1) for j in range(i, STEPS + 1)]
cross = [(i, j) for i in range(STEPS + 1) for j in range(i + 1, STEPS + 1)]
entry = {(kind, i, j): None for kind, ij in (("re", same), ("im", same), ("x", cross)) for i, j in ij}
for at, name in enumerate(entry):
    entry[name] = at


def tree_sum(terms):
    while len(terms) > 1:
        terms = [sum(terms[i : i + 2][1:], terms[i]) for i in range(0, len(terms), 2)]
    return terms[0]


def pick(slot, values):
    found = jnp.float32(values[0])
    for i in range(1, len(values)):
        found = jnp.where(slot == i, jnp.float32(values[i]), found)
    return found


def edges_kernel(own_ref, first_ref, second_ref):
    low = lax.axis_index("core") == 0
    for sp in range(16):
        for i in range(4):
            up, down = own_ref[1, sp, i, pl.ds(8 - HALO, HALO), :], own_ref[0, sp, i, pl.ds(0, HALO), :]
            first_ref[sp, pl.ds(HALO * i, HALO), :] = jnp.where(low, up, down)
            second_ref[sp, pl.ds(HALO * i, HALO), :] = jnp.where(low, down, up)


def basis_kernel(own_ref, first_ref, second_ref, abs_ref, swap_ref, v_ref, inv_ref, gram_ref, u, edge_inv, sums):
    slot, z, core = lax.axis_index(SLOTS), lax.axis_index("z"), lax.axis_index("core")
    home = lax.axis_index(SPACE)
    shifts_here = slot_shifts()
    shift_a, shift_b, shift_im = (pick(slot, shifts_here[:, i]) for i in range(3))
    lanes = lax.broadcasted_iota(jnp.int32, (8, 128), 1)
    first_lane, last_lane = lanes == 0, lanes == 127
    blank = jnp.zeros((8, 128), jnp.float32)

    for turn in range(2):
        for part in range(2):
            for row in range(8, 40, 8):
                u[turn, part, 0, pl.ds(row, 8), :] = blank
                u[turn, part, NZ + 1, pl.ds(row, 8), :] = blank

    def put(turn, tile, layer, inverse, re, im):
        a, b, c = inverse
        u[turn, 0, layer, pl.ds(8 + 8 * tile, 8), :] = a * re - c * im
        u[turn, 1, layer, pl.ds(8 + 8 * tile, 8), :] = b * im + c * re

    def prepare(sp, _):
        for turn in range(2):
            for part in range(2):
                for zz in range(2):
                    u[turn, part, 2 * sp + zz + 1, pl.ds(0, 8), :] = blank
                    u[turn, part, 2 * sp + zz + 1, pl.ds(40, 8), :] = blank
        for tile in range(4):
            for zz in range(2):
                mine, other = (ref[sp ^ home, tile % 2, zz] for ref in (abs_ref, swap_ref))
                base = jnp.where(core == tile // 2, mine, other)
                da, db = (shift_a + 6.0) + base, (shift_b + 6.0) + base
                ra, rb = 1.0 / (da * da + shift_im * shift_im), 1.0 / (db * db + shift_im * shift_im)
                found = [da * ra, db * rb, -shift_im * ra]
                if tile in (1, 2):
                    for i in range(3):
                        inv_ref[i, tile - 1, sp, zz] = found[i]
                    re, im = (own_ref[tile - 1, sp, 2 * part + zz] for part in range(2))
                else:
                    inside = z > 0 if tile == 0 else z < lax.axis_size("z") - 1
                    found = [jnp.where(inside, f, 0.0) for f in found]
                    for i in range(3):
                        edge_inv[i, tile // 3, sp, zz] = found[i]
                    pair = []
                    for part in range(2):
                        at = HALO * (2 * part + zz)
                        wanted = at - (8 - HALO) if tile == 0 else at
                        start = min(max(wanted, 0), 4 * HALO - 8)
                        first, second = (ref[sp, pl.ds(start, 8), :] for ref in (first_ref, second_ref))
                        rows = jnp.where((core == 0) == (tile == 0), first, second)
                        shift = (start - wanted) % 8
                        pair.append(pltpu.roll(rows, shift, 0) if shift else rows)
                    re, im = pair
                put(0, tile, 2 * sp + zz + 1, found, re, im)
        return 0

    lax.fori_loop(0, NZ // 2, prepare, 0, unroll=4)

    def vector(j, side, sp, zz):
        if j == 0:
            return [own_ref[side, sp, 2 * part + zz] for part in range(2)]
        return [v_ref[j - 1, part, side, sp, zz] for part in range(2)]

    for j in range(STEPS):
        names = [name for name in entry if name[2] == j + 1 or (j == 0 and name[2] == 0)]

        def step(group, totals, j=j, names=names):
            by_layer = []
            for sp in [4 * group + s for s in range(4)]:
                found = {name: [] for name in names}
                for zz in range(2):
                    for tile in range(4) if j < STEPS - 1 else (1, 2):
                        layer, row = 2 * sp + zz + 1, 8 + 8 * tile
                        pair = []
                        for part in range(2):
                            old = u.at[j % 2, part]
                            here = old[layer, pl.ds(row, 8), :]
                            total = old[layer - 1, pl.ds(row, 8), :] + old[layer + 1, pl.ds(row, 8), :]
                            total = total + (old[layer, pl.ds(row - 1, 8), :] + old[layer, pl.ds(row + 1, 8), :])
                            total = total + (
                                jnp.where(first_lane, 0.0, pltpu.roll(here, 1, 1))
                                + jnp.where(last_lane, 0.0, pltpu.roll(here, 127, 1))
                            )
                            pair.append(total)
                        if tile in (1, 2):
                            side = tile - 1
                            if j < STEPS - 1:
                                for part in range(2):
                                    v_ref[j, part, side, sp, zz] = pair[part]
                            known = [vector(i, side, sp, zz) for i in range(j + 1)] + [pair]
                            for kind, i, k in names:
                                a, b = known[i], known[k]
                                if kind == "x":
                                    found[kind, i, k].append(a[0] * b[1] - a[1] * b[0])
                                else:
                                    part = ("re", "im").index(kind)
                                    found[kind, i, k].append(a[part] * b[part])
                        if j < STEPS - 1:
                            if tile in (1, 2):
                                inverse = [inv_ref[i, tile - 1, sp, zz] for i in range(3)]
                            else:
                                inverse = [edge_inv[i, tile // 3, sp, zz] for i in range(3)]
                            put((j + 1) % 2, tile, layer, inverse, *pair)
                by_layer.append([tree_sum(found[name]) for name in names])
            return tuple(t + tree_sum(list(parts)) for t, parts in zip(totals, zip(*by_layer)))

        totals = lax.fori_loop(0, NZ // 8, step, tuple(blank for _ in names), unroll=2)
        for name, total in zip(names, totals):
            sums[entry[name]] = total
    for spare in range(len(entry), sums.shape[0]):
        sums[spare] = blank

    rows = jnp.sum(sums[...], axis=1)
    column = jnp.sum(rows, axis=1, keepdims=True)
    where = lax.broadcasted_iota(jnp.int32, rows.shape, 0) == lax.broadcasted_iota(jnp.int32, rows.shape, 1)
    packed = jnp.sum(jnp.where(where, column, 0.0), axis=0, keepdims=True)
    gram_ref[...] = jnp.broadcast_to(packed[None], gram_ref.shape)


def multiplied(a, b):
    return (a[0] * b[0] - a[1] * b[1], a[0] * b[1] + a[1] * b[0])


def combine_kernel(count_ref, part_ref, own_ref, v_ref, inv_ref, out_ref):
    slot = lax.axis_index(SLOTS)
    ends = slot == 0
    low = lax.broadcasted_iota(jnp.int32, (8, 128), 1) < 64
    row = tree_sum([part_ref[i] for i in range(part_ref.shape[0])])

    def spread(name):
        return jnp.broadcast_to(row[:, entry[name] : entry[name] + 1], (8, 128))

    gram = {}
    for i, j in same:
        re, im = spread(("re", i, j)), spread(("im", i, j))
        real = jnp.where(ends, jnp.where(low, re, im), re + im)
        imag = jnp.where(ends, 0.0, spread(("x", i, j))) if j > i else jnp.zeros_like(real)
        gram[i, j] = (real, imag)

    count_lane = lax.broadcasted_iota(jnp.int32, (1, L), 1)
    count_a, count_b = (
        jnp.sum(jnp.where(count_lane == k, count_ref[...], 0).astype(jnp.float32), axis=1, keepdims=True)
        for k in (slot, jnp.where(ends, PAIRS, L - slot))
    )
    one, none = jnp.ones((8, 128), jnp.float32), jnp.zeros((8, 128), jnp.float32)
    poly, answer = [(one, none)], [(none, none) for _ in range(STEPS)]
    sizes = [jnp.sqrt(jnp.maximum(gram[i, i][0], 0.0)) for i in range(STEPS + 1)]
    doubt, scale = none, None
    for m in range(STEPS):
        in_a, in_b = (jnp.broadcast_to(jnp.where(m < count, 1.0, 0.0), (8, 128)) for count in (count_a, count_b))
        weight = jnp.where(ends, jnp.where(low, in_a, in_b), in_a + in_b)
        g00, g01, g11 = gram[0, 0][0], gram[0, 1], gram[1, 1][0]
        denominator = (g00 - 2.0 * g01[0] + g11) + norm_floor
        inverse = 1.0 / denominator
        coef = ((g00 - g01[0]) * inverse, g01[1] * inverse)
        size = jnp.abs(coef[0]) + jnp.abs(coef[1])
        length = jnp.sqrt(jnp.maximum(g00, 0.0))
        if m == 0:
            scale = size * length
        pair = sizes[0] + sizes[1]
        step_doubt = (gram_rounding * (1 + m / 2)) * pair * (sizes[0] + size * pair) * jnp.abs(inverse) * length
        doubt = doubt + jnp.where(weight > 0.0, step_doubt, none)
        for j, p in enumerate(poly):
            term = multiplied(coef, p)
            answer[j] = (answer[j][0] + weight * term[0], answer[j][1] + weight * term[1])
        if m == STEPS - 1:
            break
        rest = (1.0 - coef[0], -coef[1])
        padded = [None] + poly + [None]
        following = []
        for j in range(len(poly) + 1):
            kept = multiplied(rest, poly[j]) if j < len(poly) else (none, none)
            moved = multiplied(coef, poly[j - 1]) if j > 0 else (none, none)
            following.append((kept[0] + moved[0], kept[1] + moved[1]))
        poly = following
        rr = rest[0] * rest[0] + rest[1] * rest[1]
        cc = coef[0] * coef[0] + coef[1] * coef[1]
        rc = multiplied((rest[0], -rest[1]), coef)
        cr = (rc[0], -rc[1])
        size_rest = jnp.abs(rest[0]) + jnp.abs(rest[1])
        sizes = [size_rest * a + size * b for a, b in zip(sizes[:-1], sizes[1:])]

        def at(i, j):
            return gram[i, j] if i <= j else (gram[j, i][0], -gram[j, i][1])

        shrunk = {}
        top = STEPS - m
        for i in range(top):
            for j in range(i, top):
                a, b, d = at(i, j), at(i, j + 1), at(i + 1, j + 1)
                if i == j:
                    ab = multiplied(rc, b)
                    shrunk[i, j] = (rr * a[0] + 2.0 * ab[0] + cc * d[0], none)
                else:
                    ab, ac = multiplied(rc, b), multiplied(cr, at(i + 1, j))
                    shrunk[i, j] = tuple(rr * a[x] + (ab[x] + ac[x]) + cc * d[x] for x in range(2))
        gram = shrunk

    trusted = doubt <= error_allowed * scale
    weights = []
    for re, im in answer:
        re = jnp.where(trusted, re, jnp.nan)
        weights.append(
            (
                jnp.broadcast_to(re[:, 0:1], (8, 128)),
                jnp.broadcast_to(re[:, 127:128], (8, 128)),
                jnp.broadcast_to(im[:, 0:1], (8, 128)),
            )
        )

    def finish(sp, _):
        for side in range(2):
            for zz in range(2):
                res, ims = [], []
                for j, (wa, wb, wi) in enumerate(weights):
                    re, im = ((own_ref[side, sp, 2 * part + zz] if j == 0 else v_ref[j - 1, part, side, sp, zz]) for part in range(2))
                    res.append(wa * re - wi * im)
                    ims.append(wb * im + wi * re)
                re, im = tree_sum(res), tree_sum(ims)
                a, b, c = (inv_ref[i, side, sp, zz] for i in range(3))
                out_ref[16 * side + sp, 0, zz] = a * re - c * im
                out_ref[16 * side + sp, 1, zz] = b * im + c * re
        return 0

    lax.fori_loop(0, NZ // 2, finish, 0, unroll=2)


def slot_shifts():
    table = np.zeros((PAIRS, 4), np.float32)
    for slot in range(PAIRS):
        angle = 2 * math.pi * slot / L
        table[slot, :2] = (1 - decay * math.cos(angle)) / step_size
        table[slot, 2] = decay * math.sin(angle) / step_size
    table[0, 1] = (1 + decay) / step_size
    return table


def exchanged(blocks, axes):
    return lax.all_to_all(blocks, axes, split_axis=0, concat_axis=0, tiled=True)


VMEM = pl.BlockSpec(memory_space=pltpu.VMEM)
SMEM = pl.BlockSpec(memory_space=pltpu.SMEM)
ANY = pl.BlockSpec(memory_space=pl.ANY)


def f32(*shape):
    return pltpu.VMEM(shape, jnp.float32)


def held(x):
    return pltpu.with_memory_space_constraint(x, pltpu.MemorySpace.VMEM)


def in_hbm(x):
    return pltpu.with_memory_space_constraint(x, pltpu.MemorySpace.HBM)


def room(mebibytes):
    return pltpu.CompilerParams(vmem_limit_bytes=mebibytes * 2**20)


def together(residual, absorption, counts):
    chips = lax.axis_size("z")
    bands, rows = pl.pallas_call(
        bands_kernel,
        out_shape=(f32(16, 4, 2, 8, 128), f32(2, 2, 8, 128)),
        in_specs=[ANY, ANY],
        out_specs=(VMEM, VMEM),
        scratch_shapes=[pltpu.SemaphoreType.DMA((18,))],
        compiler_params=room(2),
        name="bands",
    )(in_hbm(residual), in_hbm(absorption))
    series = exchanged(bands, TM).reshape(L, 2, 8, 128)
    rows = rows[None]
    for axis in ("x", "y"):
        for bit in (1, 2):
            near = lax.ppermute(rows, axis, [(i, i ^ bit) for i in range(lax.axis_size(axis))])
            rows = jnp.concatenate([rows, near])
    swap = lax.ppermute(rows, "core", [(0, 1), (1, 0)])
    spectrum = pl.pallas_call(
        forward_kernel,
        out_shape=f32(PAIRS, 4, 8, 128),
        in_specs=[VMEM],
        out_specs=VMEM,
        compiler_params=room(4),
        name="forward",
    )(held(series))
    own = held(exchanged(spectrum, SLOTS).reshape(2, 16, 4, 8, 128))
    first, second = pl.pallas_call(
        edges_kernel,
        out_shape=(f32(16, 4 * HALO, 128), f32(16, 4 * HALO, 128)),
        in_specs=[VMEM],
        out_specs=(VMEM, VMEM),
        compiler_params=room(2),
        name="edges",
    )(own)
    ups = [[(2 * i + core, 2 * i + 2 + core) for i in range(chips - 1)] for core in range(2)]
    downs = [[(b, a) for a, b in pairs] for pairs in ups]
    first = lax.ppermute(first, TM, ups[0] + downs[1])
    second = lax.ppermute(second, TM, downs[0] + ups[1])
    basis, inverses, partial = pl.pallas_call(
        basis_kernel,
        out_shape=(f32(STEPS - 1, 2, 2, 16, 2, 8, 128), f32(3, 2, 16, 2, 8, 128), f32(8, 8, 128)),
        in_specs=[VMEM, VMEM, VMEM, VMEM, VMEM],
        out_specs=(VMEM, VMEM, VMEM),
        scratch_shapes=[
            pltpu.VMEM((2, 2, NZ + 2, 48, 128), jnp.float32),
            pltpu.VMEM((3, 2, 16, 2, 8, 128), jnp.float32),
            pltpu.VMEM((80, 8, 128), jnp.float32),
        ],
        compiler_params=room(10),
        name="basis",
    )(own, held(first), held(second), held(rows), held(swap))
    partials = exchanged(partial, "z")
    solved = pl.pallas_call(
        combine_kernel,
        out_shape=f32(PAIRS, 2, 2, 8, 128),
        in_specs=[VMEM, VMEM, VMEM, VMEM, VMEM],
        out_specs=VMEM,
        compiler_params=room(6),
        name="combine",
    )(held(counts.reshape(1, L)), held(partials), own, held(basis), held(inverses))
    gathered = exchanged(solved, SLOTS)
    values, failed = pl.pallas_call(
        inverse_kernel,
        out_shape=(f32(L, 2, 8, 128), pltpu.SMEM((1,), jnp.int32)),
        in_specs=[VMEM],
        out_specs=(VMEM, SMEM),
        compiler_params=room(4),
        name="inverse",
    )(held(gathered))
    return values, failed


def taken_kernel(*refs):
    count = len(refs) // 2
    copies = [pltpu.make_async_copy(refs[i], refs[count + i], refs[-1].at[i]) for i in range(count)]
    for copy in copies:
        copy.start()
    for copy in copies:
        copy.wait()


def taken(*arrays):
    return pl.pallas_call(
        taken_kernel,
        out_shape=tuple(f32(*a.shape) for a in arrays),
        in_specs=[ANY] * len(arrays),
        out_specs=(VMEM,) * len(arrays),
        scratch_shapes=[pltpu.SemaphoreType.DMA((len(arrays),))],
        compiler_params=room(2),
        name="taken",
    )(*(in_hbm(a) for a in arrays))


def to_steps(values, shape):
    bands = exchanged(values.reshape(16, 4, 2, 8, 128), TM)
    return bands.transpose(1, 2, 0, 3, 4).reshape(shape)


def body(residual, absorption, counts):
    values, failed = together(residual, absorption, counts)
    return lax.cond(
        failed[0] > 0,
        lambda r, a, c, v: stepwise(*taken(r, a), c),
        lambda r, a, c, v: to_steps(v, r.shape),
        residual, absorption, counts, values,
    )


def solution(mesh):
    chips, cores = mesh.shape["tm"] // 2, 2
    devices = mesh.devices.reshape(chips, cores, 4, 4)
    inner = Mesh(devices, ("z", "core", "y", "x"))
    in_specs = (P(TM, SPACE, None, None), P(SPACE, None, None), P())
    out_specs = P(TM, SPACE, None, None)
    return jax.shard_map(body, mesh=inner, in_specs=in_specs, out_specs=out_specs, check_vma=False)
```

```python
import math

import jax
import jax.numpy as jnp
import numpy as np
from jax import lax
from jax.experimental import pallas as pl
from jax.experimental.pallas import tpu as pltpu
from jax.sharding import Mesh
from jax.sharding import PartitionSpec as P

L = 64
STEPS = 6
HALO = 6
NX = 128
NZ = 32
PAIRS = L // 2
TM = ("z", "core")
SPACE = ("y", "x")
SLOTS = ("core", "y", "x")

wrap_factor = 0.1
step_size = 1.0
norm_floor = 1e-06
highest = lax.Precision.HIGHEST
decay = wrap_factor ** (1.0 / L)

gram_rounding = 1e-6
error_allowed = 1.5e-4


def with_halo(cells, sides, width):
    for axis, dim in sides:
        count = lax.axis_size(axis)
        ends = count - 1
        head = lax.slice_in_dim(cells, 0, width, axis=dim)
        tail = lax.slice_in_dim(cells, cells.shape[dim] - width, cells.shape[dim], axis=dim)
        cells = jnp.concatenate(
            [
                lax.ppermute(tail, axis, [(i, (i + 1) % count) for i in range(ends)]),
                cells,
                lax.ppermute(head, axis, [((i + 1) % count, i) for i in range(ends)]),
            ],
            axis=dim,
        )
    return cells


def copy_for_each(shard, axis):
    copies = jnp.broadcast_to(shard, (lax.axis_size(axis), *shard.shape))
    return lax.all_to_all(copies, axis, split_axis=0, concat_axis=0, tiled=True)


def taken_together(shard, axis):
    return copy_for_each(shard, axis).sum(axis=0)


def packed_total(arrays, axis):
    vector, at, finished = (jnp.concatenate([a.reshape(-1) for a in arrays]), 0, [])
    so_far = taken_together(vector, axis)
    for a in arrays:
        finished.append(so_far[at : at + a.size].reshape(a.shape))
        at += a.size
    return tuple(finished)


def shifts(frequency):
    angles = frequency.astype(jnp.float32) * (2.0 * math.pi / L)
    decay_rate = wrap_factor ** (1.0 / L)
    shift_re = (1.0 - decay_rate * jnp.cos(angles)) / step_size
    shift_im = decay_rate * jnp.sin(angles) / step_size
    return (shift_re, shift_im)


def near_sum(padded):
    interior = padded[..., 1:-1, :, :]
    widths = [(0, 0)] * (interior.ndim - 2) + [(1, 1), (1, 1)]
    padded_xy = jnp.pad(interior, widths)
    summed = padded[..., 2:, :, :] + padded[..., :-2, :, :]
    summed = summed + padded_xy[..., 2:, 1:-1] + padded_xy[..., :-2, 1:-1]
    summed = summed + padded_xy[..., 1:-1, 2:] + padded_xy[..., 1:-1, :-2]
    return summed


def advance(carried, dir_re, dir_im, img_re, img_im, coef_re, coef_im):
    sol_re, sol_im, res_re, res_im = carried
    sol_re = sol_re + coef_re * dir_re - coef_im * dir_im
    sol_im = sol_im + coef_re * dir_im + coef_im * dir_re
    res_re = res_re - (coef_re * img_re - coef_im * img_im)
    res_im = res_im - (coef_re * img_im + coef_im * img_re)
    return (sol_re, sol_im, res_re, res_im)


def solve_together(spectrum, absorption, frequencies, step_counts, longest):
    shift_re, shift_im = shifts(frequencies)
    shift_re = shift_re[:, None, None, None]
    shift_im = shift_im[:, None, None, None]
    diag_re = shift_re + 6.0 + absorption[None]
    magnitude = diag_re * diag_re + shift_im * shift_im
    inv_re = diag_re / magnitude
    inv_im = -shift_im / magnitude

    def iterate(iteration, carried):
        res_re, res_im = (carried[2], carried[3])
        dir_re = inv_re * res_re - inv_im * res_im
        dir_im = inv_re * res_im + inv_im * res_re
        padded = with_halo(jnp.stack([dir_re, dir_im], axis=1), ((SPACE, 2),), 1)
        nearby = near_sum(padded)
        img_re = diag_re * dir_re - shift_im * dir_im - nearby[:, 0]
        img_im = diag_re * dir_im + shift_im * dir_re - nearby[:, 1]
        totals = packed_total(
            (
                jnp.sum(img_re * res_re + img_im * res_im, axis=(1, 2, 3)),
                jnp.sum(img_re * res_im - img_im * res_re, axis=(1, 2, 3)),
                jnp.sum(img_re * img_re + img_im * img_im, axis=(1, 2, 3)),
            ),
            SPACE,
        )
        active = iteration < step_counts
        denominator = totals[2] + norm_floor
        coef_re = jnp.where(active, totals[0] / denominator, 0.0)[:, None, None, None]
        coef_im = jnp.where(active, totals[1] / denominator, 0.0)[:, None, None, None]
        return advance(carried, dir_re, dir_im, img_re, img_im, coef_re, coef_im)

    blank = jnp.zeros_like(spectrum[:, 0])
    finished = lax.fori_loop(0, longest, iterate, (blank, blank, spectrum[:, 0], spectrum[:, 1]))
    return jnp.stack([finished[0], finished[1]], axis=1)


def slot_order():
    return jnp.arange(L, dtype=jnp.int32)


def phase_table(left, right):
    return (left[:, None] * right[None, :] % L).astype(jnp.float32) * (2.0 * math.pi / L)


def stepwise(residual, absorption, counts):
    per_device = residual.shape[0]
    decay_rate = wrap_factor ** (1.0 / L)
    first_step = lax.axis_index(TM) * per_device
    times_here = first_step + jnp.arange(per_device, dtype=jnp.int32)
    scaled = residual * jnp.power(decay_rate, times_here.astype(jnp.float32))[:, None, None, None]
    slot_freqs = slot_order()
    own_freqs = lax.dynamic_slice_in_dim(slot_freqs, first_step, per_device)
    own_counts = counts[own_freqs]
    longest = jnp.max(counts)
    all_times = jnp.arange(L, dtype=jnp.int32)
    series = lax.all_to_all(scaled, TM, split_axis=2, concat_axis=0, tiled=True)
    phases = phase_table(slot_freqs, all_times)
    real_part = jnp.einsum("sn,nzxy->szxy", jnp.cos(phases), series, precision=highest)
    imag_part = -jnp.einsum("sn,nzxy->szxy", jnp.sin(phases), series, precision=highest)
    spectrum = lax.all_to_all(
        jnp.stack([real_part, imag_part], axis=1), TM, split_axis=0, concat_axis=3, tiled=True
    )
    solved = solve_together(spectrum, absorption, own_freqs, own_counts, longest)
    gathered = lax.all_to_all(solved, TM, split_axis=3, concat_axis=0, tiled=True)
    phases = phase_table(all_times, slot_freqs)
    values = jnp.einsum("ns,szxy->nzxy", jnp.cos(phases), gathered[:, 0], precision=highest)
    values = values - jnp.einsum(
        "ns,szxy->nzxy", jnp.sin(phases), gathered[:, 1], precision=highest
    )
    weight = jnp.power(decay_rate, -all_times.astype(jnp.float32)) / L
    values = values * weight[:, None, None, None]
    return lax.all_to_all(values, TM, split_axis=0, concat_axis=2, tiled=True)


def real_transform(x):
    n = len(x)
    if n == 2:
        return [(x[0] + x[1], None), (x[0] - x[1], None)]
    even, odd = real_transform(x[0::2]), real_transform(x[1::2])
    out = [None] * (n // 2 + 1)
    out[0] = (even[0][0] + odd[0][0], None)
    out[n // 2] = (even[0][0] - odd[0][0], None)
    out[n // 4] = (even[n // 4][0], -odd[n // 4][0])
    for k in range(1, n // 4):
        cos, sin = math.cos(2 * math.pi * k / n), math.sin(2 * math.pi * k / n)
        (er, ei), (cr, ci) = even[k], odd[k]
        tr, ti = cos * cr + sin * ci, cos * ci - sin * cr
        out[k] = (er + tr, ei + ti)
        out[n // 2 - k] = (er - tr, ti - ei)
    return out


def real_inverse(spectrum):
    n = 2 * (len(spectrum) - 1)
    first, last = spectrum[0][0], spectrum[n // 2][0]
    if n == 2:
        return [first + last, first - last]
    even, odd = [None] * (n // 4 + 1), [None] * (n // 4 + 1)
    even[0], odd[0] = (first + last, None), (first - last, None)
    mid_re, mid_im = spectrum[n // 4]
    even[n // 4], odd[n // 4] = (mid_re + mid_re, None), (-(mid_im + mid_im), None)
    for k in range(1, n // 4):
        cos, sin = math.cos(2 * math.pi * k / n), math.sin(2 * math.pi * k / n)
        (ar, ai), (br, bi) = spectrum[k], spectrum[n // 2 - k]
        even[k] = (ar + br, ai - bi)
        tr, ti = ar - br, ai + bi
        odd[k] = (cos * tr - sin * ti, cos * ti + sin * tr)
    halves = real_inverse(even), real_inverse(odd)
    return [halves[i % 2][i // 2] for i in range(n)]


def bands_kernel(x_ref, a_ref, out_ref, rows_ref, sems):
    copies = [
        pltpu.make_async_copy(x_ref.at[:, :, pl.ds(8 * band, 8), :], out_ref.at[band], sems.at[band]) for band in range(16)
    ]
    first = 16 * lax.axis_index("z") + 16 * lax.axis_index("core") - 8
    for core in range(2):
        row = pl.multiple_of(jnp.clip(first + 8 * core, 0, NX - 8), 8)
        copies.append(pltpu.make_async_copy(a_ref.at[:, pl.ds(row, 8), :], rows_ref.at[core], sems.at[16 + core]))
    for copy in copies:
        copy.start()
    for copy in copies:
        copy.wait()


def forward_kernel(x_ref, rows_ref, swap_ref, out_ref):
    del rows_ref, swap_ref
    for zz in range(2):
        spectrum = real_transform([x_ref[n, zz] * decay**n for n in range(L)])
        out_ref[0, zz] = spectrum[0][0]
        out_ref[0, 2 + zz] = spectrum[PAIRS][0]
        for k in range(1, PAIRS):
            out_ref[k, zz] = spectrum[k][0]
            out_ref[k, 2 + zz] = spectrum[k][1]


def inverse_kernel(s_ref, out_ref, failed_ref):
    failed = jnp.zeros((8, 128), jnp.float32)
    for zz in range(2):
        ends = [s_ref[0, part, zz] for part in range(2)]
        spectrum = [(ends[0] + ends[0], None)]
        spectrum += [(s_ref[k, 0, zz], s_ref[k, 1, zz]) for k in range(1, PAIRS)]
        spectrum += [(ends[1] + ends[1], None)]
        values = real_inverse(spectrum)
        for n in range(L):
            out_ref[n, zz] = values[n] * (decay ** (-n) / (2 * L))
        failed = jnp.where(values[0] != values[0], 1.0, failed)
    failed_ref[0] = jnp.where(jnp.max(failed) > 0.0, 1, 0)


same = [(i, j) for i in range(STEPS + 1) for j in range(i, STEPS + 1)]
cross = [(i, j) for i in range(STEPS + 1) for j in range(i + 1, STEPS + 1)]
entry = {(kind, i, j): None for kind, ij in (("re", same), ("im", same), ("x", cross)) for i, j in ij}
for at, name in enumerate(entry):
    entry[name] = at


def tree_sum(terms):
    while len(terms) > 1:
        terms = [sum(terms[i : i + 2][1:], terms[i]) for i in range(0, len(terms), 2)]
    return terms[0]


def pick(slot, values):
    found = jnp.float32(values[0])
    for i in range(1, len(values)):
        found = jnp.where(slot == i, jnp.float32(values[i]), found)
    return found


def edges_kernel(own_ref, first_ref, second_ref):
    low = lax.axis_index("core") == 0
    for sp in range(16):
        for i in range(4):
            up, down = own_ref[1, sp, i, pl.ds(8 - HALO, HALO), :], own_ref[0, sp, i, pl.ds(0, HALO), :]
            first_ref[sp, pl.ds(HALO * i, HALO), :] = jnp.where(low, up, down)
            second_ref[sp, pl.ds(HALO * i, HALO), :] = jnp.where(low, down, up)


def basis_kernel(own_ref, first_ref, second_ref, abs_ref, swap_ref, v_ref, inv_ref, gram_ref, u, edge_inv, sums):
    slot, z, core = lax.axis_index(SLOTS), lax.axis_index("z"), lax.axis_index("core")
    home_y, home_x = lax.axis_index("y"), lax.axis_index("x")
    shifts_here = slot_shifts()
    shift_a, shift_b, shift_im = (pick(slot, shifts_here[:, i]) for i in range(3))
    lanes = lax.broadcasted_iota(jnp.int32, (8, 128), 1)
    first_lane, last_lane = lanes == 0, lanes == 127
    blank = jnp.zeros((8, 128), jnp.float32)

    for turn in range(2):
        for part in range(2):
            for row in range(8, 40, 8):
                u[turn, part, 0, pl.ds(row, 8), :] = blank
                u[turn, part, NZ + 1, pl.ds(row, 8), :] = blank

    def put(turn, tile, layer, inverse, re, im):
        a, b, c = inverse
        u[turn, 0, layer, pl.ds(8 + 8 * tile, 8), :] = a * re - c * im
        u[turn, 1, layer, pl.ds(8 + 8 * tile, 8), :] = b * im + c * re

    def prepare(sp, _):
        for turn in range(2):
            for part in range(2):
                for zz in range(2):
                    u[turn, part, 2 * sp + zz + 1, pl.ds(0, 8), :] = blank
                    u[turn, part, 2 * sp + zz + 1, pl.ds(40, 8), :] = blank
        for tile in range(4):
            for zz in range(2):
                mine, other = (ref[4 * ((home_y + 4 - sp // 4) % 4) + (home_x + 16 - sp) % 4, tile % 2, zz] for ref in (abs_ref, swap_ref))
                base = jnp.where(core == tile // 2, mine, other)
                da, db = (shift_a + 6.0) + base, (shift_b + 6.0) + base
                ra, rb = 1.0 / (da * da + shift_im * shift_im), 1.0 / (db * db + shift_im * shift_im)
                found = [da * ra, db * rb, -shift_im * ra]
                if tile in (1, 2):
                    for i in range(3):
                        inv_ref[i, tile - 1, sp, zz] = found[i]
                    re, im = (own_ref[tile - 1, sp, 2 * part + zz] for part in range(2))
                else:
                    inside = z > 0 if tile == 0 else z < lax.axis_size("z") - 1
                    found = [jnp.where(inside, f, 0.0) for f in found]
                    for i in range(3):
                        edge_inv[i, tile // 3, sp, zz] = found[i]
                    pair = []
                    for part in range(2):
                        at = HALO * (2 * part + zz)
                        wanted = at - (8 - HALO) if tile == 0 else at
                        start = min(max(wanted, 0), 4 * HALO - 8)
                        first, second = (ref[sp, pl.ds(start, 8), :] for ref in (first_ref, second_ref))
                        rows = jnp.where((core == 0) == (tile == 0), first, second)
                        shift = (start - wanted) % 8
                        pair.append(pltpu.roll(rows, shift, 0) if shift else rows)
                    re, im = pair
                put(0, tile, 2 * sp + zz + 1, found, re, im)
        return 0

    lax.fori_loop(0, NZ // 2, prepare, 0, unroll=4)

    def vector(j, side, sp, zz):
        if j == 0:
            return [own_ref[side, sp, 2 * part + zz] for part in range(2)]
        return [v_ref[j - 1, part, side, sp, zz] for part in range(2)]

    for j in range(STEPS):
        names = [name for name in entry if name[2] == j + 1 or (j == 0 and name[2] == 0)]

        def step(group, totals, j=j, names=names):
            by_layer = []
            for sp in [4 * group + s for s in range(4)]:
                found = {name: [] for name in names}
                for zz in range(2):
                    for tile in range(4) if j < STEPS - 1 else (1, 2):
                        layer, row = 2 * sp + zz + 1, 8 + 8 * tile
                        pair = []
                        for part in range(2):
                            old = u.at[j % 2, part]
                            here = old[layer, pl.ds(row, 8), :]
                            total = old[layer - 1, pl.ds(row, 8), :] + old[layer + 1, pl.ds(row, 8), :]
                            total = total + (old[layer, pl.ds(row - 1, 8), :] + old[layer, pl.ds(row + 1, 8), :])
                            total = total + (
                                jnp.where(first_lane, 0.0, pltpu.roll(here, 1, 1))
                                + jnp.where(last_lane, 0.0, pltpu.roll(here, 127, 1))
                            )
                            pair.append(total)
                        if tile in (1, 2):
                            side = tile - 1
                            if j < STEPS - 1:
                                for part in range(2):
                                    v_ref[j, part, side, sp, zz] = pair[part]
                            known = [vector(i, side, sp, zz) for i in range(j + 1)] + [pair]
                            for kind, i, k in names:
                                a, b = known[i], known[k]
                                if kind == "x":
                                    found[kind, i, k].append(a[0] * b[1] - a[1] * b[0])
                                else:
                                    part = ("re", "im").index(kind)
                                    found[kind, i, k].append(a[part] * b[part])
                        if j < STEPS - 1:
                            if tile in (1, 2):
                                inverse = [inv_ref[i, tile - 1, sp, zz] for i in range(3)]
                            else:
                                inverse = [edge_inv[i, tile // 3, sp, zz] for i in range(3)]
                            put((j + 1) % 2, tile, layer, inverse, *pair)
                by_layer.append([tree_sum(found[name]) for name in names])
            return tuple(t + tree_sum(list(parts)) for t, parts in zip(totals, zip(*by_layer)))

        totals = lax.fori_loop(0, NZ // 8, step, tuple(blank for _ in names), unroll=2)
        for name, total in zip(names, totals):
            sums[entry[name]] = total
    for spare in range(len(entry), sums.shape[0]):
        sums[spare] = blank

    rows = jnp.sum(sums[...], axis=1)
    column = jnp.sum(rows, axis=1, keepdims=True)
    where = lax.broadcasted_iota(jnp.int32, rows.shape, 0) == lax.broadcasted_iota(jnp.int32, rows.shape, 1)
    packed = jnp.sum(jnp.where(where, column, 0.0), axis=0, keepdims=True)
    gram_ref[...] = jnp.broadcast_to(packed[None], gram_ref.shape)


def multiplied(a, b):
    return (a[0] * b[0] - a[1] * b[1], a[0] * b[1] + a[1] * b[0])


def combine_kernel(count_ref, part_ref, own_ref, v_ref, inv_ref, out_ref):
    slot = lax.axis_index(SLOTS)
    ends = slot == 0
    low = lax.broadcasted_iota(jnp.int32, (8, 128), 1) < 64
    row = tree_sum([part_ref[i] for i in range(part_ref.shape[0])])

    def spread(name):
        return jnp.broadcast_to(row[:, entry[name] : entry[name] + 1], (8, 128))

    gram = {}
    for i, j in same:
        re, im = spread(("re", i, j)), spread(("im", i, j))
        real = jnp.where(ends, jnp.where(low, re, im), re + im)
        imag = jnp.where(ends, 0.0, spread(("x", i, j))) if j > i else jnp.zeros_like(real)
        gram[i, j] = (real, imag)

    count_lane = lax.broadcasted_iota(jnp.int32, (1, L), 1)
    count_a, count_b = (
        jnp.sum(jnp.where(count_lane == k, count_ref[...], 0).astype(jnp.float32), axis=1, keepdims=True)
        for k in (slot, jnp.where(ends, PAIRS, L - slot))
    )
    one, none = jnp.ones((8, 128), jnp.float32), jnp.zeros((8, 128), jnp.float32)
    poly, answer = [(one, none)], [(none, none) for _ in range(STEPS)]
    sizes = [jnp.sqrt(jnp.maximum(gram[i, i][0], 0.0)) for i in range(STEPS + 1)]
    doubt, scale = none, None
    for m in range(STEPS):
        in_a, in_b = (jnp.broadcast_to(jnp.where(m < count, 1.0, 0.0), (8, 128)) for count in (count_a, count_b))
        weight = jnp.where(ends, jnp.where(low, in_a, in_b), in_a + in_b)
        g00, g01, g11 = gram[0, 0][0], gram[0, 1], gram[1, 1][0]
        denominator = (g00 - 2.0 * g01[0] + g11) + norm_floor
        inverse = 1.0 / denominator
        coef = ((g00 - g01[0]) * inverse, g01[1] * inverse)
        size = jnp.abs(coef[0]) + jnp.abs(coef[1])
        length = jnp.sqrt(jnp.maximum(g00, 0.0))
        if m == 0:
            scale = size * length
        pair = sizes[0] + sizes[1]
        step_doubt = (gram_rounding * (1 + m / 2)) * pair * (sizes[0] + size * pair) * jnp.abs(inverse) * length
        doubt = doubt + jnp.where(weight > 0.0, step_doubt, none)
        for j, p in enumerate(poly):
            term = multiplied(coef, p)
            answer[j] = (answer[j][0] + weight * term[0], answer[j][1] + weight * term[1])
        if m == STEPS - 1:
            break
        rest = (1.0 - coef[0], -coef[1])
        padded = [None] + poly + [None]
        following = []
        for j in range(len(poly) + 1):
            kept = multiplied(rest, poly[j]) if j < len(poly) else (none, none)
            moved = multiplied(coef, poly[j - 1]) if j > 0 else (none, none)
            following.append((kept[0] + moved[0], kept[1] + moved[1]))
        poly = following
        rr = rest[0] * rest[0] + rest[1] * rest[1]
        cc = coef[0] * coef[0] + coef[1] * coef[1]
        rc = multiplied((rest[0], -rest[1]), coef)
        cr = (rc[0], -rc[1])
        size_rest = jnp.abs(rest[0]) + jnp.abs(rest[1])
        sizes = [size_rest * a + size * b for a, b in zip(sizes[:-1], sizes[1:])]

        def at(i, j):
            return gram[i, j] if i <= j else (gram[j, i][0], -gram[j, i][1])

        shrunk = {}
        top = STEPS - m
        for i in range(top):
            for j in range(i, top):
                a, b, d = at(i, j), at(i, j + 1), at(i + 1, j + 1)
                if i == j:
                    ab = multiplied(rc, b)
                    shrunk[i, j] = (rr * a[0] + 2.0 * ab[0] + cc * d[0], none)
                else:
                    ab, ac = multiplied(rc, b), multiplied(cr, at(i + 1, j))
                    shrunk[i, j] = tuple(rr * a[x] + (ab[x] + ac[x]) + cc * d[x] for x in range(2))
        gram = shrunk

    trusted = doubt <= error_allowed * scale
    weights = []
    for re, im in answer:
        re = jnp.where(trusted, re, jnp.nan)
        weights.append(
            (
                jnp.broadcast_to(re[:, 0:1], (8, 128)),
                jnp.broadcast_to(re[:, 127:128], (8, 128)),
                jnp.broadcast_to(im[:, 0:1], (8, 128)),
            )
        )

    def finish(sp, _):
        for side in range(2):
            for zz in range(2):
                res, ims = [], []
                for j, (wa, wb, wi) in enumerate(weights):
                    re, im = ((own_ref[side, sp, 2 * part + zz] if j == 0 else v_ref[j - 1, part, side, sp, zz]) for part in range(2))
                    res.append(wa * re - wi * im)
                    ims.append(wb * im + wi * re)
                re, im = tree_sum(res), tree_sum(ims)
                a, b, c = (inv_ref[i, side, sp, zz] for i in range(3))
                out_ref[16 * side + sp, 0, zz] = a * re - c * im
                out_ref[16 * side + sp, 1, zz] = b * im + c * re
        return 0

    lax.fori_loop(0, NZ // 2, finish, 0, unroll=2)


def slot_shifts():
    table = np.zeros((PAIRS, 4), np.float32)
    for slot in range(PAIRS):
        angle = 2 * math.pi * slot / L
        table[slot, :2] = (1 - decay * math.cos(angle)) / step_size
        table[slot, 2] = decay * math.sin(angle) / step_size
    table[0, 1] = (1 + decay) / step_size
    return table


def exchanged(blocks, axes):
    return lax.all_to_all(blocks, axes, split_axis=0, concat_axis=0, tiled=True)


VMEM = pl.BlockSpec(memory_space=pltpu.VMEM)
SMEM = pl.BlockSpec(memory_space=pltpu.SMEM)
ANY = pl.BlockSpec(memory_space=pl.ANY)


def f32(*shape):
    return pltpu.VMEM(shape, jnp.float32)


def held(x):
    return pltpu.with_memory_space_constraint(x, pltpu.MemorySpace.VMEM)


def in_hbm(x):
    return pltpu.with_memory_space_constraint(x, pltpu.MemorySpace.HBM)


def room(mebibytes):
    return pltpu.CompilerParams(vmem_limit_bytes=mebibytes * 2**20)


def together(residual, absorption, counts):
    chips = lax.axis_size("z")
    bands, rows = pl.pallas_call(
        bands_kernel,
        out_shape=(f32(16, 4, 2, 8, 128), f32(2, 2, 8, 128)),
        in_specs=[ANY, ANY],
        out_specs=(VMEM, VMEM),
        scratch_shapes=[pltpu.SemaphoreType.DMA((18,))],
        compiler_params=room(2),
        name="bands",
    )(in_hbm(residual), in_hbm(absorption))
    series = exchanged(bands, TM).reshape(L, 2, 8, 128)
    rows = rows[None]
    for axis in ("x", "y"):
        size = lax.axis_size(axis)
        near = [lax.ppermute(rows, axis, [(i, (i + d) % size) for i in range(size)]) for d in range(1, size)]
        rows = jnp.concatenate([rows, *near])
    swap = lax.ppermute(rows, "core", [(0, 1), (1, 0)])
    spectrum = pl.pallas_call(
        forward_kernel,
        out_shape=f32(PAIRS, 4, 8, 128),
        in_specs=[VMEM, ANY, ANY],
        out_specs=VMEM,
        compiler_params=room(4),
        name="forward",
    )(held(series), rows, swap)
    own = held(exchanged(spectrum, SLOTS).reshape(2, 16, 4, 8, 128))
    first, second = pl.pallas_call(
        edges_kernel,
        out_shape=(f32(16, 4 * HALO, 128), f32(16, 4 * HALO, 128)),
        in_specs=[VMEM],
        out_specs=(VMEM, VMEM),
        compiler_params=room(2),
        name="edges",
    )(own)
    ups = [[(2 * i + core, 2 * i + 2 + core) for i in range(chips - 1)] for core in range(2)]
    downs = [[(b, a) for a, b in pairs] for pairs in ups]
    first = lax.ppermute(first, TM, ups[0] + downs[1])
    second = lax.ppermute(second, TM, downs[0] + ups[1])
    basis, inverses, partial = pl.pallas_call(
        basis_kernel,
        out_shape=(f32(STEPS - 1, 2, 2, 16, 2, 8, 128), f32(3, 2, 16, 2, 8, 128), f32(8, 8, 128)),
        in_specs=[VMEM, VMEM, VMEM, VMEM, VMEM],
        out_specs=(VMEM, VMEM, VMEM),
        scratch_shapes=[
            pltpu.VMEM((2, 2, NZ + 2, 48, 128), jnp.float32),
            pltpu.VMEM((3, 2, 16, 2, 8, 128), jnp.float32),
            pltpu.VMEM((80, 8, 128), jnp.float32),
        ],
        compiler_params=room(10),
        name="basis",
    )(own, held(first), held(second), held(rows), held(swap))
    partials = exchanged(partial, "z")
    solved = pl.pallas_call(
        combine_kernel,
        out_shape=f32(PAIRS, 2, 2, 8, 128),
        in_specs=[VMEM, VMEM, VMEM, VMEM, VMEM],
        out_specs=VMEM,
        compiler_params=room(6),
        name="combine",
    )(held(counts.reshape(1, L)), held(partials), own, held(basis), held(inverses))
    gathered = exchanged(solved, SLOTS)
    values, failed = pl.pallas_call(
        inverse_kernel,
        out_shape=(f32(L, 2, 8, 128), pltpu.SMEM((1,), jnp.int32)),
        in_specs=[VMEM],
        out_specs=(VMEM, SMEM),
        compiler_params=room(4),
        name="inverse",
    )(held(gathered))
    return values, failed


def taken_kernel(*refs):
    count = len(refs) // 2
    copies = [pltpu.make_async_copy(refs[i], refs[count + i], refs[-1].at[i]) for i in range(count)]
    for copy in copies:
        copy.start()
    for copy in copies:
        copy.wait()


def taken(*arrays):
    return pl.pallas_call(
        taken_kernel,
        out_shape=tuple(f32(*a.shape) for a in arrays),
        in_specs=[ANY] * len(arrays),
        out_specs=(VMEM,) * len(arrays),
        scratch_shapes=[pltpu.SemaphoreType.DMA((len(arrays),))],
        compiler_params=room(2),
        name="taken",
    )(*(in_hbm(a) for a in arrays))


def to_steps(values, shape):
    bands = exchanged(values.reshape(16, 4, 2, 8, 128), TM)
    return bands.transpose(1, 2, 0, 3, 4).reshape(shape)


def body(residual, absorption, counts):
    values, failed = together(residual, absorption, counts)
    return lax.cond(
        failed[0] > 0,
        lambda r, a, c, v: stepwise(*taken(r, a), c),
        lambda r, a, c, v: to_steps(v, r.shape),
        residual, absorption, counts, values,
    )


def solution(mesh):
    chips, cores = mesh.shape["tm"] // 2, 2
    devices = mesh.devices.reshape(chips, cores, 4, 4)
    inner = Mesh(devices, ("z", "core", "y", "x"))
    in_specs = (P(TM, SPACE, None, None), P(SPACE, None, None), P())
    out_specs = P(TM, SPACE, None, None)
    return jax.shard_map(body, mesh=inner, in_specs=in_specs, out_specs=out_specs, check_vma=False)
```

```python
import math

import jax
import jax.numpy as jnp
import numpy as np
from jax import lax
from jax.experimental import pallas as pl
from jax.experimental.pallas import tpu as pltpu
from jax.sharding import Mesh
from jax.sharding import PartitionSpec as P

L = 64
STEPS = 6
HALO = 6
NX = 128
NZ = 32
PAIRS = L // 2
TM = ("z", "core")
SPACE = ("y", "x")
SLOTS = ("core", "y", "x")

wrap_factor = 0.1
step_size = 1.0
norm_floor = 1e-06
highest = lax.Precision.HIGHEST
decay = wrap_factor ** (1.0 / L)

gram_rounding = 1e-6
error_allowed = 1.5e-4


def with_halo(cells, sides, width):
    for axis, dim in sides:
        count = lax.axis_size(axis)
        ends = count - 1
        head = lax.slice_in_dim(cells, 0, width, axis=dim)
        tail = lax.slice_in_dim(cells, cells.shape[dim] - width, cells.shape[dim], axis=dim)
        cells = jnp.concatenate(
            [
                lax.ppermute(tail, axis, [(i, (i + 1) % count) for i in range(ends)]),
                cells,
                lax.ppermute(head, axis, [((i + 1) % count, i) for i in range(ends)]),
            ],
            axis=dim,
        )
    return cells


def copy_for_each(shard, axis):
    copies = jnp.broadcast_to(shard, (lax.axis_size(axis), *shard.shape))
    return lax.all_to_all(copies, axis, split_axis=0, concat_axis=0, tiled=True)


def taken_together(shard, axis):
    return copy_for_each(shard, axis).sum(axis=0)


def packed_total(arrays, axis):
    vector, at, finished = (jnp.concatenate([a.reshape(-1) for a in arrays]), 0, [])
    so_far = taken_together(vector, axis)
    for a in arrays:
        finished.append(so_far[at : at + a.size].reshape(a.shape))
        at += a.size
    return tuple(finished)


def shifts(frequency):
    angles = frequency.astype(jnp.float32) * (2.0 * math.pi / L)
    decay_rate = wrap_factor ** (1.0 / L)
    shift_re = (1.0 - decay_rate * jnp.cos(angles)) / step_size
    shift_im = decay_rate * jnp.sin(angles) / step_size
    return (shift_re, shift_im)


def near_sum(padded):
    interior = padded[..., 1:-1, :, :]
    widths = [(0, 0)] * (interior.ndim - 2) + [(1, 1), (1, 1)]
    padded_xy = jnp.pad(interior, widths)
    summed = padded[..., 2:, :, :] + padded[..., :-2, :, :]
    summed = summed + padded_xy[..., 2:, 1:-1] + padded_xy[..., :-2, 1:-1]
    summed = summed + padded_xy[..., 1:-1, 2:] + padded_xy[..., 1:-1, :-2]
    return summed


def advance(carried, dir_re, dir_im, img_re, img_im, coef_re, coef_im):
    sol_re, sol_im, res_re, res_im = carried
    sol_re = sol_re + coef_re * dir_re - coef_im * dir_im
    sol_im = sol_im + coef_re * dir_im + coef_im * dir_re
    res_re = res_re - (coef_re * img_re - coef_im * img_im)
    res_im = res_im - (coef_re * img_im + coef_im * img_re)
    return (sol_re, sol_im, res_re, res_im)


def solve_together(spectrum, absorption, frequencies, step_counts, longest):
    shift_re, shift_im = shifts(frequencies)
    shift_re = shift_re[:, None, None, None]
    shift_im = shift_im[:, None, None, None]
    diag_re = shift_re + 6.0 + absorption[None]
    magnitude = diag_re * diag_re + shift_im * shift_im
    inv_re = diag_re / magnitude
    inv_im = -shift_im / magnitude

    def iterate(iteration, carried):
        res_re, res_im = (carried[2], carried[3])
        dir_re = inv_re * res_re - inv_im * res_im
        dir_im = inv_re * res_im + inv_im * res_re
        padded = with_halo(jnp.stack([dir_re, dir_im], axis=1), ((SPACE, 2),), 1)
        nearby = near_sum(padded)
        img_re = diag_re * dir_re - shift_im * dir_im - nearby[:, 0]
        img_im = diag_re * dir_im + shift_im * dir_re - nearby[:, 1]
        totals = packed_total(
            (
                jnp.sum(img_re * res_re + img_im * res_im, axis=(1, 2, 3)),
                jnp.sum(img_re * res_im - img_im * res_re, axis=(1, 2, 3)),
                jnp.sum(img_re * img_re + img_im * img_im, axis=(1, 2, 3)),
            ),
            SPACE,
        )
        active = iteration < step_counts
        denominator = totals[2] + norm_floor
        coef_re = jnp.where(active, totals[0] / denominator, 0.0)[:, None, None, None]
        coef_im = jnp.where(active, totals[1] / denominator, 0.0)[:, None, None, None]
        return advance(carried, dir_re, dir_im, img_re, img_im, coef_re, coef_im)

    blank = jnp.zeros_like(spectrum[:, 0])
    finished = lax.fori_loop(0, longest, iterate, (blank, blank, spectrum[:, 0], spectrum[:, 1]))
    return jnp.stack([finished[0], finished[1]], axis=1)


def slot_order():
    return jnp.arange(L, dtype=jnp.int32)


def phase_table(left, right):
    return (left[:, None] * right[None, :] % L).astype(jnp.float32) * (2.0 * math.pi / L)


def stepwise(residual, absorption, counts):
    per_device = residual.shape[0]
    decay_rate = wrap_factor ** (1.0 / L)
    first_step = lax.axis_index(TM) * per_device
    times_here = first_step + jnp.arange(per_device, dtype=jnp.int32)
    scaled = residual * jnp.power(decay_rate, times_here.astype(jnp.float32))[:, None, None, None]
    slot_freqs = slot_order()
    own_freqs = lax.dynamic_slice_in_dim(slot_freqs, first_step, per_device)
    own_counts = counts[own_freqs]
    longest = jnp.max(counts)
    all_times = jnp.arange(L, dtype=jnp.int32)
    series = lax.all_to_all(scaled, TM, split_axis=2, concat_axis=0, tiled=True)
    phases = phase_table(slot_freqs, all_times)
    real_part = jnp.einsum("sn,nzxy->szxy", jnp.cos(phases), series, precision=highest)
    imag_part = -jnp.einsum("sn,nzxy->szxy", jnp.sin(phases), series, precision=highest)
    spectrum = lax.all_to_all(
        jnp.stack([real_part, imag_part], axis=1), TM, split_axis=0, concat_axis=3, tiled=True
    )
    solved = solve_together(spectrum, absorption, own_freqs, own_counts, longest)
    gathered = lax.all_to_all(solved, TM, split_axis=3, concat_axis=0, tiled=True)
    phases = phase_table(all_times, slot_freqs)
    values = jnp.einsum("ns,szxy->nzxy", jnp.cos(phases), gathered[:, 0], precision=highest)
    values = values - jnp.einsum(
        "ns,szxy->nzxy", jnp.sin(phases), gathered[:, 1], precision=highest
    )
    weight = jnp.power(decay_rate, -all_times.astype(jnp.float32)) / L
    values = values * weight[:, None, None, None]
    return lax.all_to_all(values, TM, split_axis=0, concat_axis=2, tiled=True)


def real_transform(x):
    n = len(x)
    if n == 2:
        return [(x[0] + x[1], None), (x[0] - x[1], None)]
    even, odd = real_transform(x[0::2]), real_transform(x[1::2])
    out = [None] * (n // 2 + 1)
    out[0] = (even[0][0] + odd[0][0], None)
    out[n // 2] = (even[0][0] - odd[0][0], None)
    out[n // 4] = (even[n // 4][0], -odd[n // 4][0])
    for k in range(1, n // 4):
        cos, sin = math.cos(2 * math.pi * k / n), math.sin(2 * math.pi * k / n)
        (er, ei), (cr, ci) = even[k], odd[k]
        tr, ti = cos * cr + sin * ci, cos * ci - sin * cr
        out[k] = (er + tr, ei + ti)
        out[n // 2 - k] = (er - tr, ti - ei)
    return out


def real_inverse(spectrum):
    n = 2 * (len(spectrum) - 1)
    first, last = spectrum[0][0], spectrum[n // 2][0]
    if n == 2:
        return [first + last, first - last]
    even, odd = [None] * (n // 4 + 1), [None] * (n // 4 + 1)
    even[0], odd[0] = (first + last, None), (first - last, None)
    mid_re, mid_im = spectrum[n // 4]
    even[n // 4], odd[n // 4] = (mid_re + mid_re, None), (-(mid_im + mid_im), None)
    for k in range(1, n // 4):
        cos, sin = math.cos(2 * math.pi * k / n), math.sin(2 * math.pi * k / n)
        (ar, ai), (br, bi) = spectrum[k], spectrum[n // 2 - k]
        even[k] = (ar + br, ai - bi)
        tr, ti = ar - br, ai + bi
        odd[k] = (cos * tr - sin * ti, cos * ti + sin * tr)
    halves = real_inverse(even), real_inverse(odd)
    return [halves[i % 2][i // 2] for i in range(n)]


def bands_kernel(x_ref, a_ref, out_ref, rows_ref, sems):
    copies = [
        pltpu.make_async_copy(x_ref.at[:, :, pl.ds(8 * band, 8), :], out_ref.at[band], sems.at[band]) for band in range(16)
    ]
    first = 16 * lax.axis_index("z") + 16 * lax.axis_index("core") - 8
    for core in range(2):
        row = pl.multiple_of(jnp.clip(first + 8 * core, 0, NX - 8), 8)
        copies.append(pltpu.make_async_copy(a_ref.at[:, pl.ds(row, 8), :], rows_ref.at[core], sems.at[16 + core]))
    for copy in copies:
        copy.start()
    for copy in copies:
        copy.wait()


def forward_kernel(x_ref, rows_ref, out_ref):
    for core in range(2):
        for zz in range(2):
            rows = rows_ref[core, zz]
            for slot in range(16 * core, 16 * core + 16):
                out_ref[slot, 4 + zz] = rows
    for zz in range(2):
        spectrum = real_transform([x_ref[n, zz] * decay**n for n in range(L)])
        out_ref[0, zz] = spectrum[0][0]
        out_ref[0, 2 + zz] = spectrum[PAIRS][0]
        for k in range(1, PAIRS):
            out_ref[k, zz] = spectrum[k][0]
            out_ref[k, 2 + zz] = spectrum[k][1]


def inverse_kernel(s_ref, out_ref, failed_ref):
    failed = jnp.zeros((8, 128), jnp.float32)
    for zz in range(2):
        ends = [s_ref[0, part, zz] for part in range(2)]
        spectrum = [(ends[0] + ends[0], None)]
        spectrum += [(s_ref[k, 0, zz], s_ref[k, 1, zz]) for k in range(1, PAIRS)]
        spectrum += [(ends[1] + ends[1], None)]
        values = real_inverse(spectrum)
        for n in range(L):
            out_ref[n, zz] = values[n] * (decay ** (-n) / (2 * L))
        failed = jnp.where(values[0] != values[0], 1.0, failed)
    failed_ref[0] = jnp.where(jnp.max(failed) > 0.0, 1, 0)


same = [(i, j) for i in range(STEPS + 1) for j in range(i, STEPS + 1)]
cross = [(i, j) for i in range(STEPS + 1) for j in range(i + 1, STEPS + 1)]
entry = {(kind, i, j): None for kind, ij in (("re", same), ("im", same), ("x", cross)) for i, j in ij}
for at, name in enumerate(entry):
    entry[name] = at


def tree_sum(terms):
    while len(terms) > 1:
        terms = [sum(terms[i : i + 2][1:], terms[i]) for i in range(0, len(terms), 2)]
    return terms[0]


def pick(slot, values):
    found = jnp.float32(values[0])
    for i in range(1, len(values)):
        found = jnp.where(slot == i, jnp.float32(values[i]), found)
    return found


def edges_kernel(own_ref, first_ref, second_ref, abs_ref):
    low = lax.axis_index("core") == 0
    for sp in range(16):
        for i in range(4):
            up, down = own_ref[1, sp, i, pl.ds(8 - HALO, HALO), :], own_ref[0, sp, i, pl.ds(0, HALO), :]
            first_ref[sp, pl.ds(HALO * i, HALO), :] = jnp.where(low, up, down)
            second_ref[sp, pl.ds(HALO * i, HALO), :] = jnp.where(low, down, up)
        for side in range(2):
            for zz in range(2):
                abs_ref[side, sp, zz] = own_ref[side, sp, 4 + zz]


def inverses_kernel(own_ref, swap_ref, inv_ref, edge_inv_ref):
    slot, z, core = lax.axis_index(SLOTS), lax.axis_index("z"), lax.axis_index("core")
    shifts_here = slot_shifts()
    shift_a, shift_b, shift_im = (pick(slot, shifts_here[:, i]) for i in range(3))

    def prepare(sp, _):
        for tile in range(4):
            for zz in range(2):
                mine, other = own_ref[tile // 2, sp, 4 + zz], swap_ref[tile // 2, sp, zz]
                base = jnp.where(core == tile % 2, mine, other)
                da, db = (shift_a + 6.0) + base, (shift_b + 6.0) + base
                ra, rb = 1.0 / (da * da + shift_im * shift_im), 1.0 / (db * db + shift_im * shift_im)
                found = [da * ra, db * rb, -shift_im * ra]
                if tile in (1, 2):
                    for i in range(3):
                        inv_ref[i, tile - 1, sp, zz] = found[i]
                else:
                    inside = z > 0 if tile == 0 else z < lax.axis_size("z") - 1
                    for i in range(3):
                        edge_inv_ref[i, tile // 3, sp, zz] = jnp.where(inside, found[i], 0.0)
        return 0

    lax.fori_loop(0, NZ // 2, prepare, 0, unroll=4)


def basis_kernel(own_ref, first_ref, second_ref, inv_ref, edge_inv, v_ref, gram_ref, u, sums):
    core = lax.axis_index("core")
    lanes = lax.broadcasted_iota(jnp.int32, (8, 128), 1)
    first_lane, last_lane = lanes == 0, lanes == 127
    blank = jnp.zeros((8, 128), jnp.float32)

    for turn in range(2):
        for part in range(2):
            for row in range(8, 40, 8):
                u[turn, part, 0, pl.ds(row, 8), :] = blank
                u[turn, part, NZ + 1, pl.ds(row, 8), :] = blank

    def put(turn, tile, layer, inverse, re, im):
        a, b, c = inverse
        u[turn, 0, layer, pl.ds(8 + 8 * tile, 8), :] = a * re - c * im
        u[turn, 1, layer, pl.ds(8 + 8 * tile, 8), :] = b * im + c * re

    def prepare(sp, _):
        for turn in range(2):
            for part in range(2):
                for zz in range(2):
                    u[turn, part, 2 * sp + zz + 1, pl.ds(0, 8), :] = blank
                    u[turn, part, 2 * sp + zz + 1, pl.ds(40, 8), :] = blank
        for tile in range(4):
            for zz in range(2):
                if tile in (1, 2):
                    found = [inv_ref[i, tile - 1, sp, zz] for i in range(3)]
                    re, im = (own_ref[tile - 1, sp, 2 * part + zz] for part in range(2))
                else:
                    found = [edge_inv[i, tile // 3, sp, zz] for i in range(3)]
                    pair = []
                    for part in range(2):
                        at = HALO * (2 * part + zz)
                        wanted = at - (8 - HALO) if tile == 0 else at
                        start = min(max(wanted, 0), 4 * HALO - 8)
                        first, second = (ref[sp, pl.ds(start, 8), :] for ref in (first_ref, second_ref))
                        rows = jnp.where((core == 0) == (tile == 0), first, second)
                        shift = (start - wanted) % 8
                        pair.append(pltpu.roll(rows, shift, 0) if shift else rows)
                    re, im = pair
                put(0, tile, 2 * sp + zz + 1, found, re, im)
        return 0

    lax.fori_loop(0, NZ // 2, prepare, 0, unroll=4)

    def vector(j, side, sp, zz):
        if j == 0:
            return [own_ref[side, sp, 2 * part + zz] for part in range(2)]
        return [v_ref[j - 1, part, side, sp, zz] for part in range(2)]

    for j in range(STEPS):
        names = [name for name in entry if name[2] == j + 1 or (j == 0 and name[2] == 0)]

        def step(group, totals, j=j, names=names):
            by_layer = []
            for sp in [4 * group + s for s in range(4)]:
                found = {name: [] for name in names}
                for zz in range(2):
                    for tile in range(4) if j < STEPS - 1 else (1, 2):
                        layer, row = 2 * sp + zz + 1, 8 + 8 * tile
                        pair = []
                        for part in range(2):
                            old = u.at[j % 2, part]
                            here = old[layer, pl.ds(row, 8), :]
                            total = old[layer - 1, pl.ds(row, 8), :] + old[layer + 1, pl.ds(row, 8), :]
                            total = total + (old[layer, pl.ds(row - 1, 8), :] + old[layer, pl.ds(row + 1, 8), :])
                            total = total + (
                                jnp.where(first_lane, 0.0, pltpu.roll(here, 1, 1))
                                + jnp.where(last_lane, 0.0, pltpu.roll(here, 127, 1))
                            )
                            pair.append(total)
                        if tile in (1, 2):
                            side = tile - 1
                            if j < STEPS - 1:
                                for part in range(2):
                                    v_ref[j, part, side, sp, zz] = pair[part]
                            known = [vector(i, side, sp, zz) for i in range(j + 1)] + [pair]
                            for kind, i, k in names:
                                a, b = known[i], known[k]
                                if kind == "x":
                                    found[kind, i, k].append(a[0] * b[1] - a[1] * b[0])
                                else:
                                    part = ("re", "im").index(kind)
                                    found[kind, i, k].append(a[part] * b[part])
                        if j < STEPS - 1:
                            if tile in (1, 2):
                                inverse = [inv_ref[i, tile - 1, sp, zz] for i in range(3)]
                            else:
                                inverse = [edge_inv[i, tile // 3, sp, zz] for i in range(3)]
                            put((j + 1) % 2, tile, layer, inverse, *pair)
                by_layer.append([tree_sum(found[name]) for name in names])
            return tuple(t + tree_sum(list(parts)) for t, parts in zip(totals, zip(*by_layer)))

        totals = lax.fori_loop(0, NZ // 8, step, tuple(blank for _ in names), unroll=2)
        for name, total in zip(names, totals):
            sums[entry[name]] = total
    for spare in range(len(entry), sums.shape[0]):
        sums[spare] = blank

    rows = jnp.sum(sums[...], axis=1)
    column = jnp.sum(rows, axis=1, keepdims=True)
    where = lax.broadcasted_iota(jnp.int32, rows.shape, 0) == lax.broadcasted_iota(jnp.int32, rows.shape, 1)
    packed = jnp.sum(jnp.where(where, column, 0.0), axis=0, keepdims=True)
    gram_ref[...] = jnp.broadcast_to(packed[None], gram_ref.shape)


def multiplied(a, b):
    return (a[0] * b[0] - a[1] * b[1], a[0] * b[1] + a[1] * b[0])


def combine_kernel(count_ref, part_ref, own_ref, v_ref, inv_ref, out_ref):
    slot = lax.axis_index(SLOTS)
    ends = slot == 0
    low = lax.broadcasted_iota(jnp.int32, (8, 128), 1) < 64
    row = tree_sum([part_ref[i] for i in range(part_ref.shape[0])])

    def spread(name):
        return jnp.broadcast_to(row[:, entry[name] : entry[name] + 1], (8, 128))

    gram = {}
    for i, j in same:
        re, im = spread(("re", i, j)), spread(("im", i, j))
        real = jnp.where(ends, jnp.where(low, re, im), re + im)
        imag = jnp.where(ends, 0.0, spread(("x", i, j))) if j > i else jnp.zeros_like(real)
        gram[i, j] = (real, imag)

    count_lane = lax.broadcasted_iota(jnp.int32, (1, L), 1)
    count_a, count_b = (
        jnp.sum(jnp.where(count_lane == k, count_ref[...], 0).astype(jnp.float32), axis=1, keepdims=True)
        for k in (slot, jnp.where(ends, PAIRS, L - slot))
    )
    one, none = jnp.ones((8, 128), jnp.float32), jnp.zeros((8, 128), jnp.float32)
    poly, answer = [(one, none)], [(none, none) for _ in range(STEPS)]
    sizes = [jnp.sqrt(jnp.maximum(gram[i, i][0], 0.0)) for i in range(STEPS + 1)]
    doubt, scale = none, None
    for m in range(STEPS):
        in_a, in_b = (jnp.broadcast_to(jnp.where(m < count, 1.0, 0.0), (8, 128)) for count in (count_a, count_b))
        weight = jnp.where(ends, jnp.where(low, in_a, in_b), in_a + in_b)
        g00, g01, g11 = gram[0, 0][0], gram[0, 1], gram[1, 1][0]
        denominator = (g00 - 2.0 * g01[0] + g11) + norm_floor
        inverse = 1.0 / denominator
        coef = ((g00 - g01[0]) * inverse, g01[1] * inverse)
        size = jnp.abs(coef[0]) + jnp.abs(coef[1])
        length = jnp.sqrt(jnp.maximum(g00, 0.0))
        if m == 0:
            scale = size * length
        pair = sizes[0] + sizes[1]
        step_doubt = (gram_rounding * (1 + m / 2)) * pair * (sizes[0] + size * pair) * jnp.abs(inverse) * length
        doubt = doubt + jnp.where(weight > 0.0, step_doubt, none)
        for j, p in enumerate(poly):
            term = multiplied(coef, p)
            answer[j] = (answer[j][0] + weight * term[0], answer[j][1] + weight * term[1])
        if m == STEPS - 1:
            break
        rest = (1.0 - coef[0], -coef[1])
        padded = [None] + poly + [None]
        following = []
        for j in range(len(poly) + 1):
            kept = multiplied(rest, poly[j]) if j < len(poly) else (none, none)
            moved = multiplied(coef, poly[j - 1]) if j > 0 else (none, none)
            following.append((kept[0] + moved[0], kept[1] + moved[1]))
        poly = following
        rr = rest[0] * rest[0] + rest[1] * rest[1]
        cc = coef[0] * coef[0] + coef[1] * coef[1]
        rc = multiplied((rest[0], -rest[1]), coef)
        cr = (rc[0], -rc[1])
        size_rest = jnp.abs(rest[0]) + jnp.abs(rest[1])
        sizes = [size_rest * a + size * b for a, b in zip(sizes[:-1], sizes[1:])]

        def at(i, j):
            return gram[i, j] if i <= j else (gram[j, i][0], -gram[j, i][1])

        shrunk = {}
        top = STEPS - m
        for i in range(top):
            for j in range(i, top):
                a, b, d = at(i, j), at(i, j + 1), at(i + 1, j + 1)
                if i == j:
                    ab = multiplied(rc, b)
                    shrunk[i, j] = (rr * a[0] + 2.0 * ab[0] + cc * d[0], none)
                else:
                    ab, ac = multiplied(rc, b), multiplied(cr, at(i + 1, j))
                    shrunk[i, j] = tuple(rr * a[x] + (ab[x] + ac[x]) + cc * d[x] for x in range(2))
        gram = shrunk

    trusted = doubt <= error_allowed * scale
    weights = []
    for re, im in answer:
        re = jnp.where(trusted, re, jnp.nan)
        weights.append(
            (
                jnp.broadcast_to(re[:, 0:1], (8, 128)),
                jnp.broadcast_to(re[:, 127:128], (8, 128)),
                jnp.broadcast_to(im[:, 0:1], (8, 128)),
            )
        )

    def finish(sp, _):
        for side in range(2):
            for zz in range(2):
                res, ims = [], []
                for j, (wa, wb, wi) in enumerate(weights):
                    re, im = ((own_ref[side, sp, 2 * part + zz] if j == 0 else v_ref[j - 1, part, side, sp, zz]) for part in range(2))
                    res.append(wa * re - wi * im)
                    ims.append(wb * im + wi * re)
                re, im = tree_sum(res), tree_sum(ims)
                a, b, c = (inv_ref[i, side, sp, zz] for i in range(3))
                out_ref[16 * side + sp, 0, zz] = a * re - c * im
                out_ref[16 * side + sp, 1, zz] = b * im + c * re
        return 0

    lax.fori_loop(0, NZ // 2, finish, 0, unroll=2)


def slot_shifts():
    table = np.zeros((PAIRS, 4), np.float32)
    for slot in range(PAIRS):
        angle = 2 * math.pi * slot / L
        table[slot, :2] = (1 - decay * math.cos(angle)) / step_size
        table[slot, 2] = decay * math.sin(angle) / step_size
    table[0, 1] = (1 + decay) / step_size
    return table


def exchanged(blocks, axes):
    return lax.all_to_all(blocks, axes, split_axis=0, concat_axis=0, tiled=True)


VMEM = pl.BlockSpec(memory_space=pltpu.VMEM)
SMEM = pl.BlockSpec(memory_space=pltpu.SMEM)
ANY = pl.BlockSpec(memory_space=pl.ANY)


def f32(*shape):
    return pltpu.VMEM(shape, jnp.float32)


def held(x):
    return pltpu.with_memory_space_constraint(x, pltpu.MemorySpace.VMEM)


def in_hbm(x):
    return pltpu.with_memory_space_constraint(x, pltpu.MemorySpace.HBM)


def room(mebibytes):
    return pltpu.CompilerParams(vmem_limit_bytes=mebibytes * 2**20)


def together(residual, absorption, counts):
    chips = lax.axis_size("z")
    bands, rows = pl.pallas_call(
        bands_kernel,
        out_shape=(f32(16, 4, 2, 8, 128), f32(2, 2, 8, 128)),
        in_specs=[ANY, ANY],
        out_specs=(VMEM, VMEM),
        scratch_shapes=[pltpu.SemaphoreType.DMA((18,))],
        compiler_params=room(2),
        name="bands",
    )(in_hbm(residual), in_hbm(absorption))
    series = exchanged(bands, TM).reshape(L, 2, 8, 128)
    spectrum = pl.pallas_call(
        forward_kernel,
        out_shape=f32(PAIRS, 6, 8, 128),
        in_specs=[VMEM, VMEM],
        out_specs=VMEM,
        compiler_params=room(4),
        name="forward",
    )(held(series), held(rows))
    own = held(exchanged(spectrum, SLOTS).reshape(2, 16, 6, 8, 128))
    first, second, swap = pl.pallas_call(
        edges_kernel,
        out_shape=(f32(16, 4 * HALO, 128), f32(16, 4 * HALO, 128), f32(2, 16, 2, 8, 128)),
        in_specs=[VMEM],
        out_specs=(VMEM, VMEM, VMEM),
        compiler_params=room(2),
        name="edges",
    )(own)
    ups = [[(2 * i + core, 2 * i + 2 + core) for i in range(chips - 1)] for core in range(2)]
    downs = [[(b, a) for a, b in pairs] for pairs in ups]
    swap = lax.ppermute(swap, "core", [(0, 1), (1, 0)])
    first = lax.ppermute(first, TM, ups[0] + downs[1])
    second = lax.ppermute(second, TM, downs[0] + ups[1])
    inverses, edge_inverses = pl.pallas_call(
        inverses_kernel,
        out_shape=(f32(3, 2, 16, 2, 8, 128), f32(3, 2, 16, 2, 8, 128)),
        in_specs=[VMEM, VMEM],
        out_specs=(VMEM, VMEM),
        compiler_params=room(2),
        cost_estimate=pl.CostEstimate(flops=2 * 10**6, bytes_accessed=2 * 10**6, transcendentals=0),
        name="inverses",
    )(own, held(swap))
    basis, partial = pl.pallas_call(
        basis_kernel,
        out_shape=(f32(STEPS - 1, 2, 2, 16, 2, 8, 128), f32(8, 8, 128)),
        in_specs=[VMEM] * 5,
        out_specs=(VMEM, VMEM),
        scratch_shapes=[
            pltpu.VMEM((2, 2, NZ + 2, 48, 128), jnp.float32),
            pltpu.VMEM((80, 8, 128), jnp.float32),
        ],
        compiler_params=room(10),
        name="basis",
    )(own, held(first), held(second), held(inverses), held(edge_inverses))
    partials = exchanged(partial, "z")
    solved = pl.pallas_call(
        combine_kernel,
        out_shape=f32(PAIRS, 2, 2, 8, 128),
        in_specs=[VMEM, VMEM, VMEM, VMEM, VMEM],
        out_specs=VMEM,
        compiler_params=room(6),
        name="combine",
    )(held(counts.reshape(1, L)), held(partials), own, held(basis), held(inverses))
    gathered, *arguments = lax.optimization_barrier((exchanged(solved, SLOTS), residual, absorption, counts))
    values, failed = pl.pallas_call(
        inverse_kernel,
        out_shape=(f32(L, 2, 8, 128), pltpu.SMEM((1,), jnp.int32)),
        in_specs=[VMEM],
        out_specs=(VMEM, SMEM),
        compiler_params=room(4),
        name="inverse",
    )(held(gathered))
    return values, failed, arguments


def taken_kernel(*refs):
    count = len(refs) // 2
    copies = [pltpu.make_async_copy(refs[i], refs[count + i], refs[-1].at[i]) for i in range(count)]
    for copy in copies:
        copy.start()
    for copy in copies:
        copy.wait()


def taken(*arrays):
    return pl.pallas_call(
        taken_kernel,
        out_shape=tuple(f32(*a.shape) for a in arrays),
        in_specs=[ANY] * len(arrays),
        out_specs=(VMEM,) * len(arrays),
        scratch_shapes=[pltpu.SemaphoreType.DMA((len(arrays),))],
        compiler_params=room(2),
        name="taken",
    )(*(in_hbm(a) for a in arrays))


def to_steps(values, shape):
    bands = exchanged(values.reshape(16, 4, 2, 8, 128), TM)
    return bands.transpose(1, 2, 0, 3, 4).reshape(shape)


def body(residual, absorption, counts):
    values, failed, arguments = together(residual, absorption, counts)
    return lax.cond(
        failed[0] > 0,
        lambda r, a, c, v: stepwise(*taken(r, a), c),
        lambda r, a, c, v: to_steps(v, r.shape),
        *arguments, values,
    )


def solution(mesh):
    chips, cores = mesh.shape["tm"] // 2, 2
    devices = mesh.devices.reshape(chips, cores, 4, 4)
    inner = Mesh(devices, ("z", "core", "y", "x"))
    in_specs = (P(TM, SPACE, None, None), P(SPACE, None, None), P())
    out_specs = P(TM, SPACE, None, None)
    return jax.shard_map(body, mesh=inner, in_specs=in_specs, out_specs=out_specs, check_vma=False)
```

```python
import math

import jax
import jax.numpy as jnp
import numpy as np
from jax import lax
from jax.experimental import pallas as pl
from jax.experimental.pallas import tpu as pltpu
from jax.sharding import Mesh
from jax.sharding import PartitionSpec as P

L = 64
STEPS = 6
HALO = 6
BOTH = 4
NX = 128
NZ = 32
PAIRS = L // 2
TM = ("z", "core")
SPACE = ("y", "x")
SLOTS = ("core", "y", "x")

wrap_factor = 0.1
step_size = 1.0
norm_floor = 1e-06
highest = lax.Precision.HIGHEST
decay = wrap_factor ** (1.0 / L)

gram_rounding = 1.5e-6
error_allowed = 1.5e-4


def with_halo(cells, sides, width):
    for axis, dim in sides:
        count = lax.axis_size(axis)
        ends = count - 1
        head = lax.slice_in_dim(cells, 0, width, axis=dim)
        tail = lax.slice_in_dim(cells, cells.shape[dim] - width, cells.shape[dim], axis=dim)
        cells = jnp.concatenate(
            [
                lax.ppermute(tail, axis, [(i, (i + 1) % count) for i in range(ends)]),
                cells,
                lax.ppermute(head, axis, [((i + 1) % count, i) for i in range(ends)]),
            ],
            axis=dim,
        )
    return cells


def copy_for_each(shard, axis):
    copies = jnp.broadcast_to(shard, (lax.axis_size(axis), *shard.shape))
    return lax.all_to_all(copies, axis, split_axis=0, concat_axis=0, tiled=True)


def taken_together(shard, axis):
    return copy_for_each(shard, axis).sum(axis=0)


def packed_total(arrays, axis):
    vector, at, finished = (jnp.concatenate([a.reshape(-1) for a in arrays]), 0, [])
    so_far = taken_together(vector, axis)
    for a in arrays:
        finished.append(so_far[at : at + a.size].reshape(a.shape))
        at += a.size
    return tuple(finished)


def shifts(frequency):
    angles = frequency.astype(jnp.float32) * (2.0 * math.pi / L)
    decay_rate = wrap_factor ** (1.0 / L)
    shift_re = (1.0 - decay_rate * jnp.cos(angles)) / step_size
    shift_im = decay_rate * jnp.sin(angles) / step_size
    return (shift_re, shift_im)


def near_sum(padded):
    interior = padded[..., 1:-1, :, :]
    widths = [(0, 0)] * (interior.ndim - 2) + [(1, 1), (1, 1)]
    padded_xy = jnp.pad(interior, widths)
    summed = padded[..., 2:, :, :] + padded[..., :-2, :, :]
    summed = summed + padded_xy[..., 2:, 1:-1] + padded_xy[..., :-2, 1:-1]
    summed = summed + padded_xy[..., 1:-1, 2:] + padded_xy[..., 1:-1, :-2]
    return summed


def advance(carried, dir_re, dir_im, img_re, img_im, coef_re, coef_im):
    sol_re, sol_im, res_re, res_im = carried
    sol_re = sol_re + coef_re * dir_re - coef_im * dir_im
    sol_im = sol_im + coef_re * dir_im + coef_im * dir_re
    res_re = res_re - (coef_re * img_re - coef_im * img_im)
    res_im = res_im - (coef_re * img_im + coef_im * img_re)
    return (sol_re, sol_im, res_re, res_im)


def solve_together(spectrum, absorption, frequencies, step_counts, longest):
    shift_re, shift_im = shifts(frequencies)
    shift_re = shift_re[:, None, None, None]
    shift_im = shift_im[:, None, None, None]
    diag_re = shift_re + 6.0 + absorption[None]
    magnitude = diag_re * diag_re + shift_im * shift_im
    inv_re = diag_re / magnitude
    inv_im = -shift_im / magnitude

    def iterate(iteration, carried):
        res_re, res_im = (carried[2], carried[3])
        dir_re = inv_re * res_re - inv_im * res_im
        dir_im = inv_re * res_im + inv_im * res_re
        padded = with_halo(jnp.stack([dir_re, dir_im], axis=1), ((SPACE, 2),), 1)
        nearby = near_sum(padded)
        img_re = diag_re * dir_re - shift_im * dir_im - nearby[:, 0]
        img_im = diag_re * dir_im + shift_im * dir_re - nearby[:, 1]
        totals = packed_total(
            (
                jnp.sum(img_re * res_re + img_im * res_im, axis=(1, 2, 3)),
                jnp.sum(img_re * res_im - img_im * res_re, axis=(1, 2, 3)),
                jnp.sum(img_re * img_re + img_im * img_im, axis=(1, 2, 3)),
            ),
            SPACE,
        )
        active = iteration < step_counts
        denominator = totals[2] + norm_floor
        coef_re = jnp.where(active, totals[0] / denominator, 0.0)[:, None, None, None]
        coef_im = jnp.where(active, totals[1] / denominator, 0.0)[:, None, None, None]
        return advance(carried, dir_re, dir_im, img_re, img_im, coef_re, coef_im)

    blank = jnp.zeros_like(spectrum[:, 0])
    finished = lax.fori_loop(0, longest, iterate, (blank, blank, spectrum[:, 0], spectrum[:, 1]))
    return jnp.stack([finished[0], finished[1]], axis=1)


def slot_order():
    return jnp.arange(L, dtype=jnp.int32)


def phase_table(left, right):
    return (left[:, None] * right[None, :] % L).astype(jnp.float32) * (2.0 * math.pi / L)


def stepwise(residual, absorption, counts):
    per_device = residual.shape[0]
    decay_rate = wrap_factor ** (1.0 / L)
    first_step = lax.axis_index(TM) * per_device
    times_here = first_step + jnp.arange(per_device, dtype=jnp.int32)
    scaled = residual * jnp.power(decay_rate, times_here.astype(jnp.float32))[:, None, None, None]
    slot_freqs = slot_order()
    own_freqs = lax.dynamic_slice_in_dim(slot_freqs, first_step, per_device)
    own_counts = counts[own_freqs]
    longest = jnp.max(counts)
    all_times = jnp.arange(L, dtype=jnp.int32)
    series = lax.all_to_all(scaled, TM, split_axis=2, concat_axis=0, tiled=True)
    phases = phase_table(slot_freqs, all_times)
    real_part = jnp.einsum("sn,nzxy->szxy", jnp.cos(phases), series, precision=highest)
    imag_part = -jnp.einsum("sn,nzxy->szxy", jnp.sin(phases), series, precision=highest)
    spectrum = lax.all_to_all(
        jnp.stack([real_part, imag_part], axis=1), TM, split_axis=0, concat_axis=3, tiled=True
    )
    solved = solve_together(spectrum, absorption, own_freqs, own_counts, longest)
    gathered = lax.all_to_all(solved, TM, split_axis=3, concat_axis=0, tiled=True)
    phases = phase_table(all_times, slot_freqs)
    values = jnp.einsum("ns,szxy->nzxy", jnp.cos(phases), gathered[:, 0], precision=highest)
    values = values - jnp.einsum(
        "ns,szxy->nzxy", jnp.sin(phases), gathered[:, 1], precision=highest
    )
    weight = jnp.power(decay_rate, -all_times.astype(jnp.float32)) / L
    values = values * weight[:, None, None, None]
    return lax.all_to_all(values, TM, split_axis=0, concat_axis=2, tiled=True)


def real_transform(x):
    n = len(x)
    if n == 2:
        return [(x[0] + x[1], None), (x[0] - x[1], None)]
    even, odd = real_transform(x[0::2]), real_transform(x[1::2])
    out = [None] * (n // 2 + 1)
    out[0] = (even[0][0] + odd[0][0], None)
    out[n // 2] = (even[0][0] - odd[0][0], None)
    out[n // 4] = (even[n // 4][0], -odd[n // 4][0])
    for k in range(1, n // 4):
        cos, sin = math.cos(2 * math.pi * k / n), math.sin(2 * math.pi * k / n)
        (er, ei), (cr, ci) = even[k], odd[k]
        tr, ti = cos * cr + sin * ci, cos * ci - sin * cr
        out[k] = (er + tr, ei + ti)
        out[n // 2 - k] = (er - tr, ti - ei)
    return out


def real_inverse(spectrum):
    n = 2 * (len(spectrum) - 1)
    first, last = spectrum[0][0], spectrum[n // 2][0]
    if n == 2:
        return [first + last, first - last]
    even, odd = [None] * (n // 4 + 1), [None] * (n // 4 + 1)
    even[0], odd[0] = (first + last, None), (first - last, None)
    mid_re, mid_im = spectrum[n // 4]
    even[n // 4], odd[n // 4] = (mid_re + mid_re, None), (-(mid_im + mid_im), None)
    for k in range(1, n // 4):
        cos, sin = math.cos(2 * math.pi * k / n), math.sin(2 * math.pi * k / n)
        (ar, ai), (br, bi) = spectrum[k], spectrum[n // 2 - k]
        even[k] = (ar + br, ai - bi)
        tr, ti = ar - br, ai + bi
        odd[k] = (cos * tr - sin * ti, cos * ti + sin * tr)
    halves = real_inverse(even), real_inverse(odd)
    return [halves[i % 2][i // 2] for i in range(n)]


def bands_kernel(x_ref, a_ref, out_ref, rows_ref, sems):
    copies = [
        pltpu.make_async_copy(x_ref.at[:, :, pl.ds(8 * band, 8), :], out_ref.at[band], sems.at[band]) for band in range(16)
    ]
    first = 16 * lax.axis_index("z") + 16 * lax.axis_index("core") - 8
    for core in range(2):
        row = pl.multiple_of(jnp.clip(first + 8 * core, 0, NX - 8), 8)
        copies.append(pltpu.make_async_copy(a_ref.at[:, pl.ds(row, 8), :], rows_ref.at[core], sems.at[16 + core]))
    for copy in copies:
        copy.start()
    for copy in copies:
        copy.wait()


def forward_kernel(x_ref, rows_ref, out_ref):
    for core in range(2):
        for zz in range(2):
            rows = rows_ref[core, zz]
            for slot in range(16 * core, 16 * core + 16):
                out_ref[slot, 4 + zz] = rows
    for zz in range(2):
        spectrum = real_transform([x_ref[n, zz] * decay**n for n in range(L)])
        out_ref[0, zz] = spectrum[0][0]
        out_ref[0, 2 + zz] = spectrum[PAIRS][0]
        for k in range(1, PAIRS):
            out_ref[k, zz] = spectrum[k][0]
            out_ref[k, 2 + zz] = spectrum[k][1]


def inverse_kernel(s_ref, out_ref, failed_ref):
    failed = jnp.zeros((8, 128), jnp.float32)
    for zz in range(2):
        ends = [s_ref[0, part, zz] for part in range(2)]
        spectrum = [(ends[0] + ends[0], None)]
        spectrum += [(s_ref[k, 0, zz], s_ref[k, 1, zz]) for k in range(1, PAIRS)]
        spectrum += [(ends[1] + ends[1], None)]
        values = real_inverse(spectrum)
        for n in range(L):
            out_ref[n, zz] = values[n] * (decay ** (-n) / (2 * L))
        failed = jnp.where(values[0] != values[0], 1.0, failed)
    failed_ref[0] = jnp.where(jnp.max(failed) > 0.0, 1, 0)


same = [(i, j) for i in range(STEPS + 1) for j in range(i, STEPS + 1)]
cross = [(i, j) for i in range(STEPS + 1) for j in range(i + 1, STEPS + 1)]
entry = {(kind, i, j): None for kind, ij in (("re", same), ("im", same), ("x", cross)) for i, j in ij}
for at, name in enumerate(entry):
    entry[name] = at


def tree_sum(terms):
    while len(terms) > 1:
        terms = [sum(terms[i : i + 2][1:], terms[i]) for i in range(0, len(terms), 2)]
    return terms[0]


def pick(slot, values):
    found = jnp.float32(values[0])
    for i in range(1, len(values)):
        found = jnp.where(slot == i, jnp.float32(values[i]), found)
    return found


def edges_kernel(own_ref, first_ref, second_ref, abs_ref):
    low = lax.axis_index("core") == 0
    for sp in range(16):
        for i in range(4):
            up, down = own_ref[1, sp, i, pl.ds(8 - HALO, HALO), :], own_ref[0, sp, i, pl.ds(0, HALO), :]
            first_ref[sp, pl.ds(HALO * i, HALO), :] = jnp.where(low, up, down)
            second_ref[sp, pl.ds(HALO * i, HALO), :] = jnp.where(low, down, up)
        for side in range(2):
            for zz in range(2):
                abs_ref[side, sp, zz] = own_ref[side, sp, 4 + zz]


def inverses_kernel(own_ref, swap_ref, inv_ref, edge_inv_ref):
    slot, z, core = lax.axis_index(SLOTS), lax.axis_index("z"), lax.axis_index("core")
    upper = lax.broadcasted_iota(jnp.int32, (8, 128), 0) < 4
    shifts_here = slot_shifts()
    shift_a, shift_b, shift_im = (pick(slot, shifts_here[:, i]) for i in range(3))

    def prepare(sp, _):
        edges = {}
        for tile in range(4):
            for zz in range(2):
                mine, other = own_ref[tile // 2, sp, 4 + zz], swap_ref[tile // 2, sp, zz]
                base = jnp.where(core == tile % 2, mine, other)
                da, db = (shift_a + 6.0) + base, (shift_b + 6.0) + base
                ra, rb = 1.0 / (da * da + shift_im * shift_im), 1.0 / (db * db + shift_im * shift_im)
                found = [da * ra, db * rb, -shift_im * ra]
                if tile in (1, 2):
                    for i in range(3):
                        inv_ref[i, tile - 1, sp, zz] = found[i]
                else:
                    inside = z > 0 if tile == 0 else z < lax.axis_size("z") - 1
                    for i in range(3):
                        edges[tile, zz, i] = jnp.where(inside, found[i], 0.0)
                        edge_inv_ref[i, tile // 3, sp, zz] = edges[tile, zz, i]
        for zz in range(2):
            for i in range(3):
                edge_inv_ref[i, 2, sp, zz] = jnp.where(upper, edges[3, zz, i], edges[0, zz, i])
        return 0

    lax.fori_loop(0, NZ // 2, prepare, 0, unroll=4)


def basis_kernel(own_ref, first_ref, second_ref, inv_ref, edge_inv, v_ref, gram_ref, u, sums):
    core = lax.axis_index("core")
    lanes = lax.broadcasted_iota(jnp.int32, (8, 128), 1)
    first_lane, last_lane = lanes == 0, lanes == 127
    upper = lax.broadcasted_iota(jnp.int32, (8, 128), 0) < 4
    blank = jnp.zeros((8, 128), jnp.float32)

    for turn in range(2):
        for part in range(2):
            for row in range(8, 40, 8):
                u[turn, part, 0, pl.ds(row, 8), :] = blank
                u[turn, part, NZ + 1, pl.ds(row, 8), :] = blank

    def put(turn, tiles, layer, inverse, re, im):
        a, b, c = inverse
        pair = a * re - c * im, b * im + c * re
        for tile in tiles:
            for part in range(2):
                u[turn, part, layer, pl.ds(8 + 8 * tile, 8), :] = pair[part]

    def prepare(sp, _):
        for turn in range(2):
            for part in range(2):
                for zz in range(2):
                    u[turn, part, 2 * sp + zz + 1, pl.ds(0, 8), :] = blank
                    u[turn, part, 2 * sp + zz + 1, pl.ds(40, 8), :] = blank
        for tile in range(4):
            for zz in range(2):
                if tile in (1, 2):
                    found = [inv_ref[i, tile - 1, sp, zz] for i in range(3)]
                    re, im = (own_ref[tile - 1, sp, 2 * part + zz] for part in range(2))
                else:
                    found = [edge_inv[i, tile // 3, sp, zz] for i in range(3)]
                    pair = []
                    for part in range(2):
                        at = HALO * (2 * part + zz)
                        wanted = at - (8 - HALO) if tile == 0 else at
                        start = min(max(wanted, 0), 4 * HALO - 8)
                        first, second = (ref[sp, pl.ds(start, 8), :] for ref in (first_ref, second_ref))
                        rows = jnp.where((core == 0) == (tile == 0), first, second)
                        shift = (start - wanted) % 8
                        pair.append(pltpu.roll(rows, shift, 0) if shift else rows)
                    re, im = pair
                put(0, (tile,), 2 * sp + zz + 1, found, re, im)
        return 0

    lax.fori_loop(0, NZ // 2, prepare, 0, unroll=4)

    def vector(j, side, sp, zz):
        if j == 0:
            return [own_ref[side, sp, 2 * part + zz] for part in range(2)]
        return [v_ref[j - 1, part, side, sp, zz] for part in range(2)]

    def nearby(old, tile, layer, j):
        def rows(z_off, x_off):
            before, behind = (old[layer + z_off, pl.ds(row + x_off, 8), :] for row in (8, 32))
            if j == 1:
                return jnp.where(upper, behind, before)
            return behind if x_off < 0 else before

        if tile != BOTH:
            def rows(z_off, x_off):
                return old[layer + z_off, pl.ds(8 + 8 * tile + x_off, 8), :]

        here = rows(0, 0)
        total = (rows(-1, 0) + rows(1, 0)) + (rows(0, -1) + rows(0, 1))
        return total + (
            jnp.where(first_lane, 0.0, pltpu.roll(here, 1, 1)) + jnp.where(last_lane, 0.0, pltpu.roll(here, 127, 1))
        )

    for j in range(STEPS):
        tiles = (0, 1, 2, 3) if j == 0 else (1, 2, BOTH) if j < STEPS - 1 else (1, 2)
        names = [name for name in entry if name[2] == j + 1 or (j == 0 and name[2] == 0)]

        def step(group, totals, j=j, names=names, tiles=tiles):
            found = {}
            for sp in [4 * group + s for s in range(4)]:
                for zz in range(2):
                    for tile in tiles:
                        layer = 2 * sp + zz + 1
                        pair = [nearby(u.at[j % 2, part], tile, layer, j) for part in range(2)]
                        if tile in (1, 2):
                            side = tile - 1
                            if j < STEPS - 1:
                                for part in range(2):
                                    v_ref[j, part, side, sp, zz] = pair[part]
                            known = [vector(i, side, sp, zz) for i in range(j + 1)] + [pair]
                            for kind, i, k in names:
                                a, b = known[i], known[k]
                                if kind == "x":
                                    product = a[0] * b[1] - a[1] * b[0]
                                else:
                                    part = ("re", "im").index(kind)
                                    product = a[part] * b[part]
                                name = kind, i, k
                                found[name] = found[name] + product if name in found else product
                        if j < STEPS - 1:
                            if tile in (1, 2):
                                inverse = [inv_ref[i, tile - 1, sp, zz] for i in range(3)]
                            else:
                                inverse = [edge_inv[i, (0, None, None, 1, 2)[tile], sp, zz] for i in range(3)]
                            put((j + 1) % 2, (0, 3) if tile == BOTH else (tile,), layer, inverse, *pair)
            return tuple(t + found[name] for t, name in zip(totals, names))

        totals = lax.fori_loop(0, NZ // 8, step, tuple(blank for _ in names), unroll=2)
        for name, total in zip(names, totals):
            sums[entry[name]] = total
    for spare in range(len(entry), sums.shape[0]):
        sums[spare] = blank

    rows = jnp.sum(sums[...], axis=1)
    column = jnp.sum(rows, axis=1, keepdims=True)
    where = lax.broadcasted_iota(jnp.int32, rows.shape, 0) == lax.broadcasted_iota(jnp.int32, rows.shape, 1)
    packed = jnp.sum(jnp.where(where, column, 0.0), axis=0, keepdims=True)
    gram_ref[...] = jnp.broadcast_to(packed[None], gram_ref.shape)


def multiplied(a, b):
    return (a[0] * b[0] - a[1] * b[1], a[0] * b[1] + a[1] * b[0])


def combine_kernel(count_ref, part_ref, own_ref, v_ref, inv_ref, out_ref):
    slot = lax.axis_index(SLOTS)
    ends = slot == 0
    low = lax.broadcasted_iota(jnp.int32, (8, 128), 1) < 64
    row = tree_sum([part_ref[i] for i in range(part_ref.shape[0])])

    def spread(name):
        return jnp.broadcast_to(row[:, entry[name] : entry[name] + 1], (8, 128))

    gram = {}
    for i, j in same:
        re, im = spread(("re", i, j)), spread(("im", i, j))
        real = jnp.where(ends, jnp.where(low, re, im), re + im)
        imag = jnp.where(ends, 0.0, spread(("x", i, j))) if j > i else jnp.zeros_like(real)
        gram[i, j] = (real, imag)

    count_lane = lax.broadcasted_iota(jnp.int32, (1, L), 1)
    count_a, count_b = (
        jnp.sum(jnp.where(count_lane == k, count_ref[...], 0).astype(jnp.float32), axis=1, keepdims=True)
        for k in (slot, jnp.where(ends, PAIRS, L - slot))
    )
    one, none = jnp.ones((8, 128), jnp.float32), jnp.zeros((8, 128), jnp.float32)
    poly, answer = [(one, none)], [(none, none) for _ in range(STEPS)]
    sizes = [jnp.sqrt(jnp.maximum(gram[i, i][0], 0.0)) for i in range(STEPS + 1)]
    doubt, scale = none, None
    for m in range(STEPS):
        in_a, in_b = (jnp.broadcast_to(jnp.where(m < count, 1.0, 0.0), (8, 128)) for count in (count_a, count_b))
        weight = jnp.where(ends, jnp.where(low, in_a, in_b), in_a + in_b)
        g00, g01, g11 = gram[0, 0][0], gram[0, 1], gram[1, 1][0]
        denominator = (g00 - 2.0 * g01[0] + g11) + norm_floor
        inverse = 1.0 / denominator
        coef = ((g00 - g01[0]) * inverse, g01[1] * inverse)
        size = jnp.abs(coef[0]) + jnp.abs(coef[1])
        length = jnp.sqrt(jnp.maximum(g00, 0.0))
        if m == 0:
            scale = size * length
        pair = sizes[0] + sizes[1]
        step_doubt = (gram_rounding * (1 + m / 2)) * pair * (sizes[0] + size * pair) * jnp.abs(inverse) * length
        doubt = doubt + jnp.where(weight > 0.0, step_doubt, none)
        for j, p in enumerate(poly):
            term = multiplied(coef, p)
            answer[j] = (answer[j][0] + weight * term[0], answer[j][1] + weight * term[1])
        if m == STEPS - 1:
            break
        rest = (1.0 - coef[0], -coef[1])
        padded = [None] + poly + [None]
        following = []
        for j in range(len(poly) + 1):
            kept = multiplied(rest, poly[j]) if j < len(poly) else (none, none)
            moved = multiplied(coef, poly[j - 1]) if j > 0 else (none, none)
            following.append((kept[0] + moved[0], kept[1] + moved[1]))
        poly = following
        rr = rest[0] * rest[0] + rest[1] * rest[1]
        cc = coef[0] * coef[0] + coef[1] * coef[1]
        rc = multiplied((rest[0], -rest[1]), coef)
        cr = (rc[0], -rc[1])
        size_rest = jnp.abs(rest[0]) + jnp.abs(rest[1])
        sizes = [size_rest * a + size * b for a, b in zip(sizes[:-1], sizes[1:])]

        def at(i, j):
            return gram[i, j] if i <= j else (gram[j, i][0], -gram[j, i][1])

        shrunk = {}
        top = STEPS - m
        for i in range(top):
            for j in range(i, top):
                a, b, d = at(i, j), at(i, j + 1), at(i + 1, j + 1)
                if i == j:
                    ab = multiplied(rc, b)
                    shrunk[i, j] = (rr * a[0] + 2.0 * ab[0] + cc * d[0], none)
                else:
                    ab, ac = multiplied(rc, b), multiplied(cr, at(i + 1, j))
                    shrunk[i, j] = tuple(rr * a[x] + (ab[x] + ac[x]) + cc * d[x] for x in range(2))
        gram = shrunk

    trusted = doubt <= error_allowed * scale
    weights = []
    for re, im in answer:
        re = jnp.where(trusted, re, jnp.nan)
        weights.append(
            (
                jnp.broadcast_to(re[:, 0:1], (8, 128)),
                jnp.broadcast_to(re[:, 127:128], (8, 128)),
                jnp.broadcast_to(im[:, 0:1], (8, 128)),
            )
        )

    def finish(sp, _):
        for side in range(2):
            for zz in range(2):
                res, ims = [], []
                for j, (wa, wb, wi) in enumerate(weights):
                    re, im = ((own_ref[side, sp, 2 * part + zz] if j == 0 else v_ref[j - 1, part, side, sp, zz]) for part in range(2))
                    res.append(wa * re - wi * im)
                    ims.append(wb * im + wi * re)
                re, im = tree_sum(res), tree_sum(ims)
                a, b, c = (inv_ref[i, side, sp, zz] for i in range(3))
                out_ref[16 * side + sp, 0, zz] = a * re - c * im
                out_ref[16 * side + sp, 1, zz] = b * im + c * re
        return 0

    lax.fori_loop(0, NZ // 2, finish, 0, unroll=2)


def slot_shifts():
    table = np.zeros((PAIRS, 4), np.float32)
    for slot in range(PAIRS):
        angle = 2 * math.pi * slot / L
        table[slot, :2] = (1 - decay * math.cos(angle)) / step_size
        table[slot, 2] = decay * math.sin(angle) / step_size
    table[0, 1] = (1 + decay) / step_size
    return table


def exchanged(blocks, axes):
    return lax.all_to_all(blocks, axes, split_axis=0, concat_axis=0, tiled=True)


VMEM = pl.BlockSpec(memory_space=pltpu.VMEM)
SMEM = pl.BlockSpec(memory_space=pltpu.SMEM)
ANY = pl.BlockSpec(memory_space=pl.ANY)


def f32(*shape):
    return pltpu.VMEM(shape, jnp.float32)


def held(x):
    return pltpu.with_memory_space_constraint(x, pltpu.MemorySpace.VMEM)


def in_hbm(x):
    return pltpu.with_memory_space_constraint(x, pltpu.MemorySpace.HBM)


def room(mebibytes):
    return pltpu.CompilerParams(vmem_limit_bytes=mebibytes * 2**20)


def together(residual, absorption, counts):
    chips = lax.axis_size("z")
    bands, rows = pl.pallas_call(
        bands_kernel,
        out_shape=(f32(16, 4, 2, 8, 128), f32(2, 2, 8, 128)),
        in_specs=[ANY, ANY],
        out_specs=(VMEM, VMEM),
        scratch_shapes=[pltpu.SemaphoreType.DMA((18,))],
        compiler_params=room(2),
        name="bands",
    )(in_hbm(residual), in_hbm(absorption))
    series = exchanged(bands, TM).reshape(L, 2, 8, 128)
    spectrum = pl.pallas_call(
        forward_kernel,
        out_shape=f32(PAIRS, 6, 8, 128),
        in_specs=[VMEM, VMEM],
        out_specs=VMEM,
        compiler_params=room(4),
        name="forward",
    )(held(series), held(rows))
    own = held(exchanged(spectrum, SLOTS).reshape(2, 16, 6, 8, 128))
    first, second, swap = pl.pallas_call(
        edges_kernel,
        out_shape=(f32(16, 4 * HALO, 128), f32(16, 4 * HALO, 128), f32(2, 16, 2, 8, 128)),
        in_specs=[VMEM],
        out_specs=(VMEM, VMEM, VMEM),
        compiler_params=room(2),
        name="edges",
    )(own)
    ups = [[(2 * i + core, 2 * i + 2 + core) for i in range(chips - 1)] for core in range(2)]
    downs = [[(b, a) for a, b in pairs] for pairs in ups]
    swap = lax.ppermute(swap, "core", [(0, 1), (1, 0)])
    first = lax.ppermute(first, TM, ups[0] + downs[1])
    second = lax.ppermute(second, TM, downs[0] + ups[1])
    inverses, edge_inverses = pl.pallas_call(
        inverses_kernel,
        out_shape=(f32(3, 2, 16, 2, 8, 128), f32(3, 3, 16, 2, 8, 128)),
        in_specs=[VMEM, VMEM],
        out_specs=(VMEM, VMEM),
        compiler_params=room(2),
        cost_estimate=pl.CostEstimate(flops=2 * 10**6, bytes_accessed=2 * 10**6, transcendentals=0),
        name="inverses",
    )(own, held(swap))
    basis, partial = pl.pallas_call(
        basis_kernel,
        out_shape=(f32(STEPS - 1, 2, 2, 16, 2, 8, 128), f32(8, 8, 128)),
        in_specs=[VMEM] * 5,
        out_specs=(VMEM, VMEM),
        scratch_shapes=[
            pltpu.VMEM((2, 2, NZ + 2, 48, 128), jnp.float32),
            pltpu.VMEM((80, 8, 128), jnp.float32),
        ],
        compiler_params=room(10),
        name="basis",
    )(own, held(first), held(second), held(inverses), held(edge_inverses))
    partials = exchanged(partial, "z")
    solved = pl.pallas_call(
        combine_kernel,
        out_shape=f32(PAIRS, 2, 2, 8, 128),
        in_specs=[VMEM, VMEM, VMEM, VMEM, VMEM],
        out_specs=VMEM,
        compiler_params=room(6),
        name="combine",
    )(held(counts.reshape(1, L)), held(partials), own, held(basis), held(inverses))
    gathered, *arguments = lax.optimization_barrier((exchanged(solved, SLOTS), residual, absorption, counts))
    values, failed = pl.pallas_call(
        inverse_kernel,
        out_shape=(f32(L, 2, 8, 128), pltpu.SMEM((1,), jnp.int32)),
        in_specs=[VMEM],
        out_specs=(VMEM, SMEM),
        compiler_params=room(4),
        name="inverse",
    )(held(gathered))
    return values, failed, arguments


def taken_kernel(*refs):
    count = len(refs) // 2
    copies = [pltpu.make_async_copy(refs[i], refs[count + i], refs[-1].at[i]) for i in range(count)]
    for copy in copies:
        copy.start()
    for copy in copies:
        copy.wait()


def taken(*arrays):
    return pl.pallas_call(
        taken_kernel,
        out_shape=tuple(f32(*a.shape) for a in arrays),
        in_specs=[ANY] * len(arrays),
        out_specs=(VMEM,) * len(arrays),
        scratch_shapes=[pltpu.SemaphoreType.DMA((len(arrays),))],
        compiler_params=room(2),
        name="taken",
    )(*(in_hbm(a) for a in arrays))


def to_steps(values, shape):
    bands = exchanged(values.reshape(16, 4, 2, 8, 128), TM)
    return bands.transpose(1, 2, 0, 3, 4).reshape(shape)


def body(residual, absorption, counts):
    values, failed, arguments = together(residual, absorption, counts)
    return lax.cond(
        failed[0] > 0,
        lambda r, a, c, v: stepwise(*taken(r, a), c),
        lambda r, a, c, v: to_steps(v, r.shape),
        *arguments, values,
    )


def solution(mesh):
    chips, cores = mesh.shape["tm"] // 2, 2
    devices = mesh.devices.reshape(chips, cores, 4, 4)
    inner = Mesh(devices, ("z", "core", "y", "x"))
    in_specs = (P(TM, SPACE, None, None), P(SPACE, None, None), P())
    out_specs = P(TM, SPACE, None, None)
    return jax.shard_map(body, mesh=inner, in_specs=in_specs, out_specs=out_specs, check_vma=False)
```

```python
import math

import jax
import jax.numpy as jnp
import numpy as np
from jax import lax
from jax.experimental import pallas as pl
from jax.experimental.pallas import tpu as pltpu
from jax.sharding import Mesh
from jax.sharding import PartitionSpec as P

L = 64
STEPS = 6
HALO = 6
BOTH = 4
NX = 128
NZ = 32
PAIRS = L // 2
TM = ("z", "core")
SPACE = ("y", "x")
SLOTS = ("core", "y", "x")

wrap_factor = 0.1
step_size = 1.0
norm_floor = 1e-06
highest = lax.Precision.HIGHEST
decay = wrap_factor ** (1.0 / L)

gram_rounding = 1.5e-6
error_allowed = 1.5e-4


def with_halo(cells, sides, width):
    for axis, dim in sides:
        count = lax.axis_size(axis)
        ends = count - 1
        head = lax.slice_in_dim(cells, 0, width, axis=dim)
        tail = lax.slice_in_dim(cells, cells.shape[dim] - width, cells.shape[dim], axis=dim)
        cells = jnp.concatenate(
            [
                lax.ppermute(tail, axis, [(i, (i + 1) % count) for i in range(ends)]),
                cells,
                lax.ppermute(head, axis, [((i + 1) % count, i) for i in range(ends)]),
            ],
            axis=dim,
        )
    return cells


def copy_for_each(shard, axis):
    copies = jnp.broadcast_to(shard, (lax.axis_size(axis), *shard.shape))
    return lax.all_to_all(copies, axis, split_axis=0, concat_axis=0, tiled=True)


def taken_together(shard, axis):
    return copy_for_each(shard, axis).sum(axis=0)


def packed_total(arrays, axis):
    vector, at, finished = (jnp.concatenate([a.reshape(-1) for a in arrays]), 0, [])
    so_far = taken_together(vector, axis)
    for a in arrays:
        finished.append(so_far[at : at + a.size].reshape(a.shape))
        at += a.size
    return tuple(finished)


def shifts(frequency):
    angles = frequency.astype(jnp.float32) * (2.0 * math.pi / L)
    decay_rate = wrap_factor ** (1.0 / L)
    shift_re = (1.0 - decay_rate * jnp.cos(angles)) / step_size
    shift_im = decay_rate * jnp.sin(angles) / step_size
    return (shift_re, shift_im)


def near_sum(padded):
    interior = padded[..., 1:-1, :, :]
    widths = [(0, 0)] * (interior.ndim - 2) + [(1, 1), (1, 1)]
    padded_xy = jnp.pad(interior, widths)
    summed = padded[..., 2:, :, :] + padded[..., :-2, :, :]
    summed = summed + padded_xy[..., 2:, 1:-1] + padded_xy[..., :-2, 1:-1]
    summed = summed + padded_xy[..., 1:-1, 2:] + padded_xy[..., 1:-1, :-2]
    return summed


def advance(carried, dir_re, dir_im, img_re, img_im, coef_re, coef_im):
    sol_re, sol_im, res_re, res_im = carried
    sol_re = sol_re + coef_re * dir_re - coef_im * dir_im
    sol_im = sol_im + coef_re * dir_im + coef_im * dir_re
    res_re = res_re - (coef_re * img_re - coef_im * img_im)
    res_im = res_im - (coef_re * img_im + coef_im * img_re)
    return (sol_re, sol_im, res_re, res_im)


def solve_together(spectrum, absorption, frequencies, step_counts, longest):
    shift_re, shift_im = shifts(frequencies)
    shift_re = shift_re[:, None, None, None]
    shift_im = shift_im[:, None, None, None]
    diag_re = shift_re + 6.0 + absorption[None]
    magnitude = diag_re * diag_re + shift_im * shift_im
    inv_re = diag_re / magnitude
    inv_im = -shift_im / magnitude

    def iterate(iteration, carried):
        res_re, res_im = (carried[2], carried[3])
        dir_re = inv_re * res_re - inv_im * res_im
        dir_im = inv_re * res_im + inv_im * res_re
        padded = with_halo(jnp.stack([dir_re, dir_im], axis=1), ((SPACE, 2),), 1)
        nearby = near_sum(padded)
        img_re = diag_re * dir_re - shift_im * dir_im - nearby[:, 0]
        img_im = diag_re * dir_im + shift_im * dir_re - nearby[:, 1]
        totals = packed_total(
            (
                jnp.sum(img_re * res_re + img_im * res_im, axis=(1, 2, 3)),
                jnp.sum(img_re * res_im - img_im * res_re, axis=(1, 2, 3)),
                jnp.sum(img_re * img_re + img_im * img_im, axis=(1, 2, 3)),
            ),
            SPACE,
        )
        active = iteration < step_counts
        denominator = totals[2] + norm_floor
        coef_re = jnp.where(active, totals[0] / denominator, 0.0)[:, None, None, None]
        coef_im = jnp.where(active, totals[1] / denominator, 0.0)[:, None, None, None]
        return advance(carried, dir_re, dir_im, img_re, img_im, coef_re, coef_im)

    blank = jnp.zeros_like(spectrum[:, 0])
    finished = lax.fori_loop(0, longest, iterate, (blank, blank, spectrum[:, 0], spectrum[:, 1]))
    return jnp.stack([finished[0], finished[1]], axis=1)


def slot_order():
    return jnp.arange(L, dtype=jnp.int32)


def phase_table(left, right):
    return (left[:, None] * right[None, :] % L).astype(jnp.float32) * (2.0 * math.pi / L)


def stepwise(residual, absorption, counts):
    per_device = residual.shape[0]
    decay_rate = wrap_factor ** (1.0 / L)
    first_step = lax.axis_index(TM) * per_device
    times_here = first_step + jnp.arange(per_device, dtype=jnp.int32)
    scaled = residual * jnp.power(decay_rate, times_here.astype(jnp.float32))[:, None, None, None]
    slot_freqs = slot_order()
    own_freqs = lax.dynamic_slice_in_dim(slot_freqs, first_step, per_device)
    own_counts = counts[own_freqs]
    longest = jnp.max(counts)
    all_times = jnp.arange(L, dtype=jnp.int32)
    series = lax.all_to_all(scaled, TM, split_axis=2, concat_axis=0, tiled=True)
    phases = phase_table(slot_freqs, all_times)
    real_part = jnp.einsum("sn,nzxy->szxy", jnp.cos(phases), series, precision=highest)
    imag_part = -jnp.einsum("sn,nzxy->szxy", jnp.sin(phases), series, precision=highest)
    spectrum = lax.all_to_all(
        jnp.stack([real_part, imag_part], axis=1), TM, split_axis=0, concat_axis=3, tiled=True
    )
    solved = solve_together(spectrum, absorption, own_freqs, own_counts, longest)
    gathered = lax.all_to_all(solved, TM, split_axis=3, concat_axis=0, tiled=True)
    phases = phase_table(all_times, slot_freqs)
    values = jnp.einsum("ns,szxy->nzxy", jnp.cos(phases), gathered[:, 0], precision=highest)
    values = values - jnp.einsum(
        "ns,szxy->nzxy", jnp.sin(phases), gathered[:, 1], precision=highest
    )
    weight = jnp.power(decay_rate, -all_times.astype(jnp.float32)) / L
    values = values * weight[:, None, None, None]
    return lax.all_to_all(values, TM, split_axis=0, concat_axis=2, tiled=True)


def real_transform(x):
    n = len(x)
    if n == 2:
        return [(x[0] + x[1], None), (x[0] - x[1], None)]
    even, odd = real_transform(x[0::2]), real_transform(x[1::2])
    out = [None] * (n // 2 + 1)
    out[0] = (even[0][0] + odd[0][0], None)
    out[n // 2] = (even[0][0] - odd[0][0], None)
    out[n // 4] = (even[n // 4][0], -odd[n // 4][0])
    for k in range(1, n // 4):
        cos, sin = math.cos(2 * math.pi * k / n), math.sin(2 * math.pi * k / n)
        (er, ei), (cr, ci) = even[k], odd[k]
        tr, ti = cos * cr + sin * ci, cos * ci - sin * cr
        out[k] = (er + tr, ei + ti)
        out[n // 2 - k] = (er - tr, ti - ei)
    return out


def real_inverse(spectrum):
    n = 2 * (len(spectrum) - 1)
    first, last = spectrum[0][0], spectrum[n // 2][0]
    if n == 2:
        return [first + last, first - last]
    even, odd = [None] * (n // 4 + 1), [None] * (n // 4 + 1)
    even[0], odd[0] = (first + last, None), (first - last, None)
    mid_re, mid_im = spectrum[n // 4]
    even[n // 4], odd[n // 4] = (mid_re + mid_re, None), (-(mid_im + mid_im), None)
    for k in range(1, n // 4):
        cos, sin = math.cos(2 * math.pi * k / n), math.sin(2 * math.pi * k / n)
        (ar, ai), (br, bi) = spectrum[k], spectrum[n // 2 - k]
        even[k] = (ar + br, ai - bi)
        tr, ti = ar - br, ai + bi
        odd[k] = (cos * tr - sin * ti, cos * ti + sin * tr)
    halves = real_inverse(even), real_inverse(odd)
    return [halves[i % 2][i // 2] for i in range(n)]


def bands_kernel(x_ref, a_ref, out_ref, rows_ref, sems):
    copies = [
        pltpu.make_async_copy(x_ref.at[:, :, pl.ds(8 * band, 8), :], out_ref.at[band], sems.at[band]) for band in range(16)
    ]
    first = 16 * lax.axis_index("z") + 16 * lax.axis_index("core") - 8
    for core in range(2):
        row = pl.multiple_of(jnp.clip(first + 8 * core, 0, NX - 8), 8)
        copies.append(pltpu.make_async_copy(a_ref.at[:, pl.ds(row, 8), :], rows_ref.at[core], sems.at[16 + core]))
    for copy in copies:
        copy.start()
    for copy in copies:
        copy.wait()


def forward_kernel(x_ref, rows_ref, out_ref):
    for core in range(2):
        for zz in range(2):
            rows = rows_ref[core, zz]
            for slot in range(16 * core, 16 * core + 16):
                out_ref[slot, 4 + zz] = rows
    for zz in range(2):
        spectrum = real_transform([x_ref[n, zz] * decay**n for n in range(L)])
        out_ref[0, zz] = spectrum[0][0]
        out_ref[0, 2 + zz] = spectrum[PAIRS][0]
        for k in range(1, PAIRS):
            out_ref[k, zz] = spectrum[k][0]
            out_ref[k, 2 + zz] = spectrum[k][1]


def inverse_kernel(s_ref, out_ref, failed_ref):
    failed = jnp.zeros((8, 128), jnp.float32)
    for zz in range(2):
        ends = [s_ref[0, part, zz] for part in range(2)]
        spectrum = [(ends[0] + ends[0], None)]
        spectrum += [(s_ref[k, 0, zz], s_ref[k, 1, zz]) for k in range(1, PAIRS)]
        spectrum += [(ends[1] + ends[1], None)]
        values = real_inverse(spectrum)
        for n in range(L):
            out_ref[n, zz] = values[n] * (decay ** (-n) / (2 * L))
        failed = jnp.where(values[0] != values[0], 1.0, failed)
    failed_ref[0] = jnp.where(jnp.max(failed) > 0.0, 1, 0)


same = [(i, j) for i in range(STEPS + 1) for j in range(i, STEPS + 1)]
cross = [(i, j) for i in range(STEPS + 1) for j in range(i + 1, STEPS + 1)]
entry = {(kind, i, j): None for kind, ij in (("re", same), ("im", same), ("x", cross)) for i, j in ij}
for at, name in enumerate(entry):
    entry[name] = at


def tree_sum(terms):
    while len(terms) > 1:
        terms = [sum(terms[i : i + 2][1:], terms[i]) for i in range(0, len(terms), 2)]
    return terms[0]


def pick(slot, values):
    found = jnp.float32(values[0])
    for i in range(1, len(values)):
        found = jnp.where(slot == i, jnp.float32(values[i]), found)
    return found


def edges_kernel(own_ref, first_ref, second_ref, abs_ref):
    low = lax.axis_index("core") == 0
    for sp in range(16):
        for i in range(4):
            up, down = own_ref[1, sp, i, pl.ds(8 - HALO, HALO), :], own_ref[0, sp, i, pl.ds(0, HALO), :]
            first_ref[sp, pl.ds(HALO * i, HALO), :] = jnp.where(low, up, down)
            second_ref[sp, pl.ds(HALO * i, HALO), :] = jnp.where(low, down, up)
        for side in range(2):
            for zz in range(2):
                abs_ref[side, sp, zz] = own_ref[side, sp, 4 + zz]


def inverses_kernel(own_ref, swap_ref, inv_ref, edge_inv_ref):
    slot, z, core = lax.axis_index(SLOTS), lax.axis_index("z"), lax.axis_index("core")
    upper = lax.broadcasted_iota(jnp.int32, (8, 128), 0) < 4
    shifts_here = slot_shifts()
    shift_a, shift_b, shift_im = (pick(slot, shifts_here[:, i]) for i in range(3))

    def prepare(sp, _):
        edges = {}
        for tile in range(4):
            for zz in range(2):
                mine, other = own_ref[tile // 2, sp, 4 + zz], swap_ref[tile // 2, sp, zz]
                base = jnp.where(core == tile % 2, mine, other)
                da, db = (shift_a + 6.0) + base, (shift_b + 6.0) + base
                ra, rb = 1.0 / (da * da + shift_im * shift_im), 1.0 / (db * db + shift_im * shift_im)
                found = [da * ra, db * rb, -shift_im * ra]
                if tile in (1, 2):
                    for i in range(3):
                        inv_ref[i, tile - 1, sp, zz] = found[i]
                else:
                    inside = z > 0 if tile == 0 else z < lax.axis_size("z") - 1
                    for i in range(3):
                        edges[tile, zz, i] = jnp.where(inside, found[i], 0.0)
                        edge_inv_ref[i, tile // 3, sp, zz] = edges[tile, zz, i]
        for zz in range(2):
            for i in range(3):
                edge_inv_ref[i, 2, sp, zz] = jnp.where(upper, edges[3, zz, i], edges[0, zz, i])
        return 0

    lax.fori_loop(0, NZ // 2, prepare, 0, unroll=4)


def basis_kernel(own_ref, first_ref, second_ref, inv_ref, edge_inv, v_ref, gram_ref, u, sums):
    core = lax.axis_index("core")
    lanes = lax.broadcasted_iota(jnp.int32, (8, 128), 1)
    first_lane, last_lane = lanes == 0, lanes == 127
    upper = lax.broadcasted_iota(jnp.int32, (8, 128), 0) < 4
    blank = jnp.zeros((8, 128), jnp.float32)

    for turn in range(2):
        for part in range(2):
            for row in range(8, 40, 8):
                u[turn, part, 0, pl.ds(row, 8), :] = blank
                u[turn, part, NZ + 1, pl.ds(row, 8), :] = blank

    def put(turn, tiles, layer, inverse, re, im):
        a, b, c = inverse
        pair = a * re - c * im, b * im + c * re
        for tile in tiles:
            for part in range(2):
                u[turn, part, layer, pl.ds(8 + 8 * tile, 8), :] = pair[part]

    def prepare(sp, _):
        for turn in range(2):
            for part in range(2):
                for zz in range(2):
                    u[turn, part, 2 * sp + zz + 1, pl.ds(0, 8), :] = blank
                    u[turn, part, 2 * sp + zz + 1, pl.ds(40, 8), :] = blank
        for tile in range(4):
            for zz in range(2):
                if tile in (1, 2):
                    found = [inv_ref[i, tile - 1, sp, zz] for i in range(3)]
                    re, im = (own_ref[tile - 1, sp, 2 * part + zz] for part in range(2))
                else:
                    found = [edge_inv[i, tile // 3, sp, zz] for i in range(3)]
                    pair = []
                    for part in range(2):
                        at = HALO * (2 * part + zz)
                        wanted = at - (8 - HALO) if tile == 0 else at
                        start = min(max(wanted, 0), 4 * HALO - 8)
                        first, second = (ref[sp, pl.ds(start, 8), :] for ref in (first_ref, second_ref))
                        rows = jnp.where((core == 0) == (tile == 0), first, second)
                        shift = (start - wanted) % 8
                        pair.append(pltpu.roll(rows, shift, 0) if shift else rows)
                    re, im = pair
                put(0, (tile,), 2 * sp + zz + 1, found, re, im)
        return 0

    lax.fori_loop(0, NZ // 2, prepare, 0, unroll=4)

    def vector(j, side, sp, zz):
        if j == 0:
            return [own_ref[side, sp, 2 * part + zz] for part in range(2)]
        return [v_ref[j - 1, part, side, sp, zz] for part in range(2)]

    def nearby(old, tile, layer, j):
        def rows(z_off, x_off):
            before, behind = (old[layer + z_off, pl.ds(row + x_off, 8), :] for row in (8, 32))
            if j == 1:
                return jnp.where(upper, behind, before)
            return behind if x_off < 0 else before

        if tile != BOTH:
            def rows(z_off, x_off):
                return old[layer + z_off, pl.ds(8 + 8 * tile + x_off, 8), :]

        here = rows(0, 0)
        total = (rows(-1, 0) + rows(1, 0)) + (rows(0, -1) + rows(0, 1))
        return total + (
            jnp.where(first_lane, 0.0, pltpu.roll(here, 1, 1)) + jnp.where(last_lane, 0.0, pltpu.roll(here, 127, 1))
        )

    for j in range(STEPS):
        tiles = (0, 1, 2, 3) if j == 0 else (1, 2, BOTH) if j < STEPS - 1 else (1, 2)
        names = [name for name in entry if name[2] == j + 1 or (j == 0 and name[2] == 0)]

        def step(group, totals, j=j, names=names, tiles=tiles):
            found = {}
            for sp in [4 * group + s for s in range(4)]:
                for zz in range(2):
                    for tile in tiles:
                        layer = 2 * sp + zz + 1
                        pair = [nearby(u.at[j % 2, part], tile, layer, j) for part in range(2)]
                        if tile in (1, 2):
                            side = tile - 1
                            if j < STEPS - 1:
                                for part in range(2):
                                    v_ref[j, part, side, sp, zz] = pair[part]
                            known = [vector(i, side, sp, zz) for i in range(j + 1)] + [pair]
                            for kind, i, k in names:
                                a, b = known[i], known[k]
                                if kind == "x":
                                    product = a[0] * b[1] - a[1] * b[0]
                                else:
                                    part = ("re", "im").index(kind)
                                    product = a[part] * b[part]
                                name = kind, i, k
                                found[name] = found[name] + product if name in found else product
                        if j < STEPS - 1:
                            if tile in (1, 2):
                                inverse = [inv_ref[i, tile - 1, sp, zz] for i in range(3)]
                            else:
                                inverse = [edge_inv[i, (0, None, None, 1, 2)[tile], sp, zz] for i in range(3)]
                            put((j + 1) % 2, (0, 3) if tile == BOTH else (tile,), layer, inverse, *pair)
            return tuple(t + found[name] for t, name in zip(totals, names))

        totals = lax.fori_loop(0, NZ // 8, step, tuple(blank for _ in names), unroll=2)
        for name, total in zip(names, totals):
            sums[entry[name]] = total
    for spare in range(len(entry), sums.shape[0]):
        sums[spare] = blank

    rows = jnp.sum(sums[...], axis=1)
    column = jnp.sum(rows, axis=1, keepdims=True)
    where = lax.broadcasted_iota(jnp.int32, rows.shape, 0) == lax.broadcasted_iota(jnp.int32, rows.shape, 1)
    packed = jnp.sum(jnp.where(where, column, 0.0), axis=0, keepdims=True)
    gram_ref[...] = jnp.broadcast_to(packed[None], gram_ref.shape)


def multiplied(a, b):
    return (a[0] * b[0] - a[1] * b[1], a[0] * b[1] + a[1] * b[0])


def combine_kernel(count_ref, part_ref, own_ref, v_ref, inv_ref, out_ref):
    slot = lax.axis_index(SLOTS)
    ends = slot == 0
    low = lax.broadcasted_iota(jnp.int32, (8, 128), 1) < 64
    row = tree_sum([part_ref[i] for i in range(part_ref.shape[0])])

    def spread(name):
        return jnp.broadcast_to(row[:, entry[name] : entry[name] + 1], (8, 128))

    gram = {}
    for i, j in same:
        re, im = spread(("re", i, j)), spread(("im", i, j))
        real = jnp.where(ends, jnp.where(low, re, im), re + im)
        imag = jnp.where(ends, 0.0, spread(("x", i, j))) if j > i else jnp.zeros_like(real)
        gram[i, j] = (real, imag)

    count_lane = lax.broadcasted_iota(jnp.int32, (1, L), 1)
    count_a, count_b = (
        jnp.sum(jnp.where(count_lane == k, count_ref[...], 0).astype(jnp.float32), axis=1, keepdims=True)
        for k in (slot, jnp.where(ends, PAIRS, L - slot))
    )
    one, none = jnp.ones((8, 128), jnp.float32), jnp.zeros((8, 128), jnp.float32)
    poly, answer = [(one, none)], [(none, none) for _ in range(STEPS)]
    sizes = [jnp.sqrt(jnp.maximum(gram[i, i][0], 0.0)) for i in range(STEPS + 1)]
    doubt, scale = none, None
    for m in range(STEPS):
        in_a, in_b = (jnp.broadcast_to(jnp.where(m < count, 1.0, 0.0), (8, 128)) for count in (count_a, count_b))
        weight = jnp.where(ends, jnp.where(low, in_a, in_b), in_a + in_b)
        g00, g01, g11 = gram[0, 0][0], gram[0, 1], gram[1, 1][0]
        denominator = (g00 - 2.0 * g01[0] + g11) + norm_floor
        inverse = 1.0 / denominator
        coef = ((g00 - g01[0]) * inverse, g01[1] * inverse)
        size = jnp.abs(coef[0]) + jnp.abs(coef[1])
        length = jnp.sqrt(jnp.maximum(g00, 0.0))
        if m == 0:
            scale = size * length
        pair = sizes[0] + sizes[1]
        step_doubt = (gram_rounding * (1 + m / 2)) * pair * (sizes[0] + size * pair) * jnp.abs(inverse) * length
        doubt = doubt + jnp.where(weight > 0.0, step_doubt, none)
        for j, p in enumerate(poly):
            term = multiplied(coef, p)
            answer[j] = (answer[j][0] + weight * term[0], answer[j][1] + weight * term[1])
        if m == STEPS - 1:
            break
        rest = (1.0 - coef[0], -coef[1])
        following = []
        for j in range(len(poly) + 1):
            kept = multiplied(rest, poly[j]) if j < len(poly) else (none, none)
            moved = multiplied(coef, poly[j - 1]) if j > 0 else (none, none)
            following.append((kept[0] + moved[0], kept[1] + moved[1]))
        poly = following
        rr = rest[0] * rest[0] + rest[1] * rest[1]
        cc = coef[0] * coef[0] + coef[1] * coef[1]
        rc = multiplied((rest[0], -rest[1]), coef)
        cr = (rc[0], -rc[1])
        size_rest = jnp.abs(rest[0]) + jnp.abs(rest[1])
        sizes = [size_rest * a + size * b for a, b in zip(sizes[:-1], sizes[1:])]

        def at(i, j):
            return gram[i, j] if i <= j else (gram[j, i][0], -gram[j, i][1])

        shrunk = {}
        top = STEPS - m
        for i in range(top):
            for j in range(i, top):
                a, b, d = at(i, j), at(i, j + 1), at(i + 1, j + 1)
                if i == j:
                    ab = multiplied(rc, b)
                    shrunk[i, j] = (rr * a[0] + 2.0 * ab[0] + cc * d[0], none)
                else:
                    ab, ac = multiplied(rc, b), multiplied(cr, at(i + 1, j))
                    shrunk[i, j] = tuple(rr * a[x] + (ab[x] + ac[x]) + cc * d[x] for x in range(2))
        gram = shrunk

    trusted = doubt <= error_allowed * scale
    weights = []
    for re, im in answer:
        re = jnp.where(trusted, re, jnp.nan)
        weights.append(
            (
                jnp.broadcast_to(re[:, 0:1], (8, 128)),
                jnp.broadcast_to(re[:, 127:128], (8, 128)),
                jnp.broadcast_to(im[:, 0:1], (8, 128)),
            )
        )

    def finish(sp, _):
        for side in range(2):
            for zz in range(2):
                res, ims = [], []
                for j, (wa, wb, wi) in enumerate(weights):
                    re, im = ((own_ref[side, sp, 2 * part + zz] if j == 0 else v_ref[j - 1, part, side, sp, zz]) for part in range(2))
                    res.append(wa * re - wi * im)
                    ims.append(wb * im + wi * re)
                re, im = tree_sum(res), tree_sum(ims)
                a, b, c = (inv_ref[i, side, sp, zz] for i in range(3))
                out_ref[16 * side + sp, 0, zz] = a * re - c * im
                out_ref[16 * side + sp, 1, zz] = b * im + c * re
        return 0

    lax.fori_loop(0, NZ // 2, finish, 0, unroll=2)


def slot_shifts():
    table = np.zeros((PAIRS, 4), np.float32)
    for slot in range(PAIRS):
        angle = 2 * math.pi * slot / L
        table[slot, :2] = (1 - decay * math.cos(angle)) / step_size
        table[slot, 2] = decay * math.sin(angle) / step_size
    table[0, 1] = (1 + decay) / step_size
    return table


def exchanged(blocks, axes):
    return lax.all_to_all(blocks, axes, split_axis=0, concat_axis=0, tiled=True)


VMEM = pl.BlockSpec(memory_space=pltpu.VMEM)
SMEM = pl.BlockSpec(memory_space=pltpu.SMEM)
ANY = pl.BlockSpec(memory_space=pl.ANY)


def f32(*shape):
    return pltpu.VMEM(shape, jnp.float32)


def held(x):
    return pltpu.with_memory_space_constraint(x, pltpu.MemorySpace.VMEM)


def in_hbm(x):
    return pltpu.with_memory_space_constraint(x, pltpu.MemorySpace.HBM)


def room(mebibytes):
    return pltpu.CompilerParams(vmem_limit_bytes=mebibytes * 2**20)


def together(residual, absorption, counts):
    chips = lax.axis_size("z")
    bands, rows = pl.pallas_call(
        bands_kernel,
        out_shape=(f32(16, 4, 2, 8, 128), f32(2, 2, 8, 128)),
        in_specs=[ANY, ANY],
        out_specs=(VMEM, VMEM),
        scratch_shapes=[pltpu.SemaphoreType.DMA((18,))],
        compiler_params=room(2),
        name="bands",
    )(in_hbm(residual), in_hbm(absorption))
    series = exchanged(bands, TM).reshape(L, 2, 8, 128)
    spectrum = pl.pallas_call(
        forward_kernel,
        out_shape=f32(PAIRS, 6, 8, 128),
        in_specs=[VMEM, VMEM],
        out_specs=VMEM,
        compiler_params=room(4),
        name="forward",
    )(held(series), held(rows))
    own = held(exchanged(spectrum, SLOTS).reshape(2, 16, 6, 8, 128))
    first, second, swap = pl.pallas_call(
        edges_kernel,
        out_shape=(f32(16, 4 * HALO, 128), f32(16, 4 * HALO, 128), f32(2, 16, 2, 8, 128)),
        in_specs=[VMEM],
        out_specs=(VMEM, VMEM, VMEM),
        compiler_params=room(2),
        name="edges",
    )(own)
    ups = [[(2 * i + core, 2 * i + 2 + core) for i in range(chips - 1)] for core in range(2)]
    downs = [[(b, a) for a, b in pairs] for pairs in ups]
    first = lax.ppermute(first, TM, ups[0] + downs[1])
    second = lax.ppermute(second, TM, downs[0] + ups[1])
    swap = lax.ppermute(swap, "core", [(0, 1), (1, 0)])
    inverses, edge_inverses = pl.pallas_call(
        inverses_kernel,
        out_shape=(f32(3, 2, 16, 2, 8, 128), f32(3, 3, 16, 2, 8, 128)),
        in_specs=[VMEM, VMEM],
        out_specs=(VMEM, VMEM),
        compiler_params=room(2),
        cost_estimate=pl.CostEstimate(flops=2 * 10**6, bytes_accessed=2 * 10**6, transcendentals=0),
        name="inverses",
    )(own, held(swap))
    basis, partial = pl.pallas_call(
        basis_kernel,
        out_shape=(f32(STEPS - 1, 2, 2, 16, 2, 8, 128), f32(8, 8, 128)),
        in_specs=[VMEM] * 5,
        out_specs=(VMEM, VMEM),
        scratch_shapes=[
            pltpu.VMEM((2, 2, NZ + 2, 48, 128), jnp.float32),
            pltpu.VMEM((80, 8, 128), jnp.float32),
        ],
        compiler_params=room(10),
        name="basis",
    )(own, held(first), held(second), held(inverses), held(edge_inverses))
    partials = exchanged(partial, "z")
    solved = pl.pallas_call(
        combine_kernel,
        out_shape=f32(PAIRS, 2, 2, 8, 128),
        in_specs=[VMEM, VMEM, VMEM, VMEM, VMEM],
        out_specs=VMEM,
        compiler_params=room(6),
        name="combine",
    )(held(counts.reshape(1, L)), held(partials), own, held(basis), held(inverses))
    gathered, *arguments = lax.optimization_barrier((exchanged(solved, SLOTS), residual, absorption, counts))
    values, failed = pl.pallas_call(
        inverse_kernel,
        out_shape=(f32(L, 2, 8, 128), pltpu.SMEM((1,), jnp.int32)),
        in_specs=[VMEM],
        out_specs=(VMEM, SMEM),
        compiler_params=room(4),
        name="inverse",
    )(held(gathered))
    return values, failed, arguments


def taken_kernel(*refs):
    count = len(refs) // 2
    copies = [pltpu.make_async_copy(refs[i], refs[count + i], refs[-1].at[i]) for i in range(count)]
    for copy in copies:
        copy.start()
    for copy in copies:
        copy.wait()


def taken(*arrays):
    return pl.pallas_call(
        taken_kernel,
        out_shape=tuple(f32(*a.shape) for a in arrays),
        in_specs=[ANY] * len(arrays),
        out_specs=(VMEM,) * len(arrays),
        scratch_shapes=[pltpu.SemaphoreType.DMA((len(arrays),))],
        compiler_params=room(2),
        name="taken",
    )(*(in_hbm(a) for a in arrays))


def to_bands(steps):
    return steps.reshape(4, 2, 16, 8, 128).transpose(2, 0, 1, 3, 4)


def body(residual, absorption, counts):
    values, failed, arguments = together(residual, absorption, counts)
    bands = lax.cond(
        failed[0] > 0,
        lambda r, a, c, v: to_bands(stepwise(*taken(r, a), c)),
        lambda r, a, c, v: exchanged(v.reshape(16, 4, 2, 8, 128), TM),
        *arguments, values,
    )
    return bands.transpose(1, 2, 0, 3, 4).reshape(residual.shape)


def solution(mesh):
    chips, cores = mesh.shape["tm"] // 2, 2
    devices = mesh.devices.reshape(chips, cores, 4, 4)
    inner = Mesh(devices, ("z", "core", "y", "x"))
    in_specs = (P(TM, SPACE, None, None), P(SPACE, None, None), P())
    out_specs = P(TM, SPACE, None, None)
    return jax.shard_map(body, mesh=inner, in_specs=in_specs, out_specs=out_specs, check_vma=False)
```
